256 devices in a mesh: row: 16 (over y, x), col: 16 (over z, core).
Axes of the slice: x: 4, y: 4, z: 8, core: 2. Of those that a mesh axis runs over, the one named last changes fastest.
Arguments:
- tile_data: bfloat16 [1024, 128, 128], P(('row', 'col')), may hold values from -24 to 24
- tile_coords: int32 [3, 1024], P(None, ('row', 'col')), may hold values from 0 to 2047, as said below
- tile_counts: int32 [256], P(('row', 'col')), may hold values from 1 to 4, as said below
- factor_rows: float32 [64, 32768], P(None, ('row', 'col')), may hold values from -6 to 6
- factor_cols: float32 [64, 32768], P(None, ('col', 'row')), may hold values from -6 to 6
- factor_depth: float32 [64, 2048], P(None, ('row', 'col')), may hold values from -6 to 6
- damping: float32 [], replicated, may hold values from 128 to 512
Outputs:
- step_a: float32 [64, 32768], P(None, ('row', 'col'))
- step_b: float32 [64, 32768], P(None, ('col', 'row'))
- step_c: float32 [64, 2048], P(None, ('row', 'col'))
The draws below stay inside these ranges and needn't reach their ends.
Inputs may be any that keep to these rules, and one draw needn't show every extreme that they name: `tile_coords`: the first row names a tile's block within its device's group of 16 first-mode blocks, the second its block within the group of 16 second-mode blocks, the third its third-mode index below 2048. `tile_counts`: slots at and beyond a device's count are padding and carry nothing; some device fills all 4 slots.
All inputs are finite; a program needn't handle non-finite values.
Results may differ from the reference program's by a relative error of at most 0.0003.
Values sent between devices are 32-bit elements; how exact they have to be, the bound alone decides.
No kernel may reach another device: no remote copies, remote signals or barrier semaphores. Data moves between devices by JAX's collectives and lax.ppermute only.
A program may use at most 64 MiB of HBM per device.

```python
import math
import jax
import jax.numpy as jnp
from jax import lax

RANK = 64
TILE = 128
RB = 16
CB = 16
TCAP = 4
ITERS = 2
MODE_ROWS = 32768
MODE_COLS = 32768
DEPTH = 2048
TILES_ALL = 1024
N_ROW = 16
N_COL = 16


def draw_tile_coords(key, part):
    key_rows, key_cols, key_depth = jax.random.split(key, 3)
    block_rows = jax.random.randint(key_rows, (TILES_ALL,), 0, RB)
    block_cols = jax.random.randint(key_cols, (TILES_ALL,), 0, CB)
    depth_index = jax.random.randint(key_depth, (TILES_ALL,), 0, DEPTH)
    return jnp.stack([block_rows, block_cols, depth_index]).astype(jnp.int32)


def draw_tile_counts(key, part):
    key_base, key_top = jax.random.split(key, 2)
    device_total = N_ROW * N_COL
    base_counts = jax.random.randint(key_base, (device_total,), TCAP // 4, TCAP + 1)
    fullest = jax.random.randint(key_top, (), 0, device_total)
    placed = jnp.arange(device_total, dtype=jnp.int32) == fullest
    return jnp.where(placed, TCAP, base_counts).astype(jnp.int32)


def level_of(stream_key, shape, cuts, least, largest):
    loudness, own = 1.0, jax.random.fold_in(stream_key, 6)
    for position, shards_of in cuts:
        heights = jnp.exp(jax.random.uniform(jax.random.fold_in(own, position), (shards_of,), jnp.float32, least / len(cuts), largest / len(cuts)))
        loudness = loudness * jnp.repeat(heights, shape[position] // shards_of).reshape([-1 if axis == position else 1 for axis in range(len(shape))])
    return loudness


def noise(stream_key, shape, spread, most, cuts=(), kind=jnp.bfloat16):
    factor_of = level_of(stream_key, shape, cuts, -0.22, 0.18) if cuts else 1.0
    result = jax.random.normal(stream_key, shape, jnp.float32) * spread * factor_of
    return jnp.minimum(jnp.maximum(result, -most), most).astype(kind)


def setup_inputs(seed: int = 0) -> dict:
    arg_keys = jax.random.split(jax.random.key(seed), 8)
    tile_data = noise(arg_keys[0], (TILES_ALL, TILE, TILE), 4.0, 24.0, ((0, 256),))
    tile_coords = draw_tile_coords(jax.random.fold_in(arg_keys[7], 71), 0)
    tile_counts = draw_tile_counts(jax.random.fold_in(arg_keys[7], 71), 0)
    factor_rows = noise(arg_keys[3], (RANK, MODE_ROWS), 1.0, 6.0, ((1, 256),), jnp.float32)
    factor_cols = noise(arg_keys[4], (RANK, MODE_COLS), 1.0, 6.0, ((1, 256),), jnp.float32)
    factor_depth = noise(arg_keys[5], (RANK, DEPTH), 1.0, 6.0, ((1, 256),), jnp.float32)
    damping = jnp.clip(jnp.exp(jax.random.uniform(arg_keys[6], (), jnp.float32, math.log(128.0), math.log(512.0))), 128.0, 512.0)
    return {"tile_data": tile_data, "tile_coords": tile_coords, "tile_counts": tile_counts, "factor_rows": factor_rows, "factor_cols": factor_cols, "factor_depth": factor_depth, "damping": damping}


exact_precision = lax.Precision.HIGHEST


def make_onehot(indices, block_count):
    return (indices[:, None] == jnp.arange(block_count, dtype=jnp.int32)[None, :]).astype(jnp.float32)


def pick_rows(onehot, blocks):
    shaped = blocks.reshape(blocks.shape[0], onehot.shape[1], blocks.shape[1] // onehot.shape[1])
    return jnp.einsum('tq,rqa->tra', onehot.astype(blocks.dtype), shaped, precision=exact_precision)


def fold_rows(onehot, grads):
    summed = jnp.einsum('tq,tra->rqa', onehot.astype(grads.dtype), grads, precision=exact_precision)
    return summed.reshape(summed.shape[0], summed.shape[1] * summed.shape[2])


def tile_model(rows_a, rows_b, rows_c):
    return jnp.einsum('tra,trb->tab', rows_a, rows_b * rows_c[:, :, None], precision=exact_precision)


def tile_products(rows_a, rows_b, rows_c, dir_a, dir_b, dir_c):
    depth_cols = rows_c[:, :, None]
    left_side = jnp.concatenate([dir_a, rows_a, rows_a], axis=1)
    right_side = jnp.concatenate([rows_b * depth_cols, dir_b * depth_cols, rows_b * dir_c[:, :, None]], axis=1)
    return jnp.einsum('tra,trb->tab', left_side, right_side, precision=exact_precision)


def tile_transpose(values, rows_a, rows_b, rows_c):
    depth_cols = rows_c[:, :, None]
    row_raw = jnp.einsum('tab,trb->tra', values, rows_b, precision=exact_precision)
    grad_rows = row_raw * depth_cols
    grad_cols = jnp.einsum('tab,tra->trb', values, rows_a * depth_cols, precision=exact_precision)
    grad_depth = jnp.sum(rows_a * row_raw, axis=2)
    return grad_rows, grad_cols, grad_depth


def reference(tile_data, tile_coords, tile_counts, factor_rows, factor_cols, factor_depth, damping):
    rows_group = RB * TILE
    cols_group = CB * TILE

    def apply_all(direction):
        def per_device(device, totals):
            device = jnp.asarray(device).astype(jnp.int32)
            grid_row = device // N_COL
            grid_col = device % N_COL
            start_a = (grid_row * rows_group).astype(jnp.int32)
            start_b = (grid_col * cols_group).astype(jnp.int32)
            block_a = lax.dynamic_slice_in_dim(factor_rows, start_a, rows_group, 1)
            block_b = lax.dynamic_slice_in_dim(factor_cols, start_b, cols_group, 1)
            coords_here = lax.dynamic_slice_in_dim(tile_coords, (device * TCAP).astype(jnp.int32), TCAP, 1)
            live_mask = (jnp.arange(TCAP, dtype=jnp.int32) < tile_counts[device]).astype(factor_rows.dtype)[:, None, None]
            pick_a = make_onehot(coords_here[0], RB)
            pick_b = make_onehot(coords_here[1], CB)
            rows_a = pick_rows(pick_a, block_a)
            rows_b = pick_rows(pick_b, block_b)
            rows_c = jnp.take(factor_depth, coords_here[2], axis=1).T
            if direction is None:
                data_here = lax.dynamic_slice_in_dim(tile_data, (device * TCAP).astype(jnp.int32), TCAP, 0).astype(factor_rows.dtype)
                values = data_here - tile_model(rows_a, rows_b, rows_c)
            else:
                dir_block_a = lax.dynamic_slice_in_dim(direction[0], start_a, rows_group, 1)
                dir_block_b = lax.dynamic_slice_in_dim(direction[1], start_b, cols_group, 1)
                dir_c = jnp.take(direction[2], coords_here[2], axis=1).T
                values = tile_products(rows_a, rows_b, rows_c, pick_rows(pick_a, dir_block_a), pick_rows(pick_b, dir_block_b), dir_c)
            grad_rows, grad_cols, grad_depth = tile_transpose(values * live_mask, rows_a, rows_b, rows_c)
            old_a = lax.dynamic_slice_in_dim(totals[0], start_a, rows_group, 1)
            total_a = lax.dynamic_update_slice_in_dim(totals[0], old_a + fold_rows(pick_a, grad_rows), start_a, 1)
            old_b = lax.dynamic_slice_in_dim(totals[1], start_b, cols_group, 1)
            total_b = lax.dynamic_update_slice_in_dim(totals[1], old_b + fold_rows(pick_b, grad_cols), start_b, 1)
            total_c = totals[2] + jax.ops.segment_sum(grad_depth, coords_here[2], num_segments=DEPTH).T
            return (total_a, total_b, total_c)

        start = (jnp.zeros_like(factor_rows), jnp.zeros_like(factor_cols), jnp.zeros_like(factor_depth))
        return lax.fori_loop(0, N_ROW * N_COL, per_device, start)

    def hessian(direction):
        applied = apply_all(direction)
        return tuple(part_one + damping * part_two for part_one, part_two in zip(applied, direction))

    def inner(first, second):
        return sum(jnp.sum(part_one * part_two) for part_one, part_two in zip(first, second))

    rhs = apply_all(None)
    solution = tuple(jnp.zeros_like(member) for member in rhs)
    residual = rhs
    direction = rhs
    norm_now = inner(residual, residual)
    for iteration in range(ITERS):
        image_vec = hessian(direction)
        step_size = norm_now / inner(direction, image_vec)
        solution = tuple(sol + step_size * dvec for sol, dvec in zip(solution, direction))
        residual = tuple(res - step_size * ivec for res, ivec in zip(residual, image_vec))
        norm_next = inner(residual, residual)
        direction = tuple(res + (norm_next / norm_now) * dvec for res, dvec in zip(residual, direction))
        norm_now = norm_next
    return (solution[0], solution[1], solution[2])
```

```python
import jax
import jax.numpy as jnp
from jax import lax
from jax.experimental import pallas as pl
from jax.experimental.pallas import tpu as pltpu
from jax.sharding import Mesh
from jax.sharding import PartitionSpec as P

ROW = ("y", "x")
ALL = ("y", "x", "z", "c")
ROW_COL = ("y", "x", "z", "c")
COL_ROW = ("z", "c", "y", "x")
R = 64
T = 128
TILES = 4
NZ = 8
NP = 16
F32 = jnp.float32
HIGH = lax.Precision.HIGHEST

VMEM = pl.BlockSpec(memory_space=pltpu.VMEM)
SMEM = pl.BlockSpec(memory_space=pltpu.SMEM)


def dot(a, b, ca, cb):
    return lax.dot_general(
        a, b, (((ca,), (cb,)), ((), ())), precision=HIGH, preferred_element_type=F32
    )


def shaped(*shape):
    return jax.ShapeDtypeStruct(shape, F32)


def call(body, outs, ins, scalars=0):
    return pl.pallas_call(
        body,
        out_shape=outs,
        in_specs=[SMEM] * scalars + [VMEM] * (len(ins) - scalars),
        out_specs=jax.tree.map(lambda _: VMEM, outs),
    )(*ins)


def lanes(shape):
    return lax.broadcasted_iota(jnp.int32, shape, len(shape) - 1)


def rows_of(shape):
    return lax.broadcasted_iota(jnp.int32, shape, len(shape) - 2)


def start_body(coords, fr, fd, out):
    eye = (rows_of((8, 8)) == lanes((8, 8))).astype(F32)
    columns = jnp.concatenate([dot(eye, fd[...], 1, 1), jnp.zeros((8, T - R), F32)], axis=1)
    row, lane = rows_of((8, T)), lanes((8, T))
    for t in range(TILES):
        here = (row == t // 2) & (lane == R + t % 2)
        columns = jnp.where(here, coords[2, t].astype(F32), columns)
    a = fr[...]
    for z in range(NZ):
        out[z, :R] = a
        out[z, R : R + 8] = columns


def turn_body(gz, fc, out):
    low = jnp.concatenate([gz[z, R : R + 8] for z in range(4)], axis=0)
    high = jnp.concatenate([gz[z, R : R + 8] for z in range(4, 8)], axis=0)
    lane = lanes((32, T))
    packed = jnp.where(lane < R, low, pltpu.roll(high, R, 1))
    index = jnp.concatenate([gz[z, R : R + 2] for z in range(NZ)], axis=0)
    index = pltpu.roll(index, R, 1)
    b = fc[...]
    for p in range(NP):
        out[p, :R] = b
        out[p, R : R + 32] = packed
        out[p, R + 32 : R + 48] = index


def scatter_tile(t, coords, core, grad_a, grad_b, keep, send, fb):
    block = jnp.bitwise_and(coords[0, t], NP - 1)
    place, other = block // 2, jnp.bitwise_xor(block % 2, core)
    mine = other == 0
    keep[place] += jnp.where(mine, grad_a, 0.0)
    send[place] += jnp.where(mine, 0.0, grad_a)
    fb[jnp.bitwise_and(coords[1, t], NP - 1)] += grad_b


def pick_a(t, coords, core, own, oth):
    block = jnp.bitwise_and(coords[0, t], NP - 1)
    place, other = block // 2, jnp.bitwise_xor(block % 2, core)
    return jnp.where(other == 0, own[place, :R], oth[place, :R])


def depth_rows(parts):
    pad = jnp.zeros((6, T), F32)
    first = jnp.concatenate([parts[0], parts[1]], axis=1)
    second = jnp.concatenate([parts[2], parts[3]], axis=1)
    return jnp.concatenate([first, second, pad], axis=0)


def transposed_tile(v, a, b, c):
    raw = dot(b, v, 1, 1)
    grad_b = dot(a * c, v, 1, 0)
    depth = dot(jnp.ones((8, T), F32), a * raw, 1, 1)
    return raw * c, grad_b, depth[:1]


def first_body(
    coords, counts, core_ref, gz, oz, gr, orr, data, keep, send, fb, depth, ta, tb, tc, index
):
    core = core_ref[0]
    keep[...] = jnp.zeros(keep.shape, F32)
    send[...] = jnp.zeros(send.shape, F32)
    fb[...] = jnp.zeros(fb.shape, F32)
    picked = []
    lane_row = lanes((1, T))
    for t in range(TILES):
        k = jnp.bitwise_and(coords[2, t], 2047)
        far, near = k // T, k % T
        q, j = near // 8, near % 8
        z = q // 2
        place = (z % 4) * 8 + j
        own = gr[far, pl.ds(R + place, 1), :]
        oth = orr[far, pl.ds(place, 1), :]
        row = jnp.where(jnp.bitwise_xor(q % 2, core) == 0, own, oth)
        row = jnp.where(z // 4 == 0, row, pltpu.roll(row, R, 1))
        picked.append(jnp.where(lane_row < R, row, 0.0))
    chosen = jnp.concatenate([*picked, jnp.zeros((T - TILES, T), F32)], axis=0)
    column = chosen.T[:R]
    tc[...] = column
    mine = gr[:, R + 32 : R + 48, :].reshape(NP * 16, T)
    theirs = orr[:, 32:48, :].reshape(NP * 16, T)
    lane = lanes((NP * 16, T))
    index[...] = jnp.where(lane < 2, mine, pltpu.roll(theirs, 2, 1))
    parts = []
    for t in range(TILES):
        a = pick_a(t, coords, core, gz, oz)
        b = gr[jnp.bitwise_and(coords[1, t], NP - 1), :R]
        c = column[:, t : t + 1]
        ta[t] = a
        tb[t] = b
        model = dot(a, b * c, 0, 0)
        v = jnp.where(t < counts[0], data[t].astype(F32) - model, 0.0)
        grad_a, grad_b, part = transposed_tile(v, a, b, c)
        scatter_tile(t, coords, core, grad_a, grad_b, keep, send, fb)
        parts.append(part)
    depth[...] = depth_rows(parts)


def join_body(keep, received, depth, out):
    d = depth[...]
    for z in range(NZ):
        out[z, :R] = keep[z] + received[z]
        out[z, R : R + 8] = d


def cross_body(gz, fb, ga, spread, out):
    total = gz[0, :R]
    for z in range(1, NZ):
        total = total + gz[z, :R]
    ga[...] = total
    for z in range(NZ):
        spread[z] = total
    rows = jnp.concatenate([gz[z, R : R + 2] for z in range(NZ)], axis=0)
    if out.shape[1] > R + 16:
        scalars = gz[0, R : R + 8]
        for z in range(1, NZ):
            scalars = scalars + gz[z, R : R + 8]
    for p in range(NP):
        out[p, :R] = fb[p]
        out[p, R : R + 16] = rows
        if out.shape[1] > R + 16:
            out[p, R + 16 : R + 24] = scalars


def sum_b_body(gr, gb, spread):
    total = gr[0, :R]
    for p in range(1, NP):
        total = total + gr[p, :R]
    gb[...] = total
    for p in range(NP):
        spread[p] = total


def depth_sums(coords, start, gr, other, index):
    lane = lanes((1, T))
    wanted = jnp.where(
        (lane >= 8) & (lane < 16), (start + lane - 8).astype(F32), jnp.full((1, T), -1.0, F32)
    )
    for t in range(TILES):
        wanted = jnp.where(lane == t, coords[2, t].astype(F32), wanted)
    total = jnp.zeros((R, T), F32)
    for side in range(2):
        rows = gr[:, R : R + 16, :] if side == 0 else other[:, :16, :]
        rows = rows.reshape(NP * 16, T)
        for half in range(2):
            at = 2 * side + half
            chosen = (index[:, at : at + 1] == wanted).astype(F32)
            part = dot(rows, chosen, 0, 0)
            total = total + part[half * R : (half + 1) * R]
    return total


def apply_tile(t, coords, core, az, ao, br, ta, tb, tc, sums):
    a, b, c = ta[t], tb[t], tc[:, t : t + 1]
    da = pick_a(t, coords, core, az, ao)
    db = br[jnp.bitwise_and(coords[1, t], NP - 1)]
    dc = sums[:, t : t + 1]
    left = jnp.concatenate([da, a], axis=0)
    right = jnp.concatenate([b * c, db * c + b * dc], axis=0)
    return dot(left, right, 0, 0), a, b, c


def owned(sums):
    lane = lanes((R, T))
    return jnp.where((lane >= 8) & (lane < 16), sums, 0.0)


def middle_body(
    coords, counts, core_ref, start_ref, az, ao, br, gr, other, index, ta, tb, tc, ga, gb,
    keep, send, fb, depth, w, gc,
):
    core = core_ref[0]
    keep[...] = jnp.zeros(keep.shape, F32)
    send[...] = jnp.zeros(send.shape, F32)
    fb[...] = jnp.zeros(fb.shape, F32)
    sums = depth_sums(coords, start_ref[0], gr, other, index)
    mine = owned(sums)
    gc[...] = mine
    norm = jnp.sum(ga[...] * ga[...] + gb[...] * gb[...] + mine * mine)
    curve = jnp.zeros((T, T), F32)
    parts = []
    for t in range(TILES):
        product, a, b, c = apply_tile(t, coords, core, az, ao, br, ta, tb, tc, sums)
        v = jnp.where(t < counts[0], product, 0.0)
        w[t] = v
        curve = curve + v * v
        grad_a, grad_b, part = transposed_tile(v, a, b, c)
        scatter_tile(t, coords, core, grad_a, grad_b, keep, send, fb)
        parts.append(part)
    row, lane = rows_of((8, T)), lanes((8, T))
    out = depth_rows(parts)
    out = jnp.where((row == 2) & (lane == 0), norm, out)
    depth[...] = jnp.where((row == 2) & (lane == 1), jnp.sum(curve), out)


def both_norms(gr, other):
    total = jnp.sum(gr[:, R + 16 : R + 24, :], axis=0) + jnp.sum(other[:, 16:24, :], axis=0)
    row, lane = rows_of((8, T)), lanes((8, T))
    norm = jnp.sum(jnp.where((row == 2) & (lane == 0), total, 0.0))
    curve = jnp.sum(jnp.where((row == 2) & (lane == 1), total, 0.0))
    return norm, curve


def last_body(
    coords, counts, core_ref, start_ref, az, ao, br, gr, other, index, ta, tb, tc, w,
    ga0, gb0, gc0, ga1, gb1, ha, hb, hc, out,
):
    core = core_ref[0]
    norm, curve = both_norms(gr, other)
    mu = jnp.full((1, 1), curve, F32) / jnp.full((1, 1), norm, F32)
    sums = depth_sums(coords, start_ref[0], gr, other, index)
    a_rest = ga1[...] - mu * ga0[...]
    b_rest = gb1[...] - mu * gb0[...]
    c_rest = owned(sums) - mu * gc0[...]
    ha[...] = a_rest
    hb[...] = b_rest
    hc[...] = c_rest
    rest = jnp.sum(a_rest * a_rest + b_rest * b_rest + c_rest * c_rest)
    bend = jnp.zeros((T, T), F32)
    for t in range(TILES):
        product, _, _, _ = apply_tile(t, coords, core, az, ao, br, ta, tb, tc, sums)
        v = jnp.where(t < counts[0], product, 0.0) - mu * w[t]
        bend = bend + v * v
    row, lane = rows_of((8, T)), lanes((8, T))
    put = jnp.where((row == 0) & (lane == 0), rest, 0.0)
    put = jnp.where((row == 0) & (lane == 1), jnp.sum(bend), put)
    put = jnp.where((row == 0) & (lane == 2), norm, put)
    out[...] = jnp.where((row == 0) & (lane == 3), curve, put)


def end_body(damping, sums, own, ga0, gb0, gc0, ha, hb, hc, oa, ob, oc):
    lane = lanes((1, T))

    def scalar(ref, at):
        return jnp.sum(jnp.where(lane == at, ref[:1], 0.0), axis=1, keepdims=True)

    rest, bend = scalar(sums, 0), scalar(sums, 1)
    norm, curve = scalar(own, 2), scalar(own, 3)
    lam = damping[0]
    mu = curve / norm
    nu = 1.0 / (mu + lam)
    ratio = rest / norm
    second = 1.0 / (bend / rest + lam - ratio * nu)
    on_g = nu + second * ratio * nu * nu
    on_h = -second * nu
    oa[...] = on_g * ga0[...] + on_h * ha[...]
    ob[...] = on_g * gb0[...] + on_h * hb[...]
    oc[...] = (on_g * gc0[...] + on_h * hc[...])[:, 8:16]


def along_z(x):
    return lax.all_to_all(x, "z", 0, 0, tiled=True)


def along_row(x):
    return lax.all_to_all(x, ROW, 0, 0, tiled=True)


def swap(x):
    return lax.ppermute(x, "c", [(0, 1), (1, 0)])


def shares(keep, send, fb, depth, extra):
    joined = call(join_body, shaped(NZ, R + 8, T), (keep, swap(send), depth))
    gz = along_z(joined)
    ga, spread_a, payload = call(
        cross_body, (shaped(R, T), shaped(NZ, R, T), shaped(NP, R + 16 + extra, T)), (gz, fb)
    )
    gr = along_row(payload)
    gb, spread_b = call(sum_b_body, (shaped(R, T), shaped(NP, R, T)), (gr,))
    other = swap(gr[:, R:])
    az = along_z(spread_a)
    ao = swap(az)
    br = along_row(spread_b)
    return ga, gb, gr, other, az, ao, br


def per_device(data, coords, counts, fr, fc, fd, damping):
    core = lax.axis_index("c").reshape(1)
    start = (lax.axis_index(ROW_COL) * fd.shape[1]).reshape(1)
    gz = along_z(call(start_body, shaped(NZ, R + 8, T), (coords, fr, fd), 1))
    oz = swap(gz)
    gr = along_row(call(turn_body, shaped(NP, R + 48, T), (gz, fc)))
    orr = swap(gr[:, R:])
    folded = (shaped(NZ, R, T), shaped(NZ, R, T), shaped(NP, R, T), shaped(8, T))
    saved = (shaped(TILES, R, T), shaped(TILES, R, T), shaped(R, T), shaped(NP * 16, T))
    keep, send, fb, depth, ta, tb, tc, index = call(
        first_body, folded + saved, (coords, counts, core, gz, oz, gr, orr, data), 3
    )
    ga0, gb0, gr, other, az, ao, br = shares(keep, send, fb, depth, 0)
    keep, send, fb, depth, w, gc0 = call(
        middle_body,
        folded + (shaped(TILES, T, T), shaped(R, T)),
        (coords, counts, core, start, az, ao, br, gr, other, index, ta, tb, tc, ga0, gb0),
        4,
    )
    ga1, gb1, gr, other, az, ao, br = shares(keep, send, fb, depth, 8)
    ha, hb, hc, own = call(
        last_body,
        (shaped(R, T), shaped(R, T), shaped(R, T), shaped(8, T)),
        (coords, counts, core, start, az, ao, br, gr, other, index, ta, tb, tc, w)
        + (ga0, gb0, gc0, ga1, gb1),
        4,
    )
    spread = jnp.broadcast_to(own[None, :1], (256, 1, T))
    sums = jnp.sum(lax.all_to_all(spread, ALL, 0, 0, tiled=True), axis=0)
    return call(
        end_body,
        (shaped(R, T), shaped(R, T), shaped(R, 8)),
        (damping.reshape(1), sums, own, ga0, gb0, gc0, ha, hb, hc),
        1,
    )


def solution(mesh):
    finer = Mesh(mesh.devices.reshape(4, 4, 8, 2), ("y", "x", "z", "c"))
    in_specs = (
        P(ROW_COL, None, None),
        P(None, ROW_COL),
        P(ROW_COL),
        P(None, ROW_COL),
        P(None, COL_ROW),
        P(None, ROW_COL),
        P(),
    )
    out_specs = (P(None, ROW_COL), P(None, COL_ROW), P(None, ROW_COL))
    return jax.shard_map(
        per_device, mesh=finer, in_specs=in_specs, out_specs=out_specs, check_vma=False
    )
```

```python
import jax
import jax.numpy as jnp
from jax import lax
from jax.experimental import pallas as pl
from jax.experimental.pallas import tpu as pltpu
from jax.sharding import Mesh
from jax.sharding import PartitionSpec as P

ROW = ("y", "x")
ALL = ("y", "x", "z", "c")
ROW_COL = ("y", "x", "z", "c")
COL_ROW = ("z", "c", "y", "x")
R = 64
T = 128
TILES = 4
NZ = 8
NP = 16
F32 = jnp.float32
HIGH = lax.Precision.HIGHEST

VMEM = pl.BlockSpec(memory_space=pltpu.VMEM)
SMEM = pl.BlockSpec(memory_space=pltpu.SMEM)


def dot(a, b, ca, cb):
    return lax.dot_general(
        a, b, (((ca,), (cb,)), ((), ())), precision=HIGH, preferred_element_type=F32
    )


def shaped(*shape):
    return jax.ShapeDtypeStruct(shape, F32)


def call(body, outs, ins, scalars=0):
    return pl.pallas_call(
        body,
        out_shape=outs,
        in_specs=[SMEM] * scalars + [VMEM] * (len(ins) - scalars),
        out_specs=jax.tree.map(lambda _: VMEM, outs),
        compiler_params=pltpu.CompilerParams(vmem_limit_bytes=16 * 2**20),
    )(*ins)


def lanes(shape):
    return lax.broadcasted_iota(jnp.int32, shape, len(shape) - 1)


def rows_of(shape):
    return lax.broadcasted_iota(jnp.int32, shape, len(shape) - 2)


def start_body(coords, fr, fd, out):
    eye = (rows_of((8, 8)) == lanes((8, 8))).astype(F32)
    columns = jnp.concatenate([dot(eye, fd[...], 1, 1), jnp.zeros((8, T - R), F32)], axis=1)
    row, lane = rows_of((8, T)), lanes((8, T))
    for t in range(TILES):
        here = (row == t // 2) & (lane == R + t % 2)
        columns = jnp.where(here, coords[2, t].astype(F32), columns)
    a = fr[...]
    for z in range(NZ):
        out[z, :R] = a
        out[z, R : R + 8] = columns


def turn_body(gz, fc, out):
    low = jnp.concatenate([gz[z, R : R + 8] for z in range(4)], axis=0)
    high = jnp.concatenate([gz[z, R : R + 8] for z in range(4, 8)], axis=0)
    lane = lanes((32, T))
    packed = jnp.where(lane < R, low, pltpu.roll(high, R, 1))
    index = jnp.concatenate([gz[z, R : R + 2] for z in range(NZ)], axis=0)
    index = pltpu.roll(index, R, 1)
    b = fc[...]
    for p in range(NP):
        out[p, :R] = b
        out[p, R : R + 32] = packed
        out[p, R + 32 : R + 48] = index


def scatter_tile(t, coords, core, grad_a, grad_b, keep, send, fb):
    block = jnp.bitwise_and(coords[0, t], NP - 1)
    place, other = block // 2, jnp.bitwise_xor(block % 2, core)
    mine = other == 0
    keep[place] += jnp.where(mine, grad_a, 0.0)
    send[place] += jnp.where(mine, 0.0, grad_a)
    fb[jnp.bitwise_and(coords[1, t], NP - 1)] += grad_b


def pick_a(t, coords, core, own, oth):
    block = jnp.bitwise_and(coords[0, t], NP - 1)
    place, other = block // 2, jnp.bitwise_xor(block % 2, core)
    return jnp.where(other == 0, own[place, :R], oth[place, :R])


def depth_rows(parts):
    pad = jnp.zeros((6, T), F32)
    first = jnp.concatenate([parts[0], parts[1]], axis=1)
    second = jnp.concatenate([parts[2], parts[3]], axis=1)
    return jnp.concatenate([first, second, pad], axis=0)


def transposed_tile(v, a, b, c):
    raw = dot(b, v, 1, 1)
    grad_b = dot(a * c, v, 1, 0)
    depth = dot(jnp.ones((8, T), F32), a * raw, 1, 1)
    return raw * c, grad_b, depth[:1]


def first_body(
    coords, counts, core_ref, gz, oz, gr, orr, data, keep, send, fb, depth, ta, tb, tc, index
):
    core = core_ref[0]
    keep[...] = jnp.zeros(keep.shape, F32)
    send[...] = jnp.zeros(send.shape, F32)
    fb[...] = jnp.zeros(fb.shape, F32)
    picked = []
    lane_row = lanes((1, T))
    for t in range(TILES):
        k = jnp.bitwise_and(coords[2, t], 2047)
        far, near = k // T, k % T
        q, j = near // 8, near % 8
        z = q // 2
        place = (z % 4) * 8 + j
        own = gr[far, pl.ds(R + place, 1), :]
        oth = orr[far, pl.ds(place, 1), :]
        row = jnp.where(jnp.bitwise_xor(q % 2, core) == 0, own, oth)
        row = jnp.where(z // 4 == 0, row, pltpu.roll(row, R, 1))
        picked.append(jnp.where(lane_row < R, row, 0.0))
    chosen = jnp.concatenate([*picked, jnp.zeros((T - TILES, T), F32)], axis=0)
    column = chosen.T[:R]
    tc[...] = column
    mine = gr[:, R + 32 : R + 48, :].reshape(NP * 16, T)
    theirs = orr[:, 32:48, :].reshape(NP * 16, T)
    lane = lanes((NP * 16, T))
    index[...] = jnp.where(lane < 2, mine, pltpu.roll(theirs, 2, 1))
    parts = []
    for t in range(TILES):
        a = pick_a(t, coords, core, gz, oz)
        b = gr[jnp.bitwise_and(coords[1, t], NP - 1), :R]
        c = column[:, t : t + 1]
        ta[t] = a
        tb[t] = b
        model = dot(a, b * c, 0, 0)
        v = jnp.where(t < counts[0], data[t].astype(F32) - model, 0.0)
        grad_a, grad_b, part = transposed_tile(v, a, b, c)
        scatter_tile(t, coords, core, grad_a, grad_b, keep, send, fb)
        parts.append(part)
    depth[...] = depth_rows(parts)


def join_body(keep, received, depth, out):
    d = depth[...]
    for z in range(NZ):
        out[z, :R] = keep[z] + received[z]
        out[z, R : R + 8] = d


def cross_body(gz, fb, ga, spread, out):
    total = gz[0, :R]
    for z in range(1, NZ):
        total = total + gz[z, :R]
    ga[...] = total
    for z in range(NZ):
        spread[z] = total
    rows = jnp.concatenate([gz[z, R : R + 2] for z in range(NZ)], axis=0)
    if out.shape[1] > R + 16:
        scalars = gz[0, R : R + 8]
        for z in range(1, NZ):
            scalars = scalars + gz[z, R : R + 8]
    for p in range(NP):
        out[p, :R] = fb[p]
        out[p, R : R + 16] = rows
        if out.shape[1] > R + 16:
            out[p, R + 16 : R + 24] = scalars


def sum_b_body(gr, gb, spread):
    total = gr[0, :R]
    for p in range(1, NP):
        total = total + gr[p, :R]
    gb[...] = total
    for p in range(NP):
        spread[p] = total


def depth_sums(coords, start, gr, other, index):
    lane = lanes((1, T))
    wanted = jnp.where(
        (lane >= 8) & (lane < 16), (start + lane - 8).astype(F32), jnp.full((1, T), -1.0, F32)
    )
    for t in range(TILES):
        wanted = jnp.where(lane == t, coords[2, t].astype(F32), wanted)
    total = jnp.zeros((R, T), F32)
    for side in range(2):
        rows = gr[:, R : R + 16, :] if side == 0 else other[:, :16, :]
        rows = rows.reshape(NP * 16, T)
        for half in range(2):
            at = 2 * side + half
            chosen = (index[:, at : at + 1] == wanted).astype(F32)
            part = dot(rows, chosen, 0, 0)
            total = total + part[half * R : (half + 1) * R]
    return total


def apply_tile(t, coords, core, az, ao, br, ta, tb, tc, sums):
    a, b, c = ta[t], tb[t], tc[:, t : t + 1]
    da = pick_a(t, coords, core, az, ao)
    db = br[jnp.bitwise_and(coords[1, t], NP - 1)]
    dc = sums[:, t : t + 1]
    left = jnp.concatenate([da, a], axis=0)
    right = jnp.concatenate([b * c, db * c + b * dc], axis=0)
    return dot(left, right, 0, 0), a, b, c


def owned(sums):
    lane = lanes((R, T))
    return jnp.where((lane >= 8) & (lane < 16), sums, 0.0)


def middle_body(
    coords, counts, core_ref, start_ref, az, ao, br, gr, other, index, ta, tb, tc, ga, gb,
    keep, send, fb, depth, w, gc,
):
    core = core_ref[0]
    keep[...] = jnp.zeros(keep.shape, F32)
    send[...] = jnp.zeros(send.shape, F32)
    fb[...] = jnp.zeros(fb.shape, F32)
    sums = depth_sums(coords, start_ref[0], gr, other, index)
    mine = owned(sums)
    gc[...] = mine
    norm = jnp.sum(ga[...] * ga[...] + gb[...] * gb[...] + mine * mine)
    curve = jnp.zeros((T, T), F32)
    parts = []
    for t in range(TILES):
        product, a, b, c = apply_tile(t, coords, core, az, ao, br, ta, tb, tc, sums)
        v = jnp.where(t < counts[0], product, 0.0)
        w[t] = v
        curve = curve + v * v
        grad_a, grad_b, part = transposed_tile(v, a, b, c)
        scatter_tile(t, coords, core, grad_a, grad_b, keep, send, fb)
        parts.append(part)
    row, lane = rows_of((8, T)), lanes((8, T))
    out = depth_rows(parts)
    out = jnp.where((row == 2) & (lane == 0), norm, out)
    depth[...] = jnp.where((row == 2) & (lane == 1), jnp.sum(curve), out)


def both_norms(gr, other):
    total = jnp.sum(gr[:, R + 16 : R + 24, :], axis=0) + jnp.sum(other[:, 16:24, :], axis=0)
    row, lane = rows_of((8, T)), lanes((8, T))
    norm = jnp.sum(jnp.where((row == 2) & (lane == 0), total, 0.0))
    curve = jnp.sum(jnp.where((row == 2) & (lane == 1), total, 0.0))
    return norm, curve


def last_body(
    coords, counts, core_ref, start_ref, az, ao, br, gr, other, index, ta, tb, tc, w,
    ga0, gb0, gc0, ga1, gb1, ha, hb, hc, out,
):
    core = core_ref[0]
    norm, curve = both_norms(gr, other)
    mu = jnp.full((1, 1), curve, F32) / jnp.full((1, 1), norm, F32)
    sums = depth_sums(coords, start_ref[0], gr, other, index)
    a_rest = ga1[...] - mu * ga0[...]
    b_rest = gb1[...] - mu * gb0[...]
    c_rest = owned(sums) - mu * gc0[...]
    ha[...] = a_rest
    hb[...] = b_rest
    hc[...] = c_rest
    rest = jnp.sum(a_rest * a_rest + b_rest * b_rest + c_rest * c_rest)
    bend = jnp.zeros((T, T), F32)
    for t in range(TILES):
        product, _, _, _ = apply_tile(t, coords, core, az, ao, br, ta, tb, tc, sums)
        v = jnp.where(t < counts[0], product, 0.0) - mu * w[t]
        bend = bend + v * v
    row, lane = rows_of((8, T)), lanes((8, T))
    put = jnp.where((row == 0) & (lane == 0), rest, 0.0)
    put = jnp.where((row == 0) & (lane == 1), jnp.sum(bend), put)
    put = jnp.where((row == 0) & (lane == 2), norm, put)
    out[...] = jnp.where((row == 0) & (lane == 3), curve, put)


def end_body(damping, sums, own, ga0, gb0, gc0, ha, hb, hc, oa, ob, oc):
    lane = lanes((1, T))

    def scalar(ref, at):
        return jnp.sum(jnp.where(lane == at, ref[:1], 0.0), axis=1, keepdims=True)

    rest, bend = scalar(sums, 0), scalar(sums, 1)
    norm, curve = scalar(own, 2), scalar(own, 3)
    lam = damping[0]
    mu = curve / norm
    nu = 1.0 / (mu + lam)
    ratio = rest / norm
    second = 1.0 / (bend / rest + lam - ratio * nu)
    on_g = nu + second * ratio * nu * nu
    on_h = -second * nu
    oa[...] = on_g * ga0[...] + on_h * ha[...]
    ob[...] = on_g * gb0[...] + on_h * hb[...]
    oc[...] = (on_g * gc0[...] + on_h * hc[...])[:, 8:16]


def along_z(x):
    return lax.all_to_all(x, "z", 0, 0, tiled=True)


def along_row(x):
    return lax.all_to_all(x, ROW, 0, 0, tiled=True)


def swap(x):
    return lax.ppermute(x, "c", [(0, 1), (1, 0)])


def shares(keep, send, fb, depth, extra):
    joined = call(join_body, shaped(NZ, R + 8, T), (keep, swap(send), depth))
    gz = along_z(joined)
    ga, spread_a, payload = call(
        cross_body, (shaped(R, T), shaped(NZ, R, T), shaped(NP, R + 16 + extra, T)), (gz, fb)
    )
    gr = along_row(payload)
    gb, spread_b = call(sum_b_body, (shaped(R, T), shaped(NP, R, T)), (gr,))
    other = swap(gr[:, R:])
    az = along_z(spread_a)
    ao = swap(az)
    br = along_row(spread_b)
    return ga, gb, gr, other, az, ao, br


def per_device(data, coords, counts, fr, fc, fd, damping):
    core = lax.axis_index("c").reshape(1)
    start = (lax.axis_index(ROW_COL) * fd.shape[1]).reshape(1)
    gz = along_z(call(start_body, shaped(NZ, R + 8, T), (coords, fr, fd), 1))
    oz = swap(gz)
    gr = along_row(call(turn_body, shaped(NP, R + 48, T), (gz, fc)))
    orr = swap(gr[:, R:])
    folded = (shaped(NZ, R, T), shaped(NZ, R, T), shaped(NP, R, T), shaped(8, T))
    saved = (shaped(TILES, R, T), shaped(TILES, R, T), shaped(R, T), shaped(NP * 16, T))
    keep, send, fb, depth, ta, tb, tc, index = call(
        first_body, folded + saved, (coords, counts, core, gz, oz, gr, orr, data), 3
    )
    ga0, gb0, gr, other, az, ao, br = shares(keep, send, fb, depth, 0)
    keep, send, fb, depth, w, gc0 = call(
        middle_body,
        folded + (shaped(TILES, T, T), shaped(R, T)),
        (coords, counts, core, start, az, ao, br, gr, other, index, ta, tb, tc, ga0, gb0),
        4,
    )
    ga1, gb1, gr, other, az, ao, br = shares(keep, send, fb, depth, 8)
    ha, hb, hc, own = call(
        last_body,
        (shaped(R, T), shaped(R, T), shaped(R, T), shaped(8, T)),
        (coords, counts, core, start, az, ao, br, gr, other, index, ta, tb, tc, w)
        + (ga0, gb0, gc0, ga1, gb1),
        4,
    )
    spread = jnp.broadcast_to(own[None, :1], (256, 1, T))
    sums = jnp.sum(lax.all_to_all(spread, ALL, 0, 0, tiled=True), axis=0)
    return call(
        end_body,
        (shaped(R, T), shaped(R, T), shaped(R, 8)),
        (damping.reshape(1), sums, own, ga0, gb0, gc0, ha, hb, hc),
        1,
    )


def solution(mesh):
    finer = Mesh(mesh.devices.reshape(4, 4, 8, 2), ("y", "x", "z", "c"))
    in_specs = (
        P(ROW_COL, None, None),
        P(None, ROW_COL),
        P(ROW_COL),
        P(None, ROW_COL),
        P(None, COL_ROW),
        P(None, ROW_COL),
        P(),
    )
    out_specs = (P(None, ROW_COL), P(None, COL_ROW), P(None, ROW_COL))
    return jax.shard_map(
        per_device, mesh=finer, in_specs=in_specs, out_specs=out_specs, check_vma=False
    )
```

```python
import jax
import jax.numpy as jnp
from jax import lax
from jax.experimental import pallas as pl
from jax.experimental.pallas import tpu as pltpu
from jax.sharding import Mesh
from jax.sharding import PartitionSpec as P

ROW = ("y", "x")
ALL = ("y", "x", "z", "c")
ROW_COL = ("y", "x", "z", "c")
COL_ROW = ("z", "c", "y", "x")
R = 64
T = 128
TILES = 4
NZ = 8
NP = 16
F32 = jnp.float32
HIGH = lax.Precision.HIGHEST

VMEM = pl.BlockSpec(memory_space=pltpu.VMEM)
SMEM = pl.BlockSpec(memory_space=pltpu.SMEM)


def dot(a, b, ca, cb):
    return lax.dot_general(
        a, b, (((ca,), (cb,)), ((), ())), precision=HIGH, preferred_element_type=F32
    )


def shaped(*shape):
    return jax.ShapeDtypeStruct(shape, F32)


def call(body, outs, ins, scalars=0):
    return pl.pallas_call(
        body,
        out_shape=outs,
        in_specs=[SMEM] * scalars + [VMEM] * (len(ins) - scalars),
        out_specs=jax.tree.map(lambda _: VMEM, outs),
        compiler_params=pltpu.CompilerParams(vmem_limit_bytes=16 * 2**20),
    )(*ins)


def lanes(shape):
    return lax.broadcasted_iota(jnp.int32, shape, len(shape) - 1)


def rows_of(shape):
    return lax.broadcasted_iota(jnp.int32, shape, len(shape) - 2)


def decode(code):
    return code % 2, (code // 2) % 8, (code // 16) % 4, (code // 64) % 4


def start_body(coords, code, fr, fd, out):
    _, z_here, _, _ = decode(code[0])
    eye = (rows_of((8, 8)) == lanes((8, 8))).astype(F32)
    columns = jnp.concatenate([dot(eye, fd[...], 1, 1), jnp.zeros((8, T - R), F32)], axis=1)
    row, lane = rows_of((8, T)), lanes((8, T))
    for t in range(TILES):
        here = (row == 0) & (lane == R + 32 * (t % 2) + t // 2 + 2 * z_here)
        columns = jnp.where(here, coords[2, t].astype(F32), columns)
    a = fr[...]
    for z in range(NZ):
        out[z, :R] = a
        out[z, R : R + 8] = columns


def turn_body(gz, b1, b2, b3, out):
    del b1, b2, b3
    low = jnp.concatenate([gz[z, R : R + 8] for z in range(4)], axis=0)
    high = jnp.concatenate([gz[z, R : R + 8] for z in range(4, 8)], axis=0)
    packed = jnp.where(lanes((32, T)) < R, low, pltpu.roll(high, R, 1))
    index = gz[0, R : R + 8]
    for z in range(1, NZ):
        index = index + gz[z, R : R + 8]
    index = jnp.where(lanes((8, T)) < R, pltpu.roll(index, R, 1), 0.0)
    for p in range(NP):
        out[p, :32] = packed
        out[p, 32:40] = index


def apart(index, code):
    _, _, x, y = decode(code)
    return jnp.bitwise_and(index // 4 - y, 3), jnp.bitwise_and(index % 4 - x, 3)


def back(index, code):
    _, _, x, y = decode(code)
    return jnp.bitwise_and(y - index // 4, 3), jnp.bitwise_and(x - index % 4, 3)


def scatter_tile(t, coords, code, grad_a, grad_b, keep, send, fb):
    block = jnp.bitwise_and(coords[0, t], NP - 1)
    place, other = block // 2, jnp.bitwise_xor(block % 2, code % 2)
    mine = other == 0
    keep[place] += jnp.where(mine, grad_a, 0.0)
    send[place] += jnp.where(mine, 0.0, grad_a)
    down, along = apart(jnp.bitwise_and(coords[1, t], NP - 1), code)
    fb[along * 4 + down] += grad_b


def pick_a(t, coords, code, own, oth):
    block = jnp.bitwise_and(coords[0, t], NP - 1)
    place, other = block // 2, jnp.bitwise_xor(block % 2, code % 2)
    return jnp.where(other == 0, own[place, :R], oth[place, :R])


def pick_b(t, coords, code, stacks):
    down, along = back(jnp.bitwise_and(coords[1, t], NP - 1), code)
    found = stacks[0][along, :R]
    for m in range(1, 4):
        found = jnp.where(down == m, stacks[m][along, :R], found)
    return found


def depth_rows(parts):
    pad = jnp.zeros((6, T), F32)
    first = jnp.concatenate([parts[0], parts[1]], axis=1)
    second = jnp.concatenate([parts[2], parts[3]], axis=1)
    return jnp.concatenate([first, second, pad], axis=0)


def transposed_tile(v, a, b, c):
    raw = dot(b, v, 1, 1)
    grad_b = dot(a * c, v, 1, 0)
    depth = dot(jnp.ones((8, T), F32), a * raw, 1, 1)
    return raw * c, grad_b, depth[:1]


def first_body(
    coords, counts, code_ref, gz, oz, b0, b1, b2, b3, gr, orr, data,
    keep, send, fb, depth, ta, tb, tc, index,
):
    code = code_ref[0]
    core, _, x, y = decode(code)
    keep[...] = jnp.zeros(keep.shape, F32)
    send[...] = jnp.zeros(send.shape, F32)
    fb[...] = jnp.zeros(fb.shape, F32)
    picked = []
    lane_row = lanes((1, T))
    for t in range(TILES):
        k = jnp.bitwise_and(coords[2, t], 2047)
        far, near = k // T, k % T
        q, j = near // 8, near % 8
        z = q // 2
        place = (z % 4) * 8 + j
        own = gr[far, pl.ds(place, 1), :]
        oth = orr[far, pl.ds(place, 1), :]
        row = jnp.where(jnp.bitwise_xor(q % 2, core) == 0, own, oth)
        row = jnp.where(z // 4 == 0, row, pltpu.roll(row, R, 1))
        picked.append(jnp.where(lane_row < R, row, 0.0))
    chosen = jnp.concatenate([*picked, jnp.zeros((T - TILES, T), F32)], axis=0)
    column = chosen.T[:R]
    tc[...] = column
    order = [
        jnp.bitwise_and(y - m, 3) * 4 + jnp.bitwise_and(x - k, 3)
        for m in range(4)
        for k in range(4)
    ]
    mine = jnp.concatenate([gr[p, 32:33, :] for p in order], axis=0)
    theirs = jnp.concatenate([orr[p, 32:33, :] for p in order], axis=0)
    both = mine + pltpu.roll(theirs, 16, 1)
    turned = jnp.concatenate([both, jnp.zeros((T - NP, T), F32)], axis=0).T
    lane = lanes((32, T))
    for j in range(NP):
        low, high = turned[:32, j : j + 1], turned[32:64, j : j + 1]
        index[32 * j : 32 * j + 32] = jnp.where(lane == 0, low, high)
    parts = []
    for t in range(TILES):
        a = pick_a(t, coords, code, gz, oz)
        b = pick_b(t, coords, code, (b0, b1, b2, b3))
        c = column[:, t : t + 1]
        ta[t] = a
        tb[t] = b
        model = dot(a, b * c, 0, 0)
        v = jnp.where(t < counts[0], data[t].astype(F32) - model, 0.0)
        grad_a, grad_b, part = transposed_tile(v, a, b, c)
        scatter_tile(t, coords, code, grad_a, grad_b, keep, send, fb)
        parts.append(part)
    depth[...] = depth_rows(parts)


def join_body(keep, received, depth, out):
    d = depth[...]
    for z in range(NZ):
        out[z, :R] = keep[z] + received[z]
        out[z, R : R + 8] = d


def sum_a_body(gz, ga, rows):
    total = gz[0, :R]
    for z in range(1, NZ):
        total = total + gz[z, :R]
    ga[...] = total
    rows[:16] = jnp.concatenate([gz[z, R : R + 2] for z in range(NZ)], axis=0)
    scalars = gz[0, R : R + 8]
    for z in range(1, NZ):
        scalars = scalars + gz[z, R : R + 8]
    rows[16:24] = scalars


def add_body(s0, s1, s2, s3, out):
    out[...] = s0[...] + s1[...] + s2[...] + s3[...]


def sum_b_body(s0, s1, s2, s3, ga, mine, theirs, gb, spread, out):
    total = s0[0] + s1[...] + s2[...] + s3[...]
    gb[...] = total
    a = ga[...]
    for z in range(NZ):
        spread[z] = a
    out[:R] = total
    out[R : R + 16] = mine[:16]
    out[R + 16 : R + 32] = theirs[:16]
    if out.shape[0] > R + 32:
        out[R + 32 : R + 40] = mine[16:24] + theirs[16:24]


def stack_body(s0, s1, s2, s3, out):
    for k, part in enumerate((s0, s1, s2, s3)):
        out[k] = part[...]


def depth_sums(coords, code, stacks, index):
    lane = lanes((1, T))
    wanted = jnp.where(
        (lane >= 8) & (lane < 16), (code * 8 + lane - 8).astype(F32), jnp.full((1, T), -1.0, F32)
    )
    for t in range(TILES):
        wanted = jnp.where(lane == t, coords[2, t].astype(F32), wanted)
    rows = jnp.concatenate([s[k, R : R + 32] for s in stacks for k in range(4)], axis=0)
    total = jnp.zeros((R, T), F32)
    for half in range(2):
        chosen = (index[:, half : half + 1] == wanted).astype(F32)
        part = dot(rows, chosen, 0, 0)
        total = total + part[half * R : (half + 1) * R]
    return total


def apply_tile(t, coords, code, az, ao, stacks, ta, tb, tc, sums):
    a, b, c = ta[t], tb[t], tc[:, t : t + 1]
    da = pick_a(t, coords, code, az, ao)
    db = pick_b(t, coords, code, stacks)
    dc = sums[:, t : t + 1]
    left = jnp.concatenate([da, a], axis=0)
    right = jnp.concatenate([b * c, db * c + b * dc], axis=0)
    return dot(left, right, 0, 0), a, b, c


def owned(sums):
    lane = lanes((R, T))
    return jnp.where((lane >= 8) & (lane < 16), sums, 0.0)


def middle_body(
    coords, counts, code_ref, az, ao, b0, b1, b2, b3, index, ta, tb, tc, ga, gb,
    keep, send, fb, depth, w, gc,
):
    code, stacks = code_ref[0], (b0, b1, b2, b3)
    keep[...] = jnp.zeros(keep.shape, F32)
    send[...] = jnp.zeros(send.shape, F32)
    fb[...] = jnp.zeros(fb.shape, F32)
    sums = depth_sums(coords, code, stacks, index)
    mine = owned(sums)
    gc[...] = mine
    norm = jnp.sum(ga[...] * ga[...] + gb[...] * gb[...] + mine * mine)
    curve = jnp.zeros((T, T), F32)
    parts = []
    for t in range(TILES):
        product, a, b, c = apply_tile(t, coords, code, az, ao, stacks, ta, tb, tc, sums)
        v = jnp.where(t < counts[0], product, 0.0)
        w[t] = v
        curve = curve + v * v
        grad_a, grad_b, part = transposed_tile(v, a, b, c)
        scatter_tile(t, coords, code, grad_a, grad_b, keep, send, fb)
        parts.append(part)
    row, lane = rows_of((8, T)), lanes((8, T))
    out = depth_rows(parts)
    out = jnp.where((row == 2) & (lane == 0), norm, out)
    depth[...] = jnp.where((row == 2) & (lane == 1), jnp.sum(curve), out)


def both_norms(stacks):
    total = jnp.zeros((8, T), F32)
    for s in stacks:
        total = total + jnp.sum(s[:, R + 32 : R + 40, :], axis=0)
    row, lane = rows_of((8, T)), lanes((8, T))
    norm = jnp.sum(jnp.where((row == 2) & (lane == 0), total, 0.0))
    curve = jnp.sum(jnp.where((row == 2) & (lane == 1), total, 0.0))
    return norm, curve


def last_body(
    coords, counts, code_ref, az, ao, b0, b1, b2, b3, index, ta, tb, tc, w,
    ga0, gb0, gc0, ga1, gb1, ha, hb, hc, out,
):
    code, stacks = code_ref[0], (b0, b1, b2, b3)
    norm, curve = both_norms(stacks)
    mu = jnp.full((1, 1), curve, F32) / jnp.full((1, 1), norm, F32)
    sums = depth_sums(coords, code, stacks, index)
    a_rest = ga1[...] - mu * ga0[...]
    b_rest = gb1[...] - mu * gb0[...]
    c_rest = owned(sums) - mu * gc0[...]
    ha[...] = a_rest
    hb[...] = b_rest
    hc[...] = c_rest
    rest = jnp.sum(a_rest * a_rest + b_rest * b_rest + c_rest * c_rest)
    bend = jnp.zeros((T, T), F32)
    for t in range(TILES):
        product, _, _, _ = apply_tile(t, coords, code, az, ao, stacks, ta, tb, tc, sums)
        v = jnp.where(t < counts[0], product, 0.0) - mu * w[t]
        bend = bend + v * v
    row, lane = rows_of((8, T)), lanes((8, T))
    put = jnp.where((row == 0) & (lane == 0), rest, 0.0)
    put = jnp.where((row == 0) & (lane == 1), jnp.sum(bend), put)
    put = jnp.where((row == 0) & (lane == 2), norm, put)
    out[...] = jnp.where((row == 0) & (lane == 3), curve, put)


def end_body(damping, sums, own, ga0, gb0, gc0, ha, hb, hc, oa, ob, oc):
    lane = lanes((1, T))

    def scalar(ref, at):
        return jnp.sum(jnp.where(lane == at, ref[:1], 0.0), axis=1, keepdims=True)

    rest, bend = scalar(sums, 0), scalar(sums, 1)
    norm, curve = scalar(own, 2), scalar(own, 3)
    lam = damping[0]
    mu = curve / norm
    nu = 1.0 / (mu + lam)
    ratio = rest / norm
    second = 1.0 / (bend / rest + lam - ratio * nu)
    on_g = nu + second * ratio * nu * nu
    on_h = -second * nu
    oa[...] = on_g * ga0[...] + on_h * ha[...]
    ob[...] = on_g * gb0[...] + on_h * hb[...]
    oc[...] = (on_g * gc0[...] + on_h * hc[...])[:, 8:16]


def along_z(x):
    return lax.all_to_all(x, "z", 0, 0, tiled=True)


def along_row(x):
    return lax.all_to_all(x, ROW, 0, 0, tiled=True)


def swap(x):
    return lax.ppermute(x, "c", [(0, 1), (1, 0)])


def shift(x, axis, k):
    return lax.ppermute(x, axis, [(i, (i + k) % 4) for i in range(4)])


def row_gather(x):
    near = (x, *(shift(x, "x", k) for k in range(1, 4)))
    stack = call(stack_body, shaped(4, *x.shape), near)
    return (stack, *(shift(stack, "y", m) for m in range(1, 4)))


def row_shares(fb):
    near = (fb[:4], *(shift(fb[4 * k : 4 * k + 4], "x", k) for k in range(1, 4)))
    total = call(add_body, shaped(4, R, T), near)
    return (total, *(shift(total[m], "y", m) for m in range(1, 4)))


def shares(keep, send, fb, depth, extra):
    joined = call(join_body, shaped(NZ, R + 8, T), (keep, swap(send), depth))
    gz = along_z(joined)
    near = row_shares(fb)
    ga, rows = call(sum_a_body, (shaped(R, T), shaped(24, T)), (gz,))
    gb, spread, payload = call(
        sum_b_body,
        (shaped(R, T), shaped(NZ, R, T), shaped(R + 32 + extra, T)),
        (*near, ga, rows, swap(rows)),
    )
    az = along_z(spread)
    return ga, gb, (az, swap(az), *row_gather(payload))


def per_device(data, coords, counts, fr, fc, fd, damping):
    code = lax.axis_index(ROW_COL).reshape(1)
    gz = along_z(call(start_body, shaped(NZ, R + 8, T), (coords, code, fr, fd), 2))
    stacks = row_gather(fc)
    gr = along_row(call(turn_body, shaped(NP, 40, T), (gz, *stacks[1:])))
    folded = (shaped(NZ, R, T), shaped(NZ, R, T), shaped(NP, R, T), shaped(8, T))
    saved = (shaped(TILES, R, T), shaped(TILES, R, T), shaped(R, T), shaped(NP * 32, T))
    keep, send, fb, depth, ta, tb, tc, index = call(
        first_body,
        folded + saved,
        (coords, counts, code, gz, swap(gz), *stacks, gr, swap(gr), data),
        3,
    )
    ga0, gb0, gathered = shares(keep, send, fb, depth, 0)
    keep, send, fb, depth, w, gc0 = call(
        middle_body,
        folded + (shaped(TILES, T, T), shaped(R, T)),
        (coords, counts, code, *gathered, index, ta, tb, tc, ga0, gb0),
        3,
    )
    ga1, gb1, gathered = shares(keep, send, fb, depth, 8)
    ha, hb, hc, own = call(
        last_body,
        (shaped(R, T), shaped(R, T), shaped(R, T), shaped(8, T)),
        (coords, counts, code, *gathered, index, ta, tb, tc, w, ga0, gb0, gc0, ga1, gb1),
        3,
    )
    spread = jnp.broadcast_to(own[None, :1], (256, 1, T))
    sums = jnp.sum(lax.all_to_all(spread, ALL, 0, 0, tiled=True), axis=0)
    return call(
        end_body,
        (shaped(R, T), shaped(R, T), shaped(R, 8)),
        (damping.reshape(1), sums, own, ga0, gb0, gc0, ha, hb, hc),
        1,
    )


def solution(mesh):
    finer = Mesh(mesh.devices.reshape(4, 4, 8, 2), ("y", "x", "z", "c"))
    in_specs = (
        P(ROW_COL, None, None),
        P(None, ROW_COL),
        P(ROW_COL),
        P(None, ROW_COL),
        P(None, COL_ROW),
        P(None, ROW_COL),
        P(),
    )
    out_specs = (P(None, ROW_COL), P(None, COL_ROW), P(None, ROW_COL))
    return jax.shard_map(
        per_device, mesh=finer, in_specs=in_specs, out_specs=out_specs, check_vma=False
    )
```

```python
import jax
import jax.numpy as jnp
from jax import lax
from jax.experimental import pallas as pl
from jax.experimental.pallas import tpu as pltpu
from jax.sharding import Mesh
from jax.sharding import PartitionSpec as P

ROW = ("y", "x")
ALL = ("y", "x", "z", "c")
ROW_COL = ("y", "x", "z", "c")
COL_ROW = ("z", "c", "y", "x")
R = 64
T = 128
TILES = 4
NZ = 8
NP = 16
F32 = jnp.float32
HIGH = lax.Precision.HIGHEST

VMEM = pl.BlockSpec(memory_space=pltpu.VMEM)
SMEM = pl.BlockSpec(memory_space=pltpu.SMEM)


def dot(a, b, ca, cb):
    return lax.dot_general(
        a, b, (((ca,), (cb,)), ((), ())), precision=HIGH, preferred_element_type=F32
    )


def shaped(*shape):
    return jax.ShapeDtypeStruct(shape, F32)


def call(body, outs, ins, scalars=0):
    return pl.pallas_call(
        body,
        out_shape=outs,
        in_specs=[SMEM] * scalars + [VMEM] * (len(ins) - scalars),
        out_specs=jax.tree.map(lambda _: VMEM, outs),
        compiler_params=pltpu.CompilerParams(vmem_limit_bytes=16 * 2**20),
    )(*ins)


def lanes(shape):
    return lax.broadcasted_iota(jnp.int32, shape, len(shape) - 1)


def rows_of(shape):
    return lax.broadcasted_iota(jnp.int32, shape, len(shape) - 2)


def decode(code):
    return code % 2, (code // 2) % 8, (code // 16) % 4, (code // 64) % 4


def start_body(coords, code, fr, fd, out):
    _, z_here, _, _ = decode(code[0])
    columns = jnp.concatenate([fd[...], jnp.zeros((8, T - R), F32)], axis=1)
    row, lane = rows_of((8, T)), lanes((8, T))
    for t in range(TILES):
        here = (row == 0) & (lane == R + 32 * (t % 2) + t // 2 + 2 * z_here)
        columns = jnp.where(here, coords[2, t].astype(F32), columns)
    a = fr[...]
    for z in range(NZ):
        out[z, :R] = a
        out[z, R : R + 8] = columns


def turn_body(gz, b0, b1, b2, b3, out, stack):
    for k, part in enumerate((b0, b1, b2, b3)):
        stack[k] = part[...]
    low = jnp.concatenate([gz[z, R : R + 8] for z in range(4)], axis=0)
    high = jnp.concatenate([gz[z, R : R + 8] for z in range(4, 8)], axis=0)
    packed = jnp.where(lanes((32, T)) < R, low, pltpu.roll(high, R, 1))
    index = gz[0, R : R + 8]
    for z in range(1, NZ):
        index = index + gz[z, R : R + 8]
    index = jnp.where(lanes((8, T)) < R, pltpu.roll(index, R, 1), 0.0)
    for p in range(NP):
        out[p, :32] = packed
        out[p, 32:40] = index


def apart(index, code):
    _, _, x, y = decode(code)
    return jnp.bitwise_and(index // 4 - y, 3), jnp.bitwise_and(index % 4 - x, 3)


def back(index, code):
    _, _, x, y = decode(code)
    return jnp.bitwise_and(y - index // 4, 3), jnp.bitwise_and(x - index % 4, 3)


def scatter_tile(t, coords, code, grad_a, grad_b, keep, send, fb):
    block = jnp.bitwise_and(coords[0, t], NP - 1)
    place, other = block // 2, jnp.bitwise_xor(block % 2, code % 2)
    mine = other == 0
    keep[place] += jnp.where(mine, grad_a, 0.0)
    send[place] += jnp.where(mine, 0.0, grad_a)
    down, along = apart(jnp.bitwise_and(coords[1, t], NP - 1), code)
    fb[along * 4 + down] += grad_b


def pick_a(t, coords, code, own, oth):
    block = jnp.bitwise_and(coords[0, t], NP - 1)
    place, other = block // 2, jnp.bitwise_xor(block % 2, code % 2)
    return jnp.where(other == 0, own[place, :R], oth[place, :R])


def pick_b(t, coords, code, stacks):
    down, along = back(jnp.bitwise_and(coords[1, t], NP - 1), code)
    found = stacks[0][along, :R]
    for m in range(1, 4):
        found = jnp.where(down == m, stacks[m][along, :R], found)
    return found


def depth_rows(parts):
    pad = jnp.zeros((6, T), F32)
    first = jnp.concatenate([parts[0], parts[1]], axis=1)
    second = jnp.concatenate([parts[2], parts[3]], axis=1)
    return jnp.concatenate([first, second, pad], axis=0)


def transposed_tile(v, a, b, c):
    raw = dot(b, v, 1, 1)
    grad_b = dot(a * c, v, 1, 0)
    depth = dot(jnp.ones((8, T), F32), a * raw, 1, 1)
    return raw * c, grad_b, depth[:1]


def first_body(
    coords, counts, code_ref, gz, oz, b0, b1, b2, b3, gr, orr, data,
    keep, send, fb, depth, ta, tb, tc, index,
):
    code = code_ref[0]
    core = code % 2
    keep[...] = jnp.zeros(keep.shape, F32)
    send[...] = jnp.zeros(send.shape, F32)
    fb[...] = jnp.zeros(fb.shape, F32)
    picked = []
    lane_row = lanes((1, T))
    for t in range(TILES):
        k = jnp.bitwise_and(coords[2, t], 2047)
        far, near = k // T, k % T
        q, j = near // 8, near % 8
        z = q // 2
        place = (z % 4) * 8 + j
        own = gr[far, pl.ds(place, 1), :]
        oth = orr[far, pl.ds(place, 1), :]
        row = jnp.where(jnp.bitwise_xor(q % 2, core) == 0, own, oth)
        row = jnp.where(z // 4 == 0, row, pltpu.roll(row, R, 1))
        picked.append(jnp.where(lane_row < R, row, 0.0))
    chosen = jnp.concatenate([*picked, jnp.zeros((T - TILES, T), F32)], axis=0)
    column = chosen.T[:R]
    tc[...] = column
    mine = jnp.concatenate([gr[p, 32:33, :] for p in range(NP)], axis=0)
    theirs = jnp.concatenate([orr[p, 32:33, :] for p in range(NP)], axis=0)
    both = mine + pltpu.roll(theirs, 16, 1)
    turned = jnp.concatenate([both, jnp.zeros((T - NP, T), F32)], axis=0).T
    lane = lanes((32, T))
    for j in range(NP):
        low, high = turned[:32, j : j + 1], turned[32:64, j : j + 1]
        index[32 * j : 32 * j + 32] = jnp.where(lane == 0, low, high)
    parts = []
    for t in range(TILES):
        a = pick_a(t, coords, code, gz, oz)
        b = pick_b(t, coords, code, (b0, b1, b2, b3))
        c = column[:, t : t + 1]
        ta[t] = a
        tb[t] = b
        model = dot(a, b * c, 0, 0)
        v = jnp.where(t < counts[0], data[t].astype(F32) - model, 0.0)
        grad_a, grad_b, part = transposed_tile(v, a, b, c)
        scatter_tile(t, coords, code, grad_a, grad_b, keep, send, fb)
        parts.append(part)
    depth[...] = depth_rows(parts)


def join_body(keep, received, depth, out):
    d = depth[...]
    for z in range(NZ):
        out[z, :R] = keep[z] + received[z]
        out[z, R : R + 8] = d


def sum_a_body(gz, s0, s1, s2, s3, ga, spread, rows, near):
    total = gz[0, :R]
    for z in range(1, NZ):
        total = total + gz[z, :R]
    ga[...] = total
    for z in range(NZ):
        spread[z] = total
    rows[:16] = jnp.concatenate([gz[z, R : R + 2] for z in range(NZ)], axis=0)
    scalars = gz[0, R : R + 8]
    for z in range(1, NZ):
        scalars = scalars + gz[z, R : R + 8]
    rows[16:24] = scalars
    near[...] = s0[:4] + s1[...] + s2[...] + s3[...]


def sum_b_body(s0, s1, s2, s3, mine, theirs, gb, out):
    total = s0[0] + s1[...] + s2[...] + s3[...]
    gb[...] = total
    a, b = mine[:16], theirs[:16]
    scalars = mine[16:24] + theirs[16:24]
    for p in range(NP):
        out[p, :R] = total
        out[p, R : R + 16] = a
        out[p, R + 16 : R + 32] = b
        if out.shape[1] > R + 32:
            out[p, R + 32 : R + 40] = scalars


def depth_sums(coords, code, br, index):
    lane = lanes((1, T))
    wanted = jnp.where(
        (lane >= 8) & (lane < 16), (code * 8 + lane - 8).astype(F32), jnp.full((1, T), -1.0, F32)
    )
    for t in range(TILES):
        wanted = jnp.where(lane == t, coords[2, t].astype(F32), wanted)
    rows = br[:, R : R + 32, :].reshape(NP * 32, T)
    total = jnp.zeros((R, T), F32)
    for half in range(2):
        chosen = (index[:, half : half + 1] == wanted).astype(F32)
        part = dot(rows, chosen, 0, 0)
        total = total + part[half * R : (half + 1) * R]
    return total


def apply_tile(t, coords, code, az, ao, br, ta, tb, tc, sums):
    a, b, c = ta[t], tb[t], tc[:, t : t + 1]
    da = pick_a(t, coords, code, az, ao)
    db = br[jnp.bitwise_and(coords[1, t], NP - 1), :R]
    dc = sums[:, t : t + 1]
    left = jnp.concatenate([da, a], axis=0)
    right = jnp.concatenate([b * c, db * c + b * dc], axis=0)
    return dot(left, right, 0, 0), a, b, c


def owned(sums):
    lane = lanes((R, T))
    return jnp.where((lane >= 8) & (lane < 16), sums, 0.0)


def middle_body(
    coords, counts, code_ref, az, ao, br, index, ta, tb, tc, ga, gb,
    keep, send, fb, depth, w, gc,
):
    code = code_ref[0]
    keep[...] = jnp.zeros(keep.shape, F32)
    send[...] = jnp.zeros(send.shape, F32)
    fb[...] = jnp.zeros(fb.shape, F32)
    sums = depth_sums(coords, code, br, index)
    mine = owned(sums)
    gc[...] = mine
    norm = jnp.sum(ga[...] * ga[...] + gb[...] * gb[...] + mine * mine)
    curve = jnp.zeros((T, T), F32)
    parts = []
    for t in range(TILES):
        product, a, b, c = apply_tile(t, coords, code, az, ao, br, ta, tb, tc, sums)
        v = jnp.where(t < counts[0], product, 0.0)
        w[t] = v
        curve = curve + v * v
        grad_a, grad_b, part = transposed_tile(v, a, b, c)
        scatter_tile(t, coords, code, grad_a, grad_b, keep, send, fb)
        parts.append(part)
    row, lane = rows_of((8, T)), lanes((8, T))
    out = depth_rows(parts)
    out = jnp.where((row == 2) & (lane == 0), norm, out)
    depth[...] = jnp.where((row == 2) & (lane == 1), jnp.sum(curve), out)


def both_norms(br):
    total = jnp.sum(br[:, R + 32 : R + 40, :], axis=0)
    row, lane = rows_of((8, T)), lanes((8, T))
    norm = jnp.sum(jnp.where((row == 2) & (lane == 0), total, 0.0))
    curve = jnp.sum(jnp.where((row == 2) & (lane == 1), total, 0.0))
    return norm, curve


def last_body(
    coords, counts, code_ref, az, ao, br, index, ta, tb, tc, w,
    ga0, gb0, gc0, ga1, gb1, ha, hb, hc, out,
):
    code = code_ref[0]
    norm, curve = both_norms(br)
    mu = jnp.full((1, 1), curve, F32) / jnp.full((1, 1), norm, F32)
    sums = depth_sums(coords, code, br, index)
    a_rest = ga1[...] - mu * ga0[...]
    b_rest = gb1[...] - mu * gb0[...]
    c_rest = owned(sums) - mu * gc0[...]
    ha[...] = a_rest
    hb[...] = b_rest
    hc[...] = c_rest
    rest = jnp.sum(a_rest * a_rest + b_rest * b_rest + c_rest * c_rest)
    bend = jnp.zeros((T, T), F32)
    for t in range(TILES):
        product, _, _, _ = apply_tile(t, coords, code, az, ao, br, ta, tb, tc, sums)
        v = jnp.where(t < counts[0], product, 0.0) - mu * w[t]
        bend = bend + v * v
    row, lane = rows_of((8, T)), lanes((8, T))
    put = jnp.where((row == 0) & (lane == 0), rest, 0.0)
    put = jnp.where((row == 0) & (lane == 1), jnp.sum(bend), put)
    put = jnp.where((row == 0) & (lane == 2), norm, put)
    out[...] = jnp.where((row == 0) & (lane == 3), curve, put)


def end_body(damping, sums, own, ga0, gb0, gc0, ha, hb, hc, oa, ob, oc):
    lane = lanes((1, T))

    def scalar(ref, at):
        return jnp.sum(jnp.where(lane == at, ref[:1], 0.0), axis=1, keepdims=True)

    rest, bend = scalar(sums, 0), scalar(sums, 1)
    norm, curve = scalar(own, 2), scalar(own, 3)
    lam = damping[0]
    mu = curve / norm
    nu = 1.0 / (mu + lam)
    ratio = rest / norm
    second = 1.0 / (bend / rest + lam - ratio * nu)
    on_g = nu + second * ratio * nu * nu
    on_h = -second * nu
    oa[...] = on_g * ga0[...] + on_h * ha[...]
    ob[...] = on_g * gb0[...] + on_h * hb[...]
    oc[...] = (on_g * gc0[...] + on_h * hc[...]).T[8:16]


def along_z(x):
    return lax.all_to_all(x, "z", 0, 0, tiled=True)


def along_row(x):
    return lax.all_to_all(x, ROW, 0, 0, tiled=True)


def swap(x):
    return lax.ppermute(x, "c", [(0, 1), (1, 0)])


def shift(x, axis, k):
    return lax.ppermute(x, axis, [(i, (i + k) % 4) for i in range(4)])


def from_near(x, axis):
    return tuple(shift(x, axis, k) for k in range(1, 4))


def shares(keep, send, fb, depth, extra):
    joined = call(join_body, shaped(NZ, R + 8, T), (keep, swap(send), depth))
    gz = along_z(joined)
    beside = tuple(shift(fb[4 * k : 4 * k + 4], "x", k) for k in range(1, 4))
    ga, spread, rows, near = call(
        sum_a_body,
        (shaped(R, T), shaped(NZ, R, T), shaped(24, T), shaped(4, R, T)),
        (gz, fb, *beside),
    )
    az = along_z(spread)
    below = tuple(shift(near[m], "y", m) for m in range(1, 4))
    gb, payload = call(
        sum_b_body,
        (shaped(R, T), shaped(NP, R + 32 + extra, T)),
        (near, *below, rows, swap(rows)),
    )
    return ga, gb, (az, swap(az), along_row(payload))


def per_device(data, coords, counts, fr, fc, fd, damping):
    code = lax.axis_index(ROW_COL).reshape(1)
    gz = along_z(call(start_body, shaped(NZ, R + 8, T), (coords, code, fr, fd.T), 2))
    payload, stack = call(
        turn_body, (shaped(NP, 40, T), shaped(4, R, T)), (gz, fc, *from_near(fc, "x"))
    )
    gr = along_row(payload)
    stacks = (stack, *from_near(stack, "y"))
    folded = (shaped(NZ, R, T), shaped(NZ, R, T), shaped(NP, R, T), shaped(8, T))
    saved = (shaped(TILES, R, T), shaped(TILES, R, T), shaped(R, T), shaped(NP * 32, T))
    keep, send, fb, depth, ta, tb, tc, index = call(
        first_body,
        folded + saved,
        (coords, counts, code, gz, swap(gz), *stacks, gr, swap(gr), data),
        3,
    )
    ga0, gb0, gathered = shares(keep, send, fb, depth, 0)
    keep, send, fb, depth, w, gc0 = call(
        middle_body,
        folded + (shaped(TILES, T, T), shaped(R, T)),
        (coords, counts, code, *gathered, index, ta, tb, tc, ga0, gb0),
        3,
    )
    ga1, gb1, gathered = shares(keep, send, fb, depth, 8)
    ha, hb, hc, own = call(
        last_body,
        (shaped(R, T), shaped(R, T), shaped(R, T), shaped(8, T)),
        (coords, counts, code, *gathered, index, ta, tb, tc, w, ga0, gb0, gc0, ga1, gb1),
        3,
    )
    spread = jnp.broadcast_to(own[None, :1], (256, 1, T))
    sums = jnp.sum(lax.all_to_all(spread, ALL, 0, 0, tiled=True), axis=0)
    step_a, step_b, step_c = call(
        end_body,
        (shaped(R, T), shaped(R, T), shaped(8, R)),
        (damping.reshape(1), sums, own, ga0, gb0, gc0, ha, hb, hc),
        1,
    )
    return step_a, step_b, step_c.T


def solution(mesh):
    finer = Mesh(mesh.devices.reshape(4, 4, 8, 2), ("y", "x", "z", "c"))
    in_specs = (
        P(ROW_COL, None, None),
        P(None, ROW_COL),
        P(ROW_COL),
        P(None, ROW_COL),
        P(None, COL_ROW),
        P(None, ROW_COL),
        P(),
    )
    out_specs = (P(None, ROW_COL), P(None, COL_ROW), P(None, ROW_COL))
    return jax.shard_map(
        per_device, mesh=finer, in_specs=in_specs, out_specs=out_specs, check_vma=False
    )
```

```python
import jax
import jax.numpy as jnp
from jax import lax
from jax.experimental import pallas as pl
from jax.experimental.pallas import tpu as pltpu
from jax.sharding import Mesh
from jax.sharding import PartitionSpec as P

ROW = ("y", "x")
ALL = ("y", "x", "z", "c")
ROW_COL = ("y", "x", "z", "c")
COL_ROW = ("z", "c", "y", "x")
R = 64
T = 128
TILES = 4
NZ = 8
NP = 16
F32 = jnp.float32
HIGH = lax.Precision.HIGHEST

VMEM = pl.BlockSpec(memory_space=pltpu.VMEM)
SMEM = pl.BlockSpec(memory_space=pltpu.SMEM)


def dot(a, b, ca, cb):
    return lax.dot_general(
        a, b, (((ca,), (cb,)), ((), ())), precision=HIGH, preferred_element_type=F32
    )


def shaped(*shape):
    return jax.ShapeDtypeStruct(shape, F32)


def call(body, outs, ins, scalars=0, scratch=()):
    return pl.pallas_call(
        body,
        out_shape=outs,
        in_specs=[SMEM] * scalars + [VMEM] * (len(ins) - scalars),
        out_specs=jax.tree.map(lambda _: VMEM, outs),
        scratch_shapes=scratch,
        compiler_params=pltpu.CompilerParams(vmem_limit_bytes=16 * 2**20),
    )(*ins)


def lanes(shape):
    return lax.broadcasted_iota(jnp.int32, shape, len(shape) - 1)


def rows_of(shape):
    return lax.broadcasted_iota(jnp.int32, shape, len(shape) - 2)


def decode(code):
    return code % 2, (code // 2) % 8, (code // 16) % 4, (code // 64) % 4


def start_body(coords, code, fr, fd, out):
    _, z_here, _, _ = decode(code[0])
    columns = jnp.concatenate([fd[...], jnp.zeros((8, T - R), F32)], axis=1)
    row, lane = rows_of((8, T)), lanes((8, T))
    for t in range(TILES):
        here = (row == 0) & (lane == R + 32 * (t % 2) + t // 2 + 2 * z_here)
        columns = jnp.where(here, coords[2, t].astype(F32), columns)
        here = (row == 1) & (lane == R + t + 4 * z_here)
        columns = jnp.where(here, coords[0, t].astype(F32), columns)
    a = fr[...]
    for z in range(NZ):
        out[z, :R] = a
        out[z, R : R + 8] = columns


def turn_body(gz, b0, b1, b2, b3, out, stack):
    for k, part in enumerate((b0, b1, b2, b3)):
        stack[k] = part[...]
    low = jnp.concatenate([gz[z, R : R + 8] for z in range(4)], axis=0)
    high = jnp.concatenate([gz[z, R : R + 8] for z in range(4, 8)], axis=0)
    packed = jnp.where(lanes((32, T)) < R, low, pltpu.roll(high, R, 1))
    index = gz[0, R : R + 8]
    for z in range(1, NZ):
        index = index + gz[z, R : R + 8]
    index = jnp.where(lanes((8, T)) < R, pltpu.roll(index, R, 1), 0.0)
    for p in range(NP):
        out[p, :32] = packed
        out[p, 32:40] = index


def apart(index, code):
    _, _, x, y = decode(code)
    return jnp.bitwise_and(index // 4 - y, 3), jnp.bitwise_and(index % 4 - x, 3)


def back(index, code):
    _, _, x, y = decode(code)
    return jnp.bitwise_and(y - index // 4, 3), jnp.bitwise_and(x - index % 4, 3)


def scatter_tile(t, coords, code, grad_a, grad_b, payload, fb):
    for z in range(NZ):
        payload[z, R * t : R * t + R] = grad_a
    down, along = apart(jnp.bitwise_and(coords[1, t], NP - 1), code)
    fb[along * 4 + down] += grad_b


def pick_a(t, coords, code, own, oth):
    block = jnp.bitwise_and(coords[0, t], NP - 1)
    place, other = block // 2, jnp.bitwise_xor(block % 2, code % 2)
    return jnp.where(other == 0, own[place, :R], oth[place, :R])


def pick_b(t, coords, code, stacks):
    down, along = back(jnp.bitwise_and(coords[1, t], NP - 1), code)
    found = stacks[0][along, :R]
    for m in range(1, 4):
        found = jnp.where(down == m, stacks[m][along, :R], found)
    return found


def depth_rows(parts):
    pad = jnp.zeros((6, T), F32)
    first = jnp.concatenate([parts[0], parts[1]], axis=1)
    second = jnp.concatenate([parts[2], parts[3]], axis=1)
    return jnp.concatenate([first, second, pad], axis=0)


def transposed_tile(v, a, b, c):
    raw = dot(b, v, 1, 1)
    grad_b = dot(a * c, v, 1, 0)
    depth = dot(jnp.ones((8, T), F32), a * raw, 1, 1)
    return raw * c, grad_b, depth[:1]


def first_body(
    coords, counts, code_ref, gz, oz, b0, b1, b2, b3, gr, orr, data,
    payload, fb, ta, tb, tc, index, blocks,
):
    code = code_ref[0]
    core = code % 2
    fb[...] = jnp.zeros(fb.shape, F32)
    picked = []
    lane_row = lanes((1, T))
    for t in range(TILES):
        k = jnp.bitwise_and(coords[2, t], 2047)
        far, near = k // T, k % T
        q, j = near // 8, near % 8
        z = q // 2
        place = (z % 4) * 8 + j
        own = gr[far, pl.ds(place, 1), :]
        oth = orr[far, pl.ds(place, 1), :]
        row = jnp.where(jnp.bitwise_xor(q % 2, core) == 0, own, oth)
        row = jnp.where(z // 4 == 0, row, pltpu.roll(row, R, 1))
        picked.append(jnp.where(lane_row < R, row, 0.0))
    chosen = jnp.concatenate([*picked, jnp.zeros((T - TILES, T), F32)], axis=0)
    column = chosen.T[:R]
    tc[...] = column
    mine = jnp.concatenate([gr[p, 32:33, :] for p in range(NP)], axis=0)
    theirs = jnp.concatenate([orr[p, 32:33, :] for p in range(NP)], axis=0)
    both = mine + pltpu.roll(theirs, 16, 1)
    turned = jnp.concatenate([both, jnp.zeros((T - NP, T), F32)], axis=0).T
    lane = lanes((16, T))
    for side in range(2):
        for j in range(NP):
            low = turned[16 * side : 16 * side + 16, j : j + 1]
            high = turned[32 + 16 * side : 48 + 16 * side, j : j + 1]
            at = 256 * side + 16 * j
            index[at : at + 16] = jnp.where(lane == 0, low, high)
    here, there = gz[0, R : R + 8], oz[0, R : R + 8]
    for z in range(1, NZ):
        here, there = here + gz[z, R : R + 8], there + oz[z, R : R + 8]
    here, there = pltpu.roll(here, R, 1), pltpu.roll(there, R + 32, 1)
    lane = lanes((8, T))
    here = jnp.where(lane < 32, here, jnp.where(lane < R, there, 0.0))
    blocks[...] = here.astype(jnp.int32)
    parts = []
    for t in range(TILES):
        a = pick_a(t, coords, code, gz, oz)
        b = pick_b(t, coords, code, (b0, b1, b2, b3))
        c = column[:, t : t + 1]
        ta[t] = a
        tb[t] = b
        model = dot(a, b * c, 0, 0)
        v = jnp.where(t < counts[0], data[t].astype(F32) - model, 0.0)
        grad_a, grad_b, part = transposed_tile(v, a, b, c)
        scatter_tile(t, coords, code, grad_a, grad_b, payload, fb)
        parts.append(part)
    rows = depth_rows(parts)
    for z in range(NZ):
        payload[z, 4 * R :] = rows


def add_body(s0, s1, s2, s3, out):
    out[...] = s0[:4] + s1[...] + s2[...] + s3[...]


def sum_b_body(s0, s1, s2, s3, gz, gb, out):
    total = s0[0] + s1[...] + s2[...] + s3[...]
    gb[...] = total
    rows = jnp.concatenate([gz[z, 4 * R : 4 * R + 2] for z in range(NZ)], axis=0)
    scalars = gz[0, 4 * R :]
    for z in range(1, NZ):
        scalars = scalars + gz[z, 4 * R :]
    for p in range(NP):
        out[p, :R] = total
        out[p, R : R + 16] = rows
        if out.shape[1] > R + 16:
            out[p, R + 16 : R + 24] = scalars


def fold_a(blocks, gz, oz, fa):
    fa[...] = jnp.zeros(fa.shape, F32)
    for side, source in enumerate((gz, oz)):
        for z in range(NZ):
            for t in range(TILES):
                block = jnp.bitwise_and(blocks[1, 32 * side + 4 * z + t], NP - 1)
                fa[block] += source[z, R * t : R * t + R]


def depth_sums(coords, code, br, other, index):
    lane = lanes((1, T))
    wanted = jnp.where(
        (lane >= 8) & (lane < 16), (code * 8 + lane - 8).astype(F32), jnp.full((1, T), -1.0, F32)
    )
    for t in range(TILES):
        wanted = jnp.where(lane == t, coords[2, t].astype(F32), wanted)
    rows = jnp.concatenate(
        [br[:, R : R + 16, :].reshape(NP * 16, T), other[:, :16, :].reshape(NP * 16, T)], axis=0
    )
    total = jnp.zeros((R, T), F32)
    for half in range(2):
        chosen = (index[:, half : half + 1] == wanted).astype(F32)
        part = dot(rows, chosen, 0, 0)
        total = total + part[half * R : (half + 1) * R]
    return total


def apply_tile(t, coords, fa, br, ta, tb, tc, sums):
    a, b, c = ta[t], tb[t], tc[:, t : t + 1]
    da = fa[jnp.bitwise_and(coords[0, t], NP - 1)]
    db = br[jnp.bitwise_and(coords[1, t], NP - 1), :R]
    dc = sums[:, t : t + 1]
    left = jnp.concatenate([da, a], axis=0)
    right = jnp.concatenate([b * c, db * c + b * dc], axis=0)
    return dot(left, right, 0, 0), a, b, c


def owned(sums):
    lane = lanes((R, T))
    return jnp.where((lane >= 8) & (lane < 16), sums, 0.0)


def middle_body(
    coords, counts, code_ref, blocks, gz, oz, br, other, index, ta, tb, tc, gb,
    payload, fb, w, ga, gc, fa,
):
    code = code_ref[0]
    fold_a(blocks, gz, oz, fa)
    mine_a = fa[jnp.bitwise_and(code, NP - 1)]
    ga[...] = mine_a
    fb[...] = jnp.zeros(fb.shape, F32)
    sums = depth_sums(coords, code, br, other, index)
    mine = owned(sums)
    gc[...] = mine
    norm = jnp.sum(mine_a * mine_a + gb[...] * gb[...] + mine * mine)
    curve = jnp.zeros((T, T), F32)
    parts = []
    for t in range(TILES):
        product, a, b, c = apply_tile(t, coords, fa, br, ta, tb, tc, sums)
        v = jnp.where(t < counts[0], product, 0.0)
        w[t] = v
        curve = curve + v * v
        grad_a, grad_b, part = transposed_tile(v, a, b, c)
        scatter_tile(t, coords, code, grad_a, grad_b, payload, fb)
        parts.append(part)
    row, lane = rows_of((8, T)), lanes((8, T))
    out = depth_rows(parts)
    out = jnp.where((row == 2) & (lane == 0), norm, out)
    out = jnp.where((row == 2) & (lane == 1), jnp.sum(curve), out)
    for z in range(NZ):
        payload[z, 4 * R :] = out


def both_norms(br, other):
    total = jnp.sum(br[:, R + 16 : R + 24, :] + other[:, 16:24, :], axis=0)
    row, lane = rows_of((8, T)), lanes((8, T))
    norm = jnp.sum(jnp.where((row == 2) & (lane == 0), total, 0.0))
    curve = jnp.sum(jnp.where((row == 2) & (lane == 1), total, 0.0))
    return norm, curve


def last_body(
    coords, counts, code_ref, blocks, gz, oz, br, other, index, ta, tb, tc, w,
    ga0, gb0, gc0, gb1, ha, hb, hc, out, fa,
):
    code = code_ref[0]
    fold_a(blocks, gz, oz, fa)
    norm, curve = both_norms(br, other)
    mu = jnp.full((1, 1), curve, F32) / jnp.full((1, 1), norm, F32)
    sums = depth_sums(coords, code, br, other, index)
    a_rest = fa[jnp.bitwise_and(code, NP - 1)] - mu * ga0[...]
    b_rest = gb1[...] - mu * gb0[...]
    c_rest = owned(sums) - mu * gc0[...]
    ha[...] = a_rest
    hb[...] = b_rest
    hc[...] = c_rest
    rest = jnp.sum(a_rest * a_rest + b_rest * b_rest + c_rest * c_rest)
    bend = jnp.zeros((T, T), F32)
    for t in range(TILES):
        product, _, _, _ = apply_tile(t, coords, fa, br, ta, tb, tc, sums)
        v = jnp.where(t < counts[0], product, 0.0) - mu * w[t]
        bend = bend + v * v
    row, lane = rows_of((8, T)), lanes((8, T))
    put = jnp.where((row == 0) & (lane == 0), rest, 0.0)
    put = jnp.where((row == 0) & (lane == 1), jnp.sum(bend), put)
    put = jnp.where((row == 0) & (lane == 2), norm, put)
    out[...] = jnp.where((row == 0) & (lane == 3), curve, put)


def end_body(damping, sums, own, ga0, gb0, gc0, ha, hb, hc, oa, ob, oc):
    lane = lanes((1, T))

    def scalar(ref, at):
        return jnp.sum(jnp.where(lane == at, ref[:1], 0.0), axis=1, keepdims=True)

    rest, bend = scalar(sums, 0), scalar(sums, 1)
    norm, curve = scalar(own, 2), scalar(own, 3)
    lam = damping[0]
    mu = curve / norm
    nu = 1.0 / (mu + lam)
    ratio = rest / norm
    second = 1.0 / (bend / rest + lam - ratio * nu)
    on_g = nu + second * ratio * nu * nu
    on_h = -second * nu
    oa[...] = on_g * ga0[...] + on_h * ha[...]
    ob[...] = on_g * gb0[...] + on_h * hb[...]
    oc[...] = (on_g * gc0[...] + on_h * hc[...]).T[8:16]


def along_z(x):
    return lax.all_to_all(x, "z", 0, 0, tiled=True)


def along_row(x):
    return lax.all_to_all(x, ROW, 0, 0, tiled=True)


def swap(x):
    return lax.ppermute(x, "c", [(0, 1), (1, 0)])


def shift(x, axis, k):
    return lax.ppermute(x, axis, [(i, (i + k) % 4) for i in range(4)])


def from_near(x, axis):
    return tuple(shift(x, axis, k) for k in range(1, 4))


def shares(payload, fb, extra):
    gz = along_z(payload)
    beside = tuple(shift(fb[4 * k : 4 * k + 4], "x", k) for k in range(1, 4))
    near = call(add_body, shaped(4, R, T), (fb, *beside))
    below = tuple(shift(near[m], "y", m) for m in range(1, 4))
    gz, near, *below = lax.optimization_barrier((gz, near, *below))
    gb, payload = call(
        sum_b_body, (shaped(R, T), shaped(NP, R + 16 + extra, T)), (near, *below, gz)
    )
    br = along_row(payload)
    return gb, (gz, swap(gz), br, swap(br[:, R:]))


def per_device(data, coords, counts, fr, fc, fd, damping):
    code = lax.axis_index(ROW_COL).reshape(1)
    gz = along_z(call(start_body, shaped(NZ, R + 8, T), (coords, code, fr, fd.T), 2))
    payload, stack = call(
        turn_body, (shaped(NP, 40, T), shaped(4, R, T)), (gz, fc, *from_near(fc, "x"))
    )
    gr = along_row(payload)
    gr, *stacks = lax.optimization_barrier((gr, stack, *from_near(stack, "y")))
    folded = (shaped(NZ, 4 * R + 8, T), shaped(NP, R, T))
    saved = (shaped(TILES, R, T), shaped(TILES, R, T), shaped(R, T), shaped(NP * 32, T))
    payload, fb, ta, tb, tc, index, blocks = call(
        first_body,
        folded + saved + (jax.ShapeDtypeStruct((8, T), jnp.int32),),
        (coords, counts, code, gz, swap(gz), *stacks, gr, swap(gr), data),
        3,
    )
    scratch = (pltpu.VMEM((NP, R, T), F32),)
    gb0, gathered = shares(payload, fb, 0)
    payload, fb, w, ga0, gc0 = call(
        middle_body,
        folded + (shaped(TILES, T, T), shaped(R, T), shaped(R, T)),
        (coords, counts, code, blocks, *gathered, index, ta, tb, tc, gb0),
        4,
        scratch,
    )
    gb1, gathered = shares(payload, fb, 8)
    ha, hb, hc, own = call(
        last_body,
        (shaped(R, T), shaped(R, T), shaped(R, T), shaped(8, T)),
        (coords, counts, code, blocks, *gathered, index, ta, tb, tc, w, ga0, gb0, gc0, gb1),
        4,
        scratch,
    )
    spread = jnp.broadcast_to(own[None, :1], (256, 1, T))
    sums = jnp.sum(lax.all_to_all(spread, ALL, 0, 0, tiled=True), axis=0)
    step_a, step_b, step_c = call(
        end_body,
        (shaped(R, T), shaped(R, T), shaped(8, R)),
        (damping.reshape(1), sums, own, ga0, gb0, gc0, ha, hb, hc),
        1,
    )
    return step_a, step_b, step_c.T


def solution(mesh):
    finer = Mesh(mesh.devices.reshape(4, 4, 8, 2), ("y", "x", "z", "c"))
    in_specs = (
        P(ROW_COL, None, None),
        P(None, ROW_COL),
        P(ROW_COL),
        P(None, ROW_COL),
        P(None, COL_ROW),
        P(None, ROW_COL),
        P(),
    )
    out_specs = (P(None, ROW_COL), P(None, COL_ROW), P(None, ROW_COL))
    return jax.shard_map(
        per_device, mesh=finer, in_specs=in_specs, out_specs=out_specs, check_vma=False
    )
```

```python
import functools

import jax
import jax.numpy as jnp
from jax import lax
from jax.experimental import pallas as pl
from jax.experimental.pallas import tpu as pltpu
from jax.sharding import Mesh
from jax.sharding import PartitionSpec as P

ROW = ("y", "x")
ALL = ("y", "x", "z", "c")
ROW_COL = ("y", "x", "z", "c")
COL_ROW = ("z", "c", "y", "x")
R = 64
T = 128
TILES = 4
NZ = 8
NP = 16
F32 = jnp.float32
HIGH = lax.Precision.HIGHEST

VMEM = pl.BlockSpec(memory_space=pltpu.VMEM)
SMEM = pl.BlockSpec(memory_space=pltpu.SMEM)


def dot(a, b, ca, cb):
    return lax.dot_general(
        a, b, (((ca,), (cb,)), ((), ())), precision=HIGH, preferred_element_type=F32
    )


def shaped(*shape):
    return jax.ShapeDtypeStruct(shape, F32)


def call(body, outs, ins, scalars=0, limit=16):
    return pl.pallas_call(
        body,
        out_shape=outs,
        in_specs=[SMEM] * scalars + [VMEM] * (len(ins) - scalars),
        out_specs=jax.tree.map(lambda _: VMEM, outs),
        compiler_params=pltpu.CompilerParams(vmem_limit_bytes=limit * 2**20),
    )(*ins)


def lanes(shape):
    return lax.broadcasted_iota(jnp.int32, shape, len(shape) - 1)


def rows_of(shape):
    return lax.broadcasted_iota(jnp.int32, shape, len(shape) - 2)


def decode(code):
    return code % 2, (code // 2) % 8, (code // 16) % 4, (code // 64) % 4


def start_body(fr, fd, fc, out, near):
    near[...] = fc[...]
    columns = jnp.concatenate([fd[...], jnp.zeros((8, T - R), F32)], axis=1)
    a = fr[...]
    for z in range(NZ):
        out[z, :R] = a
        out[z, R : R + 8] = columns


def turn_body(gz, b0, b1, b2, b3, out, stack):
    for k, part in enumerate((b0, b1, b2, b3)):
        stack[k] = part[...]
    low = jnp.concatenate([gz[z, R : R + 8] for z in range(4)], axis=0)
    high = jnp.concatenate([gz[z, R : R + 8] for z in range(4, 8)], axis=0)
    packed = jnp.where(lanes((32, T)) < R, low, pltpu.roll(high, R, 1))
    for p in range(NP):
        out[p] = packed


def back(index, code):
    _, _, x, y = decode(code)
    return jnp.bitwise_and(y - index // 4, 3), jnp.bitwise_and(x - index % 4, 3)


def pair_place(there, here, sign):
    apart = jnp.bitwise_and(sign * (there // 2 - here // 2), 3)
    return 2 * apart + jnp.bitwise_xor(there % 2, here % 2)


def scatter_tile(t, coords, code, grad_a, grad_b, keep, send, fb):
    core, z_here, _, _ = decode(code)
    block = jnp.bitwise_and(coords[0, t], NP - 1)
    mine = jnp.bitwise_xor(block % 2, core) == 0
    place = pair_place(block // 2, z_here, 1)
    keep[place] += jnp.where(mine, grad_a, 0.0)
    send[place] += jnp.where(mine, 0.0, grad_a)
    fb[jnp.bitwise_and(coords[1, t], NP - 1)] += grad_b


def pick_a(t, coords, code, own, oth):
    block = jnp.bitwise_and(coords[0, t], NP - 1)
    place, other = block // 2, jnp.bitwise_xor(block % 2, code % 2)
    return jnp.where(other == 0, own[place, :R], oth[place, :R])


def pick_pair(t, coords, code, own, oth):
    core, z_here, _, _ = decode(code)
    block = jnp.bitwise_and(coords[0, t], NP - 1)
    place = pair_place(block // 2, z_here, -1)
    return jnp.where(jnp.bitwise_xor(block % 2, core) == 0, own[place], oth[place])


def pick_b(t, coords, code, stacks):
    down, along = back(jnp.bitwise_and(coords[1, t], NP - 1), code)
    found = stacks[0][along, :R]
    for m in range(1, 4):
        found = jnp.where(down == m, stacks[m][along, :R], found)
    return found


def depth_rows(parts):
    pad = jnp.zeros((6, T), F32)
    first = jnp.concatenate([parts[0], parts[1]], axis=1)
    second = jnp.concatenate([parts[2], parts[3]], axis=1)
    return jnp.concatenate([first, second, pad], axis=0)


def transposed_tile(v, a, b, c):
    raw = dot(b, v, 1, 1)
    grad_b = dot(a * c, v, 1, 0)
    depth = dot(jnp.ones((8, T), F32), a * raw, 1, 1)
    return raw * c, grad_b, depth[:1]


def first_body(
    coords, counts, code_ref, gz, oz, b0, b1, b2, b3, gr, orr, data,
    keep, send, fb, ta, tb, tc,
):
    code = code_ref[0]
    core = code % 2
    keep[...] = jnp.zeros(keep.shape, F32)
    send[...] = jnp.zeros(send.shape, F32)
    fb[...] = jnp.zeros(fb.shape, F32)
    picked = []
    lane_row = lanes((1, T))
    for t in range(TILES):
        k = jnp.bitwise_and(coords[2, t], 2047)
        far, near = k // T, k % T
        q, j = near // 8, near % 8
        z = q // 2
        place = (z % 4) * 8 + j
        own = gr[far, pl.ds(place, 1), :]
        oth = orr[far, pl.ds(place, 1), :]
        row = jnp.where(jnp.bitwise_xor(q % 2, core) == 0, own, oth)
        row = jnp.where(z // 4 == 0, row, pltpu.roll(row, R, 1))
        picked.append(jnp.where(lane_row < R, row, 0.0))
    chosen = jnp.concatenate([*picked, jnp.zeros((T - TILES, T), F32)], axis=0)
    column = chosen.T[:R]
    tc[...] = column
    parts = []
    for t in range(TILES):
        a = pick_a(t, coords, code, gz, oz)
        b = pick_b(t, coords, code, (b0, b1, b2, b3))
        c = column[:, t : t + 1]
        ta[t] = a
        tb[t] = b
        model = dot(a, b * c, 0, 0)
        v = jnp.where(t < counts[0], data[t].astype(F32) - model, 0.0)
        grad_a, grad_b, part = transposed_tile(v, a, b, c)
        scatter_tile(t, coords, code, grad_a, grad_b, keep, send, fb)
        parts.append(part)
    rows = depth_rows(parts)
    row, lane = rows_of((8, T)), lanes((8, T))
    for t in range(TILES):
        rows = jnp.where((row == 2) & (lane == t), coords[2, t].astype(F32), rows)
    send[NZ, :8] = rows


def join_body(keep, send, received, out):
    mine, theirs = send[NZ, :8], received[NZ, :8]
    extra = jnp.where(lanes((1, T)) < 4, mine[2:3], pltpu.roll(theirs, 4, 1)[2:3])
    pad = jnp.zeros((2, T), F32)
    rows = jnp.concatenate([mine[:2], theirs[:2], extra, mine[2:3] + theirs[2:3], pad], axis=0)
    for k in range(4):
        out[k, :R] = keep[2 * k] + received[2 * k]
        out[k, R : 2 * R] = keep[2 * k + 1] + received[2 * k + 1]
        out[k, 2 * R :] = rows


def pair_body(s0, s1, s2, s3, mine, away):
    total = s0[0, : 2 * R] + s1[: 2 * R] + s2[: 2 * R] + s3[: 2 * R]
    mine[:R] = total[:R]
    away[:R] = total[R:]
    for k, part in enumerate((s0[0, 2 * R :], s1[2 * R :], s2[2 * R :], s3[2 * R :])):
        mine[R + 8 * k : R + 8 * k + 8] = part
        away[R + 8 * k : R + 8 * k + 8] = part


def sum_body(mine, received, gr, ga, gb, out, *, scalars):
    ga[...] = mine[:R] + received[:R]
    total = gr[0]
    for p in range(1, NP):
        total = total + gr[p]
    gb[...] = total
    blocks = [half[R + 8 * k : R + 8 * k + 8] for half in (mine, received) for k in range(4)]
    rows = jnp.concatenate([b[g : g + 1] for g in range(4) for b in blocks], axis=0)
    extra = jnp.concatenate([b[4:5] for b in blocks], axis=0)
    if scalars:
        extra = blocks[0]
        for b in blocks[1:]:
            extra = extra + b
    for p in range(NP):
        out[p, :R] = total
        out[p, R : R + 32] = rows
        out[p, R + 32 : R + 40] = extra


def couple_body(s0, s1, out):
    out[0] = s0[...]
    out[1] = s1[...]


def line_body(s0, s1, s2, s3, out):
    for k, part in enumerate((s0, s1, s2, s3)):
        out[2 * k : 2 * k + 2] = part[...]


def depth_sums(coords, code, br, index):
    lane = lanes((1, T))
    wanted = jnp.where(
        (lane >= 8) & (lane < 16), (code * 8 + lane - 8).astype(F32), jnp.full((1, T), -1.0, F32)
    )
    for t in range(TILES):
        wanted = jnp.where(lane == t, coords[2, t].astype(F32), wanted)
    rows = br[:, R : R + 32, :].reshape(NP * 32, T)
    total = jnp.zeros((R, T), F32)
    for half in range(2):
        chosen = (index[:, half : half + 1] == wanted).astype(F32)
        part = dot(rows, chosen, 0, 0)
        total = total + part[half * R : (half + 1) * R]
    return total


def apply_tile(t, coords, code, az, ao, br, ta, tb, tc, sums):
    a, b, c = ta[t], tb[t], tc[:, t : t + 1]
    da = pick_pair(t, coords, code, az, ao)
    db = br[jnp.bitwise_and(coords[1, t], NP - 1), :R]
    dc = sums[:, t : t + 1]
    left = jnp.concatenate([da, a], axis=0)
    right = jnp.concatenate([b * c, db * c + b * dc], axis=0)
    return dot(left, right, 0, 0), a, b, c


def owned(sums):
    lane = lanes((R, T))
    return jnp.where((lane >= 8) & (lane < 16), sums, 0.0)


def middle_body(
    coords, counts, code_ref, az, ao, br, ta, tb, tc, ga, gb,
    keep, send, fb, w, gc, index,
):
    code = code_ref[0]
    keep[...] = jnp.zeros(keep.shape, F32)
    send[...] = jnp.zeros(send.shape, F32)
    fb[...] = jnp.zeros(fb.shape, F32)
    lane = lanes((8, T))
    for p in range(NP):
        known = br[p, R + 32 : R + 40]
        for g in range(4):
            low, high = known[:, 2 * g : 2 * g + 1], known[:, 2 * g + 1 : 2 * g + 2]
            index[32 * p + 8 * g : 32 * p + 8 * g + 8] = jnp.where(lane == 0, low, high)
    sums = depth_sums(coords, code, br, index)
    mine = owned(sums)
    gc[...] = mine
    norm = jnp.sum(ga[...] * ga[...] + gb[...] * gb[...] + mine * mine)
    curve = jnp.zeros((T, T), F32)
    parts = []
    for t in range(TILES):
        product, a, b, c = apply_tile(t, coords, code, az, ao, br, ta, tb, tc, sums)
        v = jnp.where(t < counts[0], product, 0.0)
        w[t] = v
        curve = curve + v * v
        grad_a, grad_b, part = transposed_tile(v, a, b, c)
        scatter_tile(t, coords, code, grad_a, grad_b, keep, send, fb)
        parts.append(part)
    row, lane = rows_of((8, T)), lanes((8, T))
    out = depth_rows(parts)
    out = jnp.where((row == 2) & (lane == 0), norm, out)
    send[NZ, :8] = jnp.where((row == 2) & (lane == 1), jnp.sum(curve), out)


def both_norms(br):
    total = jnp.sum(br[:, R + 32 : R + 40, :], axis=0)
    row, lane = rows_of((8, T)), lanes((8, T))
    norm = jnp.sum(jnp.where((row == 5) & (lane == 0), total, 0.0))
    curve = jnp.sum(jnp.where((row == 5) & (lane == 1), total, 0.0))
    return norm, curve


def last_body(
    coords, counts, code_ref, az, ao, br, index, ta, tb, tc, w,
    ga0, gb0, gc0, ga1, gb1, ha, hb, hc, out, spread,
):
    code = code_ref[0]
    norm, curve = both_norms(br)
    mu = jnp.full((1, 1), curve, F32) / jnp.full((1, 1), norm, F32)
    sums = depth_sums(coords, code, br, index)
    a_rest = ga1[...] - mu * ga0[...]
    b_rest = gb1[...] - mu * gb0[...]
    c_rest = owned(sums) - mu * gc0[...]
    ha[...] = a_rest
    hb[...] = b_rest
    hc[...] = c_rest
    rest = jnp.sum(a_rest * a_rest + b_rest * b_rest + c_rest * c_rest)
    bend = jnp.zeros((T, T), F32)
    for t in range(TILES):
        product, _, _, _ = apply_tile(t, coords, code, az, ao, br, ta, tb, tc, sums)
        v = jnp.where(t < counts[0], product, 0.0) - mu * w[t]
        bend = bend + v * v
    row, lane = rows_of((8, T)), lanes((8, T))
    put = jnp.where((row == 0) & (lane == 0), rest, 0.0)
    put = jnp.where((row == 0) & (lane == 1), jnp.sum(bend), put)
    put = jnp.where((row == 0) & (lane == 2), norm, put)
    put = jnp.where((row == 0) & (lane == 3), curve, put)
    out[...] = put
    spread[...] = jnp.broadcast_to(put[:1][None], spread.shape)


def end_body(damping, sums, own, ga0, gb0, gc0, ha, hb, hc, oa, ob, oc):
    lane = lanes((1, T))

    def scalar(ref, at):
        return jnp.sum(jnp.where(lane == at, ref[:1], 0.0), axis=1, keepdims=True)

    rest, bend = scalar(sums, 0), scalar(sums, 1)
    norm, curve = scalar(own, 2), scalar(own, 3)
    lam = damping[0]
    mu = curve / norm
    nu = 1.0 / (mu + lam)
    ratio = rest / norm
    second = 1.0 / (bend / rest + lam - ratio * nu)
    on_g = nu + second * ratio * nu * nu
    on_h = -second * nu
    oa[...] = on_g * ga0[...] + on_h * ha[...]
    ob[...] = on_g * gb0[...] + on_h * hb[...]
    oc[...] = (on_g * gc0[...] + on_h * hc[...]).T[8:16]


def along_z(x):
    return lax.all_to_all(x, "z", 0, 0, tiled=True)


def along_row(x):
    return lax.all_to_all(x, ROW, 0, 0, tiled=True)


def swap(x):
    return lax.ppermute(x, "c", [(0, 1), (1, 0)])


def shift(x, axis, k):
    return lax.ppermute(x, axis, [(i, (i + k) % 4) for i in range(4)])


def from_near(x, axis):
    return tuple(shift(x, axis, k) for k in range(1, 4))


def pair_shift(x, k):
    return lax.ppermute(x, "z", [(i, (i + 2 * k) % 8) for i in range(8)])


def pair_swap(x):
    return lax.ppermute(x, "z", [(i, i ^ 1) for i in range(8)])


def shares(keep, send, fb, scalars):
    gr = along_row(fb)
    joined = call(join_body, shaped(4, 2 * R + 8, T), (keep, send, swap(send)))
    mine, away = call(
        pair_body,
        (shaped(R + 32, T), shaped(R + 32, T)),
        (joined, *(pair_shift(joined[k], k) for k in range(1, 4))),
    )
    ga, gb, payload = call(
        functools.partial(sum_body, scalars=scalars),
        (shaped(R, T), shaped(R, T), shaped(NP, R + 40, T)),
        (mine, pair_swap(away), gr),
    )
    br = along_row(payload)
    couple = call(couple_body, shaped(2, R, T), (ga, pair_swap(ga)))
    az = call(line_body, shaped(NZ, R, T), (couple, *(pair_shift(couple, k) for k in range(1, 4))))
    return ga, gb, (az, swap(az), br)


def per_device(data, coords, counts, fr, fc, fd, damping):
    code = lax.axis_index(ROW_COL).reshape(1)
    first, fc = call(
        start_body, (shaped(NZ, R + 8, T), shaped(R, T)), (fr, fd.T, fc), limit=60
    )
    gz = along_z(first)
    payload, stack = call(
        turn_body, (shaped(NP, 32, T), shaped(4, R, T)), (gz, fc, *from_near(fc, "x"))
    )
    gr = along_row(payload)
    gr, *stacks = lax.optimization_barrier((gr, stack, *from_near(stack, "y")))
    folded = (shaped(NZ, R, T), shaped(NZ + 1, R, T), shaped(NP, R, T))
    saved = (shaped(TILES, R, T), shaped(TILES, R, T), shaped(R, T))
    keep, send, fb, ta, tb, tc = call(
        first_body,
        folded + saved,
        (coords, counts, code, gz, swap(gz), *stacks, gr, swap(gr), data),
        3,
    )
    ga0, gb0, gathered = shares(keep, send, fb, False)
    keep, send, fb, w, gc0, index = call(
        middle_body,
        folded + (shaped(TILES, T, T), shaped(R, T), shaped(NP * 32, T)),
        (coords, counts, code, *gathered, ta, tb, tc, ga0, gb0),
        3,
    )
    ga1, gb1, gathered = shares(keep, send, fb, True)
    ha, hb, hc, own, spread = call(
        last_body,
        (shaped(R, T), shaped(R, T), shaped(R, T), shaped(8, T), shaped(256, 1, T)),
        (coords, counts, code, *gathered, index, ta, tb, tc, w, ga0, gb0, gc0, ga1, gb1),
        3,
    )
    sums = jnp.sum(lax.all_to_all(spread, ALL, 0, 0, tiled=True), axis=0)
    step_a, step_b, step_c = call(
        end_body,
        (shaped(R, T), shaped(R, T), shaped(8, R)),
        (damping.reshape(1), sums, own, ga0, gb0, gc0, ha, hb, hc),
        1,
    )
    return step_a, step_b, step_c.T


def solution(mesh):
    finer = Mesh(mesh.devices.reshape(4, 4, 8, 2), ("y", "x", "z", "c"))
    in_specs = (
        P(ROW_COL, None, None),
        P(None, ROW_COL),
        P(ROW_COL),
        P(None, ROW_COL),
        P(None, COL_ROW),
        P(None, ROW_COL),
        P(),
    )
    out_specs = (P(None, ROW_COL), P(None, COL_ROW), P(None, ROW_COL))
    return jax.shard_map(
        per_device, mesh=finer, in_specs=in_specs, out_specs=out_specs, check_vma=False
    )
```

```python
import functools

import jax
import jax.numpy as jnp
from jax import lax
from jax.experimental import pallas as pl
from jax.experimental.pallas import tpu as pltpu
from jax.sharding import Mesh
from jax.sharding import PartitionSpec as P

ROW = ("y", "x")
ALL = ("y", "x", "z", "c")
ROW_COL = ("y", "x", "z", "c")
COL_ROW = ("z", "c", "y", "x")
R = 64
T = 128
TILES = 4
NZ = 8
NP = 16
F32 = jnp.float32
HIGH = lax.Precision.HIGHEST

VMEM = pl.BlockSpec(memory_space=pltpu.VMEM)
SMEM = pl.BlockSpec(memory_space=pltpu.SMEM)


def dot(a, b, ca, cb):
    return lax.dot_general(
        a, b, (((ca,), (cb,)), ((), ())), precision=HIGH, preferred_element_type=F32
    )


def shaped(*shape):
    return jax.ShapeDtypeStruct(shape, F32)


def call(body, outs, ins, scalars=0, limit=16):
    return pl.pallas_call(
        body,
        out_shape=outs,
        in_specs=[SMEM] * scalars + [VMEM] * (len(ins) - scalars),
        out_specs=jax.tree.map(lambda _: VMEM, outs),
        compiler_params=pltpu.CompilerParams(vmem_limit_bytes=limit * 2**20),
    )(*ins)


def lanes(shape):
    return lax.broadcasted_iota(jnp.int32, shape, len(shape) - 1)


def rows_of(shape):
    return lax.broadcasted_iota(jnp.int32, shape, len(shape) - 2)


def decode(code):
    return code % 2, (code // 2) % 8, (code // 16) % 4, (code // 64) % 4


def start_body(fr, fd, fc, out, near):
    near[...] = fc[...]
    columns = jnp.concatenate([fd[...], jnp.zeros((8, T - R), F32)], axis=1)
    a = fr[...]
    for z in range(NZ):
        out[z, :R] = a
        out[z, R : R + 8] = columns


def turn_body(gz, b0, b1, b2, b3, out, stack):
    for k, part in enumerate((b0, b1, b2, b3)):
        stack[k] = part[...]
    low = jnp.concatenate([gz[z, R : R + 8] for z in range(4)], axis=0)
    high = jnp.concatenate([gz[z, R : R + 8] for z in range(4, 8)], axis=0)
    packed = jnp.where(lanes((32, T)) < R, low, pltpu.roll(high, R, 1))
    for p in range(NP):
        out[p] = packed


def back(index, code):
    _, _, x, y = decode(code)
    return jnp.bitwise_xor(y, index // 4), jnp.bitwise_xor(x, index % 4)


def pair_place(there, here):
    return jnp.bitwise_xor(there, here)


def scatter_tile(t, coords, code, grad_a, grad_b, keep, send, fb):
    core, z_here, _, _ = decode(code)
    block = jnp.bitwise_and(coords[0, t], NP - 1)
    mine = jnp.bitwise_xor(block % 2, core) == 0
    place = pair_place(block // 2, z_here)
    keep[place] += jnp.where(mine, grad_a, 0.0)
    send[place] += jnp.where(mine, 0.0, grad_a)
    fb[jnp.bitwise_and(coords[1, t], NP - 1)] += grad_b


def pick_a(t, coords, code, own, oth):
    block = jnp.bitwise_and(coords[0, t], NP - 1)
    place, other = block // 2, jnp.bitwise_xor(block % 2, code % 2)
    return jnp.where(other == 0, own[place, :R], oth[place, :R])


def pick_pair(t, coords, code, own, oth):
    core, z_here, _, _ = decode(code)
    block = jnp.bitwise_and(coords[0, t], NP - 1)
    place = pair_place(block // 2, z_here)
    return jnp.where(jnp.bitwise_xor(block % 2, core) == 0, own[place], oth[place])


def pick_b(t, coords, code, stacks):
    down, along = back(jnp.bitwise_and(coords[1, t], NP - 1), code)
    found = stacks[0][along, :R]
    for m in range(1, 4):
        found = jnp.where(down == m, stacks[m][along, :R], found)
    return found


def depth_rows(products):
    sums = dot(jnp.ones((8, T), F32), jnp.concatenate(products, axis=0), 1, 1)
    return jnp.concatenate([sums[:1, :T], sums[:1, T:], jnp.zeros((6, T), F32)], axis=0)


def send_back(coords, code, values, rows_a, rows_b, rows_c, keep, send, fb):
    raws = [dot(b, v, 1, 1) for v, b in zip(values, rows_b)]
    grads_b = [dot(a * c, v, 1, 0) for v, a, c in zip(values, rows_a, rows_c)]
    depth = depth_rows([a * raw for a, raw in zip(rows_a, raws)])
    keep[...] = jnp.zeros(keep.shape, F32)
    send[...] = jnp.zeros(send.shape, F32)
    fb[...] = jnp.zeros(fb.shape, F32)
    for t in range(TILES):
        scatter_tile(t, coords, code, raws[t] * rows_c[t], grads_b[t], keep, send, fb)
    return depth


def first_body(
    coords, counts, code_ref, gz, oz, b0, b1, b2, b3, gr, orr, data,
    keep, send, fb, ta, tb, tc,
):
    code = code_ref[0]
    core = code % 2
    picked = []
    lane_row = lanes((1, T))
    for t in range(TILES):
        k = jnp.bitwise_and(coords[2, t], 2047)
        far, near = k // T, k % T
        q, j = near // 8, near % 8
        z = q // 2
        place = (z % 4) * 8 + j
        own = gr[far, pl.ds(place, 1), :]
        oth = orr[far, pl.ds(place, 1), :]
        row = jnp.where(jnp.bitwise_xor(q % 2, core) == 0, own, oth)
        row = jnp.where(z // 4 == 0, row, pltpu.roll(row, R, 1))
        picked.append(jnp.where(lane_row < R, row, 0.0))
    chosen = jnp.concatenate([*picked, jnp.zeros((T - TILES, T), F32)], axis=0)
    column = chosen.T[:R]
    tc[...] = column
    rows_a = [pick_a(t, coords, code, gz, oz) for t in range(TILES)]
    rows_b = [pick_b(t, coords, code, (b0, b1, b2, b3)) for t in range(TILES)]
    rows_c = [column[:, t : t + 1] for t in range(TILES)]
    models = [dot(a, b * c, 0, 0) for a, b, c in zip(rows_a, rows_b, rows_c)]
    values = [
        jnp.where(t < counts[0], data[t].astype(F32) - models[t], 0.0) for t in range(TILES)
    ]
    for t in range(TILES):
        ta[t] = rows_a[t]
        tb[t] = rows_b[t]
    rows = send_back(coords, code, values, rows_a, rows_b, rows_c, keep, send, fb)
    row, lane = rows_of((8, T)), lanes((8, T))
    for t in range(TILES):
        rows = jnp.where((row == 2) & (lane == t), coords[2, t].astype(F32), rows)
    send[NZ, :8] = rows


def join_body(keep, send, received, out):
    mine, theirs = send[NZ, :8], received[NZ, :8]
    extra = jnp.where(lanes((1, T)) < 4, mine[2:3], pltpu.roll(theirs, 4, 1)[2:3])
    pad = jnp.zeros((2, T), F32)
    rows = jnp.concatenate([mine[:2], theirs[:2], extra, mine[2:3] + theirs[2:3], pad], axis=0)
    for k in range(4):
        out[k, :R] = keep[2 * k] + received[2 * k]
        out[k, R : 2 * R] = keep[2 * k + 1] + received[2 * k + 1]
        out[k, 2 * R :] = rows


def pair_body(s0, s1, s2, s3, mine, away):
    total = s0[0, : 2 * R] + s1[: 2 * R] + s2[: 2 * R] + s3[: 2 * R]
    mine[:R] = total[:R]
    away[:R] = total[R:]
    for k, part in enumerate((s0[0, 2 * R :], s1[2 * R :], s2[2 * R :], s3[2 * R :])):
        mine[R + 8 * k : R + 8 * k + 8] = part
        away[R + 8 * k : R + 8 * k + 8] = part


def sum_body(mine, received, gr, ga, gb, out, *, scalars):
    ga[...] = mine[:R] + received[:R]
    total = gr[0]
    for p in range(1, NP):
        total = total + gr[p]
    gb[...] = total
    blocks = [half[R + 8 * k : R + 8 * k + 8] for half in (mine, received) for k in range(4)]
    rows = jnp.concatenate([b[g : g + 1] for g in range(4) for b in blocks], axis=0)
    extra = jnp.concatenate([b[4:5] for b in blocks], axis=0)
    if scalars:
        extra = blocks[0]
        for b in blocks[1:]:
            extra = extra + b
    for p in range(NP):
        out[p, :R] = total
        out[p, R : R + 32] = rows
        out[p, R + 32 : R + 40] = extra


def couple_body(s0, s1, out):
    out[0] = s0[...]
    out[1] = s1[...]


def line_body(s0, s1, s2, s3, out):
    for k, part in enumerate((s0, s1, s2, s3)):
        out[2 * k : 2 * k + 2] = part[...]


def depth_sums(coords, code, br, index):
    lane = lanes((1, T))
    wanted = jnp.where(
        (lane >= 8) & (lane < 16), (code * 8 + lane - 8).astype(F32), jnp.full((1, T), -1.0, F32)
    )
    for t in range(TILES):
        wanted = jnp.where(lane == t, coords[2, t].astype(F32), wanted)
    rows = br[:, R : R + 32, :].reshape(NP * 32, T)
    chosen = jnp.concatenate([index[:, h : h + 1] == wanted for h in range(2)], axis=1)
    part = dot(rows, chosen.astype(F32), 0, 0)
    return part[:R, :T] + part[R:, T:]


def apply_tile(t, coords, code, az, ao, br, ta, tb, tc, sums):
    a, b, c = ta[t], tb[t], tc[:, t : t + 1]
    da = pick_pair(t, coords, code, az, ao)
    db = br[jnp.bitwise_and(coords[1, t], NP - 1), :R]
    dc = sums[:, t : t + 1]
    left = jnp.concatenate([da, a], axis=0)
    right = jnp.concatenate([b * c, db * c + b * dc], axis=0)
    return dot(left, right, 0, 0), a, b, c


def owned(sums):
    lane = lanes((R, T))
    return jnp.where((lane >= 8) & (lane < 16), sums, 0.0)


def middle_body(
    coords, counts, code_ref, az, ao, br, ta, tb, tc, ga, gb,
    keep, send, fb, w, gc, index,
):
    code = code_ref[0]
    lane = lanes((8, T))
    for p in range(NP):
        known = br[p, R + 32 : R + 40]
        for g in range(4):
            low, high = known[:, 2 * g : 2 * g + 1], known[:, 2 * g + 1 : 2 * g + 2]
            index[32 * p + 8 * g : 32 * p + 8 * g + 8] = jnp.where(lane == 0, low, high)
    sums = depth_sums(coords, code, br, index)
    mine = owned(sums)
    gc[...] = mine
    norm = jnp.sum(ga[...] * ga[...] + gb[...] * gb[...] + mine * mine)
    made = [apply_tile(t, coords, code, az, ao, br, ta, tb, tc, sums) for t in range(TILES)]
    values = [jnp.where(t < counts[0], made[t][0], 0.0) for t in range(TILES)]
    rows_a, rows_b, rows_c = ([m[i] for m in made] for i in (1, 2, 3))
    curve = jnp.zeros((T, T), F32)
    for t in range(TILES):
        w[t] = values[t]
        curve = curve + values[t] * values[t]
    out = send_back(coords, code, values, rows_a, rows_b, rows_c, keep, send, fb)
    row, lane = rows_of((8, T)), lanes((8, T))
    out = jnp.where((row == 2) & (lane == 0), norm, out)
    send[NZ, :8] = jnp.where((row == 2) & (lane == 1), jnp.sum(curve), out)


def both_norms(br):
    total = jnp.sum(br[:, R + 32 : R + 40, :], axis=0)
    row, lane = rows_of((8, T)), lanes((8, T))
    norm = jnp.sum(jnp.where((row == 5) & (lane == 0), total, 0.0))
    curve = jnp.sum(jnp.where((row == 5) & (lane == 1), total, 0.0))
    return norm, curve


def last_body(
    coords, counts, code_ref, az, ao, br, index, ta, tb, tc, w,
    ga0, gb0, gc0, ga1, gb1, ha, hb, hc, out, spread,
):
    code = code_ref[0]
    norm, curve = both_norms(br)
    mu = jnp.full((1, 1), curve, F32) / jnp.full((1, 1), norm, F32)
    sums = depth_sums(coords, code, br, index)
    a_rest = ga1[...] - mu * ga0[...]
    b_rest = gb1[...] - mu * gb0[...]
    c_rest = owned(sums) - mu * gc0[...]
    ha[...] = a_rest
    hb[...] = b_rest
    hc[...] = c_rest
    rest = jnp.sum(a_rest * a_rest + b_rest * b_rest + c_rest * c_rest)
    bend = jnp.zeros((T, T), F32)
    for t in range(TILES):
        product, _, _, _ = apply_tile(t, coords, code, az, ao, br, ta, tb, tc, sums)
        v = jnp.where(t < counts[0], product, 0.0) - mu * w[t]
        bend = bend + v * v
    row, lane = rows_of((8, T)), lanes((8, T))
    put = jnp.where((row == 0) & (lane == 0), rest, 0.0)
    put = jnp.where((row == 0) & (lane == 1), jnp.sum(bend), put)
    put = jnp.where((row == 0) & (lane == 2), norm, put)
    put = jnp.where((row == 0) & (lane == 3), curve, put)
    out[...] = put
    spread[...] = jnp.broadcast_to(put[:1][None], spread.shape)


def end_body(damping, sums, own, ga0, gb0, gc0, ha, hb, hc, oa, ob, oc):
    lane = lanes((1, T))

    def scalar(ref, at):
        return jnp.sum(jnp.where(lane == at, ref[:1], 0.0), axis=1, keepdims=True)

    rest, bend = scalar(sums, 0), scalar(sums, 1)
    norm, curve = scalar(own, 2), scalar(own, 3)
    lam = damping[0]
    mu = curve / norm
    nu = 1.0 / (mu + lam)
    ratio = rest / norm
    second = 1.0 / (bend / rest + lam - ratio * nu)
    on_g = nu + second * ratio * nu * nu
    on_h = -second * nu
    oa[...] = on_g * ga0[...] + on_h * ha[...]
    ob[...] = on_g * gb0[...] + on_h * hb[...]
    oc[...] = (on_g * gc0[...] + on_h * hc[...]).T[8:16]


def along_z(x):
    return lax.all_to_all(x, "z", 0, 0, tiled=True)


def along_row(x):
    return lax.all_to_all(x, ROW, 0, 0, tiled=True)


def swap(x):
    return lax.ppermute(x, "c", [(0, 1), (1, 0)])


def shift(x, axis, k):
    return lax.ppermute(x, axis, [(i, i ^ k) for i in range(4)])


def from_near(x, axis):
    return tuple(shift(x, axis, k) for k in range(1, 4))


def pair_shift(x, k):
    return lax.ppermute(x, "z", [(i, i ^ (2 * k)) for i in range(8)])


def pair_swap(x):
    return lax.ppermute(x, "z", [(i, i ^ 1) for i in range(8)])


def shares(keep, send, fb, scalars):
    gr = along_row(fb)
    joined = call(join_body, shaped(4, 2 * R + 8, T), (keep, send, swap(send)))
    mine, away = call(
        pair_body,
        (shaped(R + 32, T), shaped(R + 32, T)),
        (joined, *(pair_shift(joined[k], k) for k in range(1, 4))),
    )
    ga, gb, payload = call(
        functools.partial(sum_body, scalars=scalars),
        (shaped(R, T), shaped(R, T), shaped(NP, R + 40, T)),
        (mine, pair_swap(away), gr),
    )
    br = along_row(payload)
    couple = call(couple_body, shaped(2, R, T), (ga, pair_swap(ga)))
    az = call(line_body, shaped(NZ, R, T), (couple, *(pair_shift(couple, k) for k in range(1, 4))))
    return ga, gb, (az, swap(az), br)


def per_device(data, coords, counts, fr, fc, fd, damping):
    code = lax.axis_index(ROW_COL).reshape(1)
    first, fc = call(
        start_body, (shaped(NZ, R + 8, T), shaped(R, T)), (fr, fd.T, fc), limit=60
    )
    gz = along_z(first)
    payload, stack = call(
        turn_body, (shaped(NP, 32, T), shaped(4, R, T)), (gz, fc, *from_near(fc, "x"))
    )
    gr = along_row(payload)
    gr, *stacks = lax.optimization_barrier((gr, stack, *from_near(stack, "y")))
    folded = (shaped(NZ, R, T), shaped(NZ + 1, R, T), shaped(NP, R, T))
    saved = (shaped(TILES, R, T), shaped(TILES, R, T), shaped(R, T))
    keep, send, fb, ta, tb, tc = call(
        first_body,
        folded + saved,
        (coords, counts, code, gz, swap(gz), *stacks, gr, swap(gr), data),
        3,
    )
    ga0, gb0, gathered = shares(keep, send, fb, False)
    keep, send, fb, w, gc0, index = call(
        middle_body,
        folded + (shaped(TILES, T, T), shaped(R, T), shaped(NP * 32, T)),
        (coords, counts, code, *gathered, ta, tb, tc, ga0, gb0),
        3,
    )
    ga1, gb1, gathered = shares(keep, send, fb, True)
    ha, hb, hc, own, spread = call(
        last_body,
        (shaped(R, T), shaped(R, T), shaped(R, T), shaped(8, T), shaped(256, 1, T)),
        (coords, counts, code, *gathered, index, ta, tb, tc, w, ga0, gb0, gc0, ga1, gb1),
        3,
    )
    sums = jnp.sum(lax.all_to_all(spread, ALL, 0, 0, tiled=True), axis=0)
    step_a, step_b, step_c = call(
        end_body,
        (shaped(R, T), shaped(R, T), shaped(8, R)),
        (damping.reshape(1), sums, own, ga0, gb0, gc0, ha, hb, hc),
        1,
    )
    return step_a, step_b, step_c.T


def solution(mesh):
    finer = Mesh(mesh.devices.reshape(4, 4, 8, 2), ("y", "x", "z", "c"))
    in_specs = (
        P(ROW_COL, None, None),
        P(None, ROW_COL),
        P(ROW_COL),
        P(None, ROW_COL),
        P(None, COL_ROW),
        P(None, ROW_COL),
        P(),
    )
    out_specs = (P(None, ROW_COL), P(None, COL_ROW), P(None, ROW_COL))
    return jax.shard_map(
        per_device, mesh=finer, in_specs=in_specs, out_specs=out_specs, check_vma=False
    )
```

```python
import functools

import jax
import jax.numpy as jnp
from jax import lax
from jax.experimental import pallas as pl
from jax.experimental.pallas import tpu as pltpu
from jax.sharding import Mesh
from jax.sharding import PartitionSpec as P

ROW = ("y", "x")
ALL = ("y", "x", "z", "c")
ROW_COL = ("y", "x", "z", "c")
COL_ROW = ("z", "c", "y", "x")
R = 64
T = 128
TILES = 4
NZ = 8
NP = 16
F32 = jnp.float32
HIGH = lax.Precision.HIGHEST

VMEM = pl.BlockSpec(memory_space=pltpu.VMEM)
SMEM = pl.BlockSpec(memory_space=pltpu.SMEM)


def dot(a, b, ca, cb):
    return lax.dot_general(
        a, b, (((ca,), (cb,)), ((), ())), precision=HIGH, preferred_element_type=F32
    )


def shaped(*shape):
    return jax.ShapeDtypeStruct(shape, F32)


def call(body, outs, ins, scalars=0, limit=16):
    return pl.pallas_call(
        body,
        out_shape=outs,
        in_specs=[SMEM] * scalars + [VMEM] * (len(ins) - scalars),
        out_specs=jax.tree.map(lambda _: VMEM, outs),
        compiler_params=pltpu.CompilerParams(vmem_limit_bytes=limit * 2**20),
    )(*ins)


def lanes(shape):
    return lax.broadcasted_iota(jnp.int32, shape, len(shape) - 1)


def rows_of(shape):
    return lax.broadcasted_iota(jnp.int32, shape, len(shape) - 2)


def decode(code):
    return code % 2, (code // 2) % 8, (code // 16) % 4, (code // 64) % 4


def start_body(fr, fd, fc, out, near):
    near[...] = fc[...]
    columns = jnp.concatenate([fd[...], jnp.zeros((8, T - R), F32)], axis=1)
    a = fr[...]
    for z in range(NZ):
        out[z, :R] = a
        out[z, R : R + 8] = columns


def turn_body(gz, b0, b1, b2, b3, out, stack):
    for k, part in enumerate((b0, b1, b2, b3)):
        stack[k] = part[...]
    low = jnp.concatenate([gz[z, R : R + 8] for z in range(4)], axis=0)
    high = jnp.concatenate([gz[z, R : R + 8] for z in range(4, 8)], axis=0)
    packed = jnp.where(lanes((32, T)) < R, low, pltpu.roll(high, R, 1))
    for p in range(NP):
        out[p] = packed


def back(index, code):
    _, _, x, y = decode(code)
    return jnp.bitwise_xor(y, index // 4), jnp.bitwise_xor(x, index % 4)


def pair_place(there, here):
    return jnp.bitwise_xor(there, here)


def scatter_tile(t, coords, code, grad_a, grad_b, keep, send, fb):
    core, z_here, _, _ = decode(code)
    block = jnp.bitwise_and(coords[0, t], NP - 1)
    mine = jnp.bitwise_xor(block % 2, core) == 0
    place = pair_place(block // 2, z_here)
    keep[place] += jnp.where(mine, grad_a, 0.0)
    send[place] += jnp.where(mine, 0.0, grad_a)
    fb[jnp.bitwise_and(coords[1, t], NP - 1)] += grad_b


def pick_a(t, coords, code, own, oth):
    block = jnp.bitwise_and(coords[0, t], NP - 1)
    place, other = block // 2, jnp.bitwise_xor(block % 2, code % 2)
    return jnp.where(other == 0, own[place, :R], oth[place, :R])


def pick_pair(t, coords, code, own, oth):
    core, z_here, _, _ = decode(code)
    block = jnp.bitwise_and(coords[0, t], NP - 1)
    place = pair_place(block // 2, z_here)
    return jnp.where(jnp.bitwise_xor(block % 2, core) == 0, own[place], oth[place])


def pick_b(t, coords, code, stacks):
    down, along = back(jnp.bitwise_and(coords[1, t], NP - 1), code)
    found = stacks[0][along, :R]
    for m in range(1, 4):
        found = jnp.where(down == m, stacks[m][along, :R], found)
    return found


def depth_rows(products):
    sums = dot(jnp.ones((8, T), F32), jnp.concatenate(products, axis=0), 1, 1)
    return jnp.concatenate([sums[:1, :T], sums[:1, T:], jnp.zeros((6, T), F32)], axis=0)


def send_back(coords, code, values, rows_a, rows_b, rows_c, keep, send, fb):
    raws = [dot(b, v, 1, 1) for v, b in zip(values, rows_b)]
    grads_b = [dot(a * c, v, 1, 0) for v, a, c in zip(values, rows_a, rows_c)]
    depth = depth_rows([a * raw for a, raw in zip(rows_a, raws)])
    keep[...] = jnp.zeros(keep.shape, F32)
    send[...] = jnp.zeros(send.shape, F32)
    fb[...] = jnp.zeros(fb.shape, F32)
    for t in range(TILES):
        scatter_tile(t, coords, code, raws[t] * rows_c[t], grads_b[t], keep, send, fb)
    return depth


def first_body(
    coords, counts, code_ref, gz, oz, b0, b1, b2, b3, gr, orr, data,
    keep, send, fb, ta, tb, tc,
):
    code = code_ref[0]
    core = code % 2
    picked = []
    lane_row = lanes((1, T))
    for t in range(TILES):
        k = jnp.bitwise_and(coords[2, t], 2047)
        far, near = k // T, k % T
        q, j = near // 8, near % 8
        z = q // 2
        place = (z % 4) * 8 + j
        own = gr[far, pl.ds(place, 1), :]
        oth = orr[far, pl.ds(place, 1), :]
        row = jnp.where(jnp.bitwise_xor(q % 2, core) == 0, own, oth)
        row = jnp.where(z // 4 == 0, row, pltpu.roll(row, R, 1))
        picked.append(jnp.where(lane_row < R, row, 0.0))
    chosen = jnp.concatenate([*picked, jnp.zeros((T - TILES, T), F32)], axis=0)
    column = chosen.T[:R]
    tc[...] = column
    rows_a = [pick_a(t, coords, code, gz, oz) for t in range(TILES)]
    rows_b = [pick_b(t, coords, code, (b0, b1, b2, b3)) for t in range(TILES)]
    rows_c = [column[:, t : t + 1] for t in range(TILES)]
    models = [dot(a, b * c, 0, 0) for a, b, c in zip(rows_a, rows_b, rows_c)]
    values = [
        jnp.where(t < counts[0], data[t].astype(F32) - models[t], 0.0) for t in range(TILES)
    ]
    for t in range(TILES):
        ta[t] = rows_a[t]
        tb[t] = rows_b[t]
    rows = send_back(coords, code, values, rows_a, rows_b, rows_c, keep, send, fb)
    row, lane = rows_of((8, T)), lanes((8, T))
    for t in range(TILES):
        rows = jnp.where((row == 2) & (lane == t), coords[2, t].astype(F32), rows)
    send[NZ, :8] = rows


def join_body(keep, send, received, out):
    mine, theirs = send[NZ, :8], received[NZ, :8]
    extra = jnp.where(lanes((1, T)) < 4, mine[2:3], pltpu.roll(theirs, 4, 1)[2:3])
    pad = jnp.zeros((2, T), F32)
    rows = jnp.concatenate([mine[:2], theirs[:2], extra, mine[2:3] + theirs[2:3], pad], axis=0)
    for k in range(4):
        out[k, :R] = keep[2 * k] + received[2 * k]
        out[k, R : 2 * R] = keep[2 * k + 1] + received[2 * k + 1]
        out[k, 2 * R :] = rows


def pair_body(s0, s1, s2, s3, out):
    out[: 2 * R] = s0[0, : 2 * R] + s1[: 2 * R] + s2[: 2 * R] + s3[: 2 * R]
    for k, part in enumerate((s0[0, 2 * R :], s1[2 * R :], s2[2 * R :], s3[2 * R :])):
        out[2 * R + 8 * k : 2 * R + 8 * k + 8] = part


def sum_body(mine, received, gr, ga, gb, couple, out, *, scalars):
    own = mine[:R] + received[R : 2 * R]
    ga[...] = own
    couple[0] = own
    couple[1] = mine[R : 2 * R] + received[:R]
    total = gr[0]
    for p in range(1, NP):
        total = total + gr[p]
    gb[...] = total
    blocks = [half[2 * R + 8 * k : 2 * R + 8 * k + 8] for half in (mine, received) for k in range(4)]
    rows = jnp.concatenate([b[g : g + 1] for g in range(4) for b in blocks], axis=0)
    extra = jnp.concatenate([b[4:5] for b in blocks], axis=0)
    if scalars:
        extra = blocks[0]
        for b in blocks[1:]:
            extra = extra + b
    for p in range(NP):
        out[p, :R] = total
        out[p, R : R + 32] = rows
        out[p, R + 32 : R + 40] = extra


def line_body(s0, s1, s2, s3, out):
    for k, part in enumerate((s0, s1, s2, s3)):
        out[2 * k : 2 * k + 2] = part[...]


def depth_sums(coords, code, br, index):
    lane = lanes((1, T))
    wanted = jnp.where(
        (lane >= 8) & (lane < 16), (code * 8 + lane - 8).astype(F32), jnp.full((1, T), -1.0, F32)
    )
    for t in range(TILES):
        wanted = jnp.where(lane == t, coords[2, t].astype(F32), wanted)
    rows = br[:, R : R + 32, :].reshape(NP * 32, T)
    chosen = jnp.concatenate([index[:, h : h + 1] == wanted for h in range(2)], axis=1)
    part = dot(rows, chosen.astype(F32), 0, 0)
    return part[:R, :T] + part[R:, T:]


def apply_tile(t, coords, code, az, ao, br, ta, tb, tc, sums):
    a, b, c = ta[t], tb[t], tc[:, t : t + 1]
    da = pick_pair(t, coords, code, az, ao)
    db = br[jnp.bitwise_and(coords[1, t], NP - 1), :R]
    dc = sums[:, t : t + 1]
    left = jnp.concatenate([da, a], axis=0)
    right = jnp.concatenate([b * c, db * c + b * dc], axis=0)
    return dot(left, right, 0, 0), a, b, c


def owned(sums):
    lane = lanes((R, T))
    return jnp.where((lane >= 8) & (lane < 16), sums, 0.0)


def middle_body(
    coords, counts, code_ref, az, ao, br, ta, tb, tc, ga, gb,
    keep, send, fb, w, gc, index,
):
    code = code_ref[0]
    lane = lanes((8, T))
    for p in range(NP):
        known = br[p, R + 32 : R + 40]
        for g in range(4):
            low, high = known[:, 2 * g : 2 * g + 1], known[:, 2 * g + 1 : 2 * g + 2]
            index[32 * p + 8 * g : 32 * p + 8 * g + 8] = jnp.where(lane == 0, low, high)
    sums = depth_sums(coords, code, br, index)
    mine = owned(sums)
    gc[...] = mine
    norm = jnp.sum(ga[...] * ga[...] + gb[...] * gb[...] + mine * mine)
    made = [apply_tile(t, coords, code, az, ao, br, ta, tb, tc, sums) for t in range(TILES)]
    values = [jnp.where(t < counts[0], made[t][0], 0.0) for t in range(TILES)]
    rows_a, rows_b, rows_c = ([m[i] for m in made] for i in (1, 2, 3))
    curve = jnp.zeros((T, T), F32)
    for t in range(TILES):
        w[t] = values[t]
        curve = curve + values[t] * values[t]
    out = send_back(coords, code, values, rows_a, rows_b, rows_c, keep, send, fb)
    row, lane = rows_of((8, T)), lanes((8, T))
    out = jnp.where((row == 2) & (lane == 0), norm, out)
    send[NZ, :8] = jnp.where((row == 2) & (lane == 1), jnp.sum(curve), out)


def both_norms(br):
    total = jnp.sum(br[:, R + 32 : R + 40, :], axis=0)
    row, lane = rows_of((8, T)), lanes((8, T))
    norm = jnp.sum(jnp.where((row == 5) & (lane == 0), total, 0.0))
    curve = jnp.sum(jnp.where((row == 5) & (lane == 1), total, 0.0))
    return norm, curve


def last_body(
    coords, counts, code_ref, az, ao, br, index, ta, tb, tc, w,
    ga0, gb0, gc0, ga1, gb1, ha, hb, hc, out, spread,
):
    code = code_ref[0]
    norm, curve = both_norms(br)
    mu = jnp.full((1, 1), curve, F32) / jnp.full((1, 1), norm, F32)
    sums = depth_sums(coords, code, br, index)
    a_rest = ga1[...] - mu * ga0[...]
    b_rest = gb1[...] - mu * gb0[...]
    c_rest = owned(sums) - mu * gc0[...]
    ha[...] = a_rest
    hb[...] = b_rest
    hc[...] = c_rest
    rest = jnp.sum(a_rest * a_rest + b_rest * b_rest + c_rest * c_rest)
    bend = jnp.zeros((T, T), F32)
    for t in range(TILES):
        product, _, _, _ = apply_tile(t, coords, code, az, ao, br, ta, tb, tc, sums)
        v = jnp.where(t < counts[0], product, 0.0) - mu * w[t]
        bend = bend + v * v
    row, lane = rows_of((8, T)), lanes((8, T))
    put = jnp.where((row == 0) & (lane == 0), rest, 0.0)
    put = jnp.where((row == 0) & (lane == 1), jnp.sum(bend), put)
    put = jnp.where((row == 0) & (lane == 2), norm, put)
    put = jnp.where((row == 0) & (lane == 3), curve, put)
    out[...] = put
    spread[...] = jnp.broadcast_to(put[:1][None], spread.shape)


def end_body(damping, sums, own, ga0, gb0, gc0, ha, hb, hc, oa, ob, oc):
    lane = lanes((1, T))

    def scalar(ref, at):
        return jnp.sum(jnp.where(lane == at, ref[:1], 0.0), axis=1, keepdims=True)

    rest, bend = scalar(sums, 0), scalar(sums, 1)
    norm, curve = scalar(own, 2), scalar(own, 3)
    lam = damping[0]
    mu = curve / norm
    nu = 1.0 / (mu + lam)
    ratio = rest / norm
    second = 1.0 / (bend / rest + lam - ratio * nu)
    on_g = nu + second * ratio * nu * nu
    on_h = -second * nu
    oa[...] = on_g * ga0[...] + on_h * ha[...]
    ob[...] = on_g * gb0[...] + on_h * hb[...]
    oc[...] = (on_g * gc0[...] + on_h * hc[...]).T[8:16]


def along_z(x):
    return lax.all_to_all(x, "z", 0, 0, tiled=True)


def along_row(x):
    return lax.all_to_all(x, ROW, 0, 0, tiled=True)


def swap(x):
    return lax.ppermute(x, "c", [(0, 1), (1, 0)])


def shift(x, axis, k):
    return lax.ppermute(x, axis, [(i, i ^ k) for i in range(4)])


def from_near(x, axis):
    return tuple(shift(x, axis, k) for k in range(1, 4))


def pair_shift(x, k):
    return lax.ppermute(x, "z", [(i, i ^ (2 * k)) for i in range(8)])


def pair_swap(x):
    return lax.ppermute(x, "z", [(i, i ^ 1) for i in range(8)])


def shares(keep, send, fb, scalars):
    gr = along_row(fb)
    joined = call(join_body, shaped(4, 2 * R + 8, T), (keep, send, swap(send)))
    mine = call(
        pair_body,
        shaped(2 * R + 32, T),
        (joined, *(pair_shift(joined[k], k) for k in range(1, 4))),
    )
    ga, gb, couple, payload = call(
        functools.partial(sum_body, scalars=scalars),
        (shaped(R, T), shaped(R, T), shaped(2, R, T), shaped(NP, R + 40, T)),
        (mine, pair_swap(mine), gr),
    )
    br = along_row(payload)
    az = call(line_body, shaped(NZ, R, T), (couple, *(pair_shift(couple, k) for k in range(1, 4))))
    return ga, gb, (az, swap(az), br)


def per_device(data, coords, counts, fr, fc, fd, damping):
    code = lax.axis_index(ROW_COL).reshape(1)
    first, fc = call(
        start_body, (shaped(NZ, R + 8, T), shaped(R, T)), (fr, fd.T, fc), limit=60
    )
    gz = along_z(first)
    payload, stack = call(
        turn_body, (shaped(NP, 32, T), shaped(4, R, T)), (gz, fc, *from_near(fc, "x"))
    )
    gr = along_row(payload)
    gr, *stacks = lax.optimization_barrier((gr, stack, *from_near(stack, "y")))
    folded = (shaped(NZ, R, T), shaped(NZ + 1, R, T), shaped(NP, R, T))
    saved = (shaped(TILES, R, T), shaped(TILES, R, T), shaped(R, T))
    keep, send, fb, ta, tb, tc = call(
        first_body,
        folded + saved,
        (coords, counts, code, gz, swap(gz), *stacks, gr, swap(gr), data),
        3,
    )
    ga0, gb0, gathered = shares(keep, send, fb, False)
    keep, send, fb, w, gc0, index = call(
        middle_body,
        folded + (shaped(TILES, T, T), shaped(R, T), shaped(NP * 32, T)),
        (coords, counts, code, *gathered, ta, tb, tc, ga0, gb0),
        3,
    )
    ga1, gb1, gathered = shares(keep, send, fb, True)
    ha, hb, hc, own, spread = call(
        last_body,
        (shaped(R, T), shaped(R, T), shaped(R, T), shaped(8, T), shaped(256, 1, T)),
        (coords, counts, code, *gathered, index, ta, tb, tc, w, ga0, gb0, gc0, ga1, gb1),
        3,
    )
    sums = jnp.sum(lax.all_to_all(spread, ALL, 0, 0, tiled=True), axis=0)
    step_a, step_b, step_c = call(
        end_body,
        (shaped(R, T), shaped(R, T), shaped(8, R)),
        (damping.reshape(1), sums, own, ga0, gb0, gc0, ha, hb, hc),
        1,
    )
    return step_a, step_b, step_c.T


def solution(mesh):
    finer = Mesh(mesh.devices.reshape(4, 4, 8, 2), ("y", "x", "z", "c"))
    in_specs = (
        P(ROW_COL, None, None),
        P(None, ROW_COL),
        P(ROW_COL),
        P(None, ROW_COL),
        P(None, COL_ROW),
        P(None, ROW_COL),
        P(),
    )
    out_specs = (P(None, ROW_COL), P(None, COL_ROW), P(None, ROW_COL))
    return jax.shard_map(
        per_device, mesh=finer, in_specs=in_specs, out_specs=out_specs, check_vma=False
    )
```

```python
import functools

import jax
import jax.numpy as jnp
from jax import lax
from jax.experimental import pallas as pl
from jax.experimental.pallas import tpu as pltpu
from jax.sharding import Mesh
from jax.sharding import PartitionSpec as P


ROW = ("y", "x")
ALL = ("y", "x", "z", "c")
ROW_COL = ("y", "x", "z", "c")
COL_ROW = ("z", "c", "y", "x")
R = 64
T = 128
TILES = 4
NZ = 8
NP = 16
F32 = jnp.float32

VMEM = pl.BlockSpec(memory_space=pltpu.VMEM)
SMEM = pl.BlockSpec(memory_space=pltpu.SMEM)


def halves(a):
    high = a.astype(jnp.bfloat16)
    return high, (a - high.astype(F32)).astype(jnp.bfloat16)


def pass_of(a, b, ca, cb):
    return lax.dot_general(a, b, (((ca,), (cb,)), ((), ())), preferred_element_type=F32)


def dot(a, b, ca, cb):
    (a_high, a_low), (b_high, b_low) = halves(a), halves(b)
    small = pass_of(a_low, b_high, ca, cb) + pass_of(a_high, b_low, ca, cb)
    return small + pass_of(a_high, b_high, ca, cb)


def shaped(*shape):
    return jax.ShapeDtypeStruct(shape, F32)


def call(body, outs, ins, scalars=0, limit=16):
    return pl.pallas_call(
        body,
        out_shape=outs,
        in_specs=[SMEM] * scalars + [VMEM] * (len(ins) - scalars),
        out_specs=jax.tree.map(lambda _: VMEM, outs),
        compiler_params=pltpu.CompilerParams(vmem_limit_bytes=limit * 2**20),
    )(*ins)


def lanes(shape):
    return lax.broadcasted_iota(jnp.int32, shape, len(shape) - 1)


def rows_of(shape):
    return lax.broadcasted_iota(jnp.int32, shape, len(shape) - 2)


def decode(code):
    return code % 2, (code // 2) % 8, (code // 16) % 4, (code // 64) % 4


def start_body(fr, fd, fc, out, near):
    near[...] = fc[...]
    columns = jnp.concatenate([fd[...], jnp.zeros((8, T - R), F32)], axis=1)
    a = fr[...]
    for z in range(NZ):
        out[z, :R] = a
        out[z, R : R + 8] = columns


def turn_body(gz, b0, b1, b2, b3, out, stack):
    for k, part in enumerate((b0, b1, b2, b3)):
        stack[k] = part[...]
    low = jnp.concatenate([gz[z, R : R + 8] for z in range(4)], axis=0)
    high = jnp.concatenate([gz[z, R : R + 8] for z in range(4, 8)], axis=0)
    packed = jnp.where(lanes((32, T)) < R, low, pltpu.roll(high, R, 1))
    for p in range(NP):
        out[p] = packed


def back(index, code):
    _, _, x, y = decode(code)
    return jnp.bitwise_xor(y, index // 4), jnp.bitwise_xor(x, index % 4)


def pair_place(there, here):
    return jnp.bitwise_xor(there, here)


def scatter_tile(t, coords, code, grad_a, grad_b, keep, send, fb):
    core, z_here, _, _ = decode(code)
    block = jnp.bitwise_and(coords[0, t], NP - 1)
    mine = jnp.bitwise_xor(block % 2, core) == 0
    place = pair_place(block // 2, z_here)
    keep[place] += jnp.where(mine, grad_a, 0.0)
    send[place] += jnp.where(mine, 0.0, grad_a)
    fb[jnp.bitwise_and(coords[1, t], NP - 1)] += grad_b


def pick_a(t, coords, code, own, oth):
    block = jnp.bitwise_and(coords[0, t], NP - 1)
    place, other = block // 2, jnp.bitwise_xor(block % 2, code % 2)
    return jnp.where(other == 0, own[place, :R], oth[place, :R])


def pick_pair(t, coords, code, own, oth):
    core, z_here, _, _ = decode(code)
    block = jnp.bitwise_and(coords[0, t], NP - 1)
    place = pair_place(block // 2, z_here)
    return jnp.where(jnp.bitwise_xor(block % 2, core) == 0, own[place], oth[place])


def pick_b(t, coords, code, stacks):
    down, along = back(jnp.bitwise_and(coords[1, t], NP - 1), code)
    found = stacks[0][along, :R]
    for m in range(1, 4):
        found = jnp.where(down == m, stacks[m][along, :R], found)
    return found


def depth_rows(products):
    sums = dot(jnp.ones((8, T), F32), jnp.concatenate(products, axis=0), 1, 1)
    return jnp.concatenate([sums[:1, :T], sums[:1, T:], jnp.zeros((6, T), F32)], axis=0)


def send_back(coords, code, values, rows_a, rows_b, rows_c, keep, send, fb):
    raws = [dot(b, v, 1, 1) for v, b in zip(values, rows_b)]
    grads_b = [dot(a * c, v, 1, 0) for v, a, c in zip(values, rows_a, rows_c)]
    depth = depth_rows([a * raw for a, raw in zip(rows_a, raws)])
    keep[...] = jnp.zeros(keep.shape, F32)
    send[...] = jnp.zeros(send.shape, F32)
    fb[...] = jnp.zeros(fb.shape, F32)
    for t in range(TILES):
        scatter_tile(t, coords, code, raws[t] * rows_c[t], grads_b[t], keep, send, fb)
    return depth


def first_body(
    coords, counts, code_ref, gz, oz, b0, b1, b2, b3, gr, orr, data,
    keep, send, fb, ta, tb, tc,
):
    code = code_ref[0]
    core = code % 2
    picked = []
    lane_row = lanes((1, T))
    for t in range(TILES):
        k = jnp.bitwise_and(coords[2, t], 2047)
        far, near = k // T, k % T
        q, j = near // 8, near % 8
        z = q // 2
        place = (z % 4) * 8 + j
        own = gr[far, pl.ds(place, 1), :]
        oth = orr[far, pl.ds(place, 1), :]
        row = jnp.where(jnp.bitwise_xor(q % 2, core) == 0, own, oth)
        row = jnp.where(z // 4 == 0, row, pltpu.roll(row, R, 1))
        picked.append(jnp.where(lane_row < R, row, 0.0))
    chosen = jnp.concatenate([*picked, jnp.zeros((T - TILES, T), F32)], axis=0)
    column = chosen.T[:R]
    tc[...] = column
    rows_a = [pick_a(t, coords, code, gz, oz) for t in range(TILES)]
    rows_b = [pick_b(t, coords, code, (b0, b1, b2, b3)) for t in range(TILES)]
    rows_c = [column[:, t : t + 1] for t in range(TILES)]
    models = [dot(a, b * c, 0, 0) for a, b, c in zip(rows_a, rows_b, rows_c)]
    values = [
        jnp.where(t < counts[0], data[t].astype(F32) - models[t], 0.0) for t in range(TILES)
    ]
    for t in range(TILES):
        ta[t] = rows_a[t]
        tb[t] = rows_b[t]
    rows = send_back(coords, code, values, rows_a, rows_b, rows_c, keep, send, fb)
    row, lane = rows_of((8, T)), lanes((8, T))
    for t in range(TILES):
        rows = jnp.where((row == 2) & (lane == t), coords[2, t].astype(F32), rows)
    send[NZ, :8] = rows


def join_body(keep, send, received, out):
    mine, theirs = send[NZ, :8], received[NZ, :8]
    extra = jnp.where(lanes((1, T)) < 4, mine[2:3], pltpu.roll(theirs, 4, 1)[2:3])
    pad = jnp.zeros((2, T), F32)
    rows = jnp.concatenate([mine[:2], theirs[:2], extra, mine[2:3] + theirs[2:3], pad], axis=0)
    for k in range(4):
        out[k, :R] = keep[2 * k] + received[2 * k]
        out[k, R : 2 * R] = keep[2 * k + 1] + received[2 * k + 1]
        out[k, 2 * R :] = rows


def pair_body(s0, s1, s2, s3, out):
    out[: 2 * R] = s0[0, : 2 * R] + s1[: 2 * R] + s2[: 2 * R] + s3[: 2 * R]
    for k, part in enumerate((s0[0, 2 * R :], s1[2 * R :], s2[2 * R :], s3[2 * R :])):
        out[2 * R + 8 * k : 2 * R + 8 * k + 8] = part


def sum_body(mine, received, gr, ga, gb, couple, out, *, scalars):
    own = mine[:R] + received[R : 2 * R]
    ga[...] = own
    couple[0] = own
    couple[1] = mine[R : 2 * R] + received[:R]
    total = gr[0]
    for p in range(1, NP):
        total = total + gr[p]
    gb[...] = total
    blocks = [half[2 * R + 8 * k : 2 * R + 8 * k + 8] for half in (mine, received) for k in range(4)]
    rows = jnp.concatenate([b[g : g + 1] for g in range(4) for b in blocks], axis=0)
    extra = jnp.concatenate([b[4:5] for b in blocks], axis=0)
    if scalars:
        extra = blocks[0]
        for b in blocks[1:]:
            extra = extra + b
    for p in range(NP):
        out[p, :R] = total
        out[p, R : R + 32] = rows
        out[p, R + 32 : R + 40] = extra


def line_body(s0, s1, s2, s3, out):
    for k, part in enumerate((s0, s1, s2, s3)):
        out[2 * k : 2 * k + 2] = part[...]


def depth_sums(coords, code, br, index):
    lane = lanes((1, T))
    near = jnp.bitwise_and(lane, 15)
    wanted = jnp.where(near >= 8, (code * 8 + near - 8).astype(F32), -1.0)
    for t in range(TILES):
        wanted = jnp.where(near == t, coords[2, t].astype(F32), wanted)
    rows = br[:, R : R + 32, :].reshape(NP * 32, T)
    known = jnp.where(lanes((NP * 32, T)) < 16, index[:, :1], index[:, 1:2])
    chosen = (known == wanted).astype(F32).astype(jnp.bfloat16)
    high, low = halves(rows)
    part = pass_of(low, chosen, 0, 0) + pass_of(high, chosen, 0, 0)
    return part[:R] + pltpu.roll(part[R:], T - 16, 1)


def apply_tile(t, coords, code, az, ao, br, ta, tb, tc, sums):
    a, b, c = ta[t], tb[t], tc[:, t : t + 1]
    da = pick_pair(t, coords, code, az, ao)
    db = br[jnp.bitwise_and(coords[1, t], NP - 1), :R]
    dc = sums[:, t : t + 1]
    left = jnp.concatenate([da, a], axis=0)
    right = jnp.concatenate([b * c, db * c + b * dc], axis=0)
    return dot(left, right, 0, 0), a, b, c


def owned(sums):
    lane = lanes((R, T))
    return jnp.where((lane >= 8) & (lane < 16), sums, 0.0)


def middle_body(
    coords, counts, code_ref, az, ao, br, ta, tb, tc, ga, gb,
    keep, send, fb, w, gc, index,
):
    code = code_ref[0]
    lane = lanes((8, T))
    for p in range(NP):
        known = br[p, R + 32 : R + 40]
        for g in range(4):
            low, high = known[:, 2 * g : 2 * g + 1], known[:, 2 * g + 1 : 2 * g + 2]
            index[32 * p + 8 * g : 32 * p + 8 * g + 8] = jnp.where(lane == 0, low, high)
    sums = depth_sums(coords, code, br, index)
    mine = owned(sums)
    gc[...] = mine
    norm = jnp.sum(ga[...] * ga[...] + gb[...] * gb[...] + mine * mine)
    made = [apply_tile(t, coords, code, az, ao, br, ta, tb, tc, sums) for t in range(TILES)]
    values = [jnp.where(t < counts[0], made[t][0], 0.0) for t in range(TILES)]
    rows_a, rows_b, rows_c = ([m[i] for m in made] for i in (1, 2, 3))
    curve = jnp.zeros((T, T), F32)
    for t in range(TILES):
        w[t] = values[t]
        curve = curve + values[t] * values[t]
    out = send_back(coords, code, values, rows_a, rows_b, rows_c, keep, send, fb)
    row, lane = rows_of((8, T)), lanes((8, T))
    out = jnp.where((row == 2) & (lane == 0), norm, out)
    send[NZ, :8] = jnp.where((row == 2) & (lane == 1), jnp.sum(curve), out)


def both_norms(br):
    total = jnp.sum(br[:, R + 32 : R + 40, :], axis=0)
    row, lane = rows_of((8, T)), lanes((8, T))
    norm = jnp.sum(jnp.where((row == 5) & (lane == 0), total, 0.0))
    curve = jnp.sum(jnp.where((row == 5) & (lane == 1), total, 0.0))
    return norm, curve


def last_body(
    coords, counts, code_ref, az, ao, br, index, ta, tb, tc, w,
    ga0, gb0, gc0, ga1, gb1, ha, hb, hc, out, spread,
):
    code = code_ref[0]
    norm, curve = both_norms(br)
    mu = jnp.full((1, 1), curve, F32) / jnp.full((1, 1), norm, F32)
    sums = depth_sums(coords, code, br, index)
    a_rest = ga1[...] - mu * ga0[...]
    b_rest = gb1[...] - mu * gb0[...]
    c_rest = owned(sums) - mu * gc0[...]
    ha[...] = a_rest
    hb[...] = b_rest
    hc[...] = c_rest
    rest = jnp.sum(a_rest * a_rest + b_rest * b_rest + c_rest * c_rest)
    bend = jnp.zeros((T, T), F32)
    for t in range(TILES):
        product, _, _, _ = apply_tile(t, coords, code, az, ao, br, ta, tb, tc, sums)
        v = jnp.where(t < counts[0], product, 0.0) - mu * w[t]
        bend = bend + v * v
    row, lane = rows_of((8, T)), lanes((8, T))
    put = jnp.where((row == 0) & (lane == 0), rest, 0.0)
    put = jnp.where((row == 0) & (lane == 1), jnp.sum(bend), put)
    put = jnp.where((row == 0) & (lane == 2), norm, put)
    put = jnp.where((row == 0) & (lane == 3), curve, put)
    out[...] = put
    spread[...] = jnp.broadcast_to(put[:1][None], spread.shape)


def end_body(damping, sums, own, ga0, gb0, gc0, ha, hb, hc, oa, ob, oc):
    lane = lanes((1, T))

    def scalar(ref, at):
        return jnp.sum(jnp.where(lane == at, ref[:1], 0.0), axis=1, keepdims=True)

    rest, bend = scalar(sums, 0), scalar(sums, 1)
    norm, curve = scalar(own, 2), scalar(own, 3)
    lam = damping[0]
    mu = curve / norm
    nu = 1.0 / (mu + lam)
    ratio = rest / norm
    second = 1.0 / (bend / rest + lam - ratio * nu)
    on_g = nu + second * ratio * nu * nu
    on_h = -second * nu
    oa[...] = on_g * ga0[...] + on_h * ha[...]
    ob[...] = on_g * gb0[...] + on_h * hb[...]
    oc[...] = (on_g * gc0[...] + on_h * hc[...]).T[8:16]


def along_z(x):
    return lax.all_to_all(x, "z", 0, 0, tiled=True)


def along_row(x):
    return lax.all_to_all(x, ROW, 0, 0, tiled=True)


def swap(x):
    return lax.ppermute(x, "c", [(0, 1), (1, 0)])


def shift(x, axis, k):
    return lax.ppermute(x, axis, [(i, i ^ k) for i in range(4)])


def from_near(x, axis):
    return tuple(shift(x, axis, k) for k in range(1, 4))


def pair_shift(x, k):
    return lax.ppermute(x, "z", [(i, i ^ (2 * k)) for i in range(8)])


def pair_swap(x):
    return lax.ppermute(x, "z", [(i, i ^ 1) for i in range(8)])


def shares(keep, send, fb, scalars):
    joined = call(join_body, shaped(4, 2 * R + 8, T), (keep, send, swap(send)))
    gr = along_row(fb)
    strides = tuple(pair_shift(joined[k], k) for k in range(1, 4))
    mine = call(
        pair_body,
        shaped(2 * R + 32, T),
        (joined, *strides),
    )
    ga, gb, couple, payload = call(
        functools.partial(sum_body, scalars=scalars),
        (shaped(R, T), shaped(R, T), shaped(2, R, T), shaped(NP, R + 40, T)),
        (mine, pair_swap(mine), gr),
    )
    br = along_row(payload)
    line = [couple]
    for k in range(1, 4):
        line.append(pair_shift(couple, k))
    az = call(line_body, shaped(NZ, R, T), line)
    return ga, gb, (az, swap(az), br)


def step_of(data, coords, counts, fr, fc, fd, damping):
    code = lax.axis_index(ROW_COL).reshape(1)
    first, fc = call(
        start_body, (shaped(NZ, R + 8, T), shaped(R, T)), (fr, fd.T, fc), limit=60
    )
    gz = along_z(first)
    payload, stack = call(
        turn_body, (shaped(NP, 32, T), shaped(4, R, T)), (gz, fc, *from_near(fc, "x"))
    )
    gr = along_row(payload)
    gr, *stacks = lax.optimization_barrier((gr, stack, *from_near(stack, "y")))
    folded = (shaped(NZ, R, T), shaped(NZ + 1, R, T), shaped(NP, R, T))
    saved = (shaped(TILES, R, T), shaped(TILES, R, T), shaped(R, T))
    keep, send, fb, ta, tb, tc = call(
        first_body,
        folded + saved,
        (coords, counts, code, gz, swap(gz), *stacks, gr, swap(gr), data),
        3,
    )
    ga0, gb0, gathered = shares(keep, send, fb, False)
    keep, send, fb, w, gc0, index = call(
        middle_body,
        folded + (shaped(TILES, T, T), shaped(R, T), shaped(NP * 32, T)),
        (coords, counts, code, *gathered, ta, tb, tc, ga0, gb0),
        3,
    )
    ga1, gb1, gathered = shares(keep, send, fb, True)
    ha, hb, hc, own, spread = call(
        last_body,
        (shaped(R, T), shaped(R, T), shaped(R, T), shaped(8, T), shaped(256, 1, T)),
        (coords, counts, code, *gathered, index, ta, tb, tc, w, ga0, gb0, gc0, ga1, gb1),
        3,
    )
    sums = jnp.sum(lax.all_to_all(spread, ALL, 0, 0, tiled=True), axis=0)
    step_a, step_b, step_c = call(
        end_body,
        (shaped(R, T), shaped(R, T), shaped(8, R)),
        (damping.reshape(1), sums, own, ga0, gb0, gc0, ha, hb, hc),
        1,
    )
    return step_a, step_b, step_c.T


def solution(mesh):
    finer = Mesh(mesh.devices.reshape(4, 4, 8, 2), ("y", "x", "z", "c"))
    in_specs = (
        P(ROW_COL, None, None),
        P(None, ROW_COL),
        P(ROW_COL),
        P(None, ROW_COL),
        P(None, COL_ROW),
        P(None, ROW_COL),
        P(),
    )
    out_specs = (P(None, ROW_COL), P(None, COL_ROW), P(None, ROW_COL))
    return jax.shard_map(
        step_of, mesh=finer, in_specs=in_specs, out_specs=out_specs, check_vma=False
    )
```

```python
import functools

import jax
import jax.numpy as jnp
from jax import lax
from jax.experimental import pallas as pl
from jax.experimental.pallas import tpu as pltpu
from jax.sharding import Mesh
from jax.sharding import PartitionSpec as P


ROW = ("y", "x")
ALL = ("y", "x", "z", "c")
ROW_COL = ("y", "x", "z", "c")
COL_ROW = ("z", "c", "y", "x")
R = 64
T = 128
TILES = 4
NZ = 8
NP = 16
F32 = jnp.float32

VMEM = pl.BlockSpec(memory_space=pltpu.VMEM)
SMEM = pl.BlockSpec(memory_space=pltpu.SMEM)


def halves(a):
    high = a.astype(jnp.bfloat16)
    return high, (a - high.astype(F32)).astype(jnp.bfloat16)


def pass_of(a, b, ca, cb):
    return lax.dot_general(a, b, (((ca,), (cb,)), ((), ())), preferred_element_type=F32)


def dot(a, b, ca, cb):
    (a_high, a_low), (b_high, b_low) = halves(a), halves(b)
    small = pass_of(a_low, b_high, ca, cb) + pass_of(a_high, b_low, ca, cb)
    return small + pass_of(a_high, b_high, ca, cb)


def shaped(*shape):
    return jax.ShapeDtypeStruct(shape, F32)


def call(body, outs, ins, scalars=0, limit=16):
    return pl.pallas_call(
        body,
        out_shape=outs,
        in_specs=[SMEM] * scalars + [VMEM] * (len(ins) - scalars),
        out_specs=jax.tree.map(lambda _: VMEM, outs),
        compiler_params=pltpu.CompilerParams(vmem_limit_bytes=limit * 2**20),
    )(*ins)


def lanes(shape):
    return lax.broadcasted_iota(jnp.int32, shape, len(shape) - 1)


def rows_of(shape):
    return lax.broadcasted_iota(jnp.int32, shape, len(shape) - 2)


def decode(code):
    return code % 2, (code // 2) % 8, (code // 16) % 4, (code // 64) % 4


def start_body(fr, fd, fc, out, near):
    near[...] = fc[...]
    columns = jnp.concatenate([fd[...], jnp.zeros((8, T - R), F32)], axis=1)
    a = fr[...]
    for z in range(NZ):
        out[z, :R] = a
        out[z, R : R + 8] = columns


def turn_body(gz, b0, b1, b2, b3, out, stack):
    for k, part in enumerate((b0, b1, b2, b3)):
        stack[k] = part[...]
    low = jnp.concatenate([gz[z, R : R + 8] for z in range(4)], axis=0)
    high = jnp.concatenate([gz[z, R : R + 8] for z in range(4, 8)], axis=0)
    packed = jnp.where(lanes((32, T)) < R, low, pltpu.roll(high, R, 1))
    for p in range(NP):
        out[p] = packed


def back(index, code):
    _, _, x, y = decode(code)
    return jnp.bitwise_xor(y, index // 4), jnp.bitwise_xor(x, index % 4)


def pair_place(there, here):
    return jnp.bitwise_xor(there, here)


def scatter_tile(t, coords, code, grad_a, grad_b, keep, send, fb):
    core, z_here, _, _ = decode(code)
    block = jnp.bitwise_and(coords[0, t], NP - 1)
    mine = jnp.bitwise_xor(block % 2, core) == 0
    place = pair_place(block // 2, z_here)
    keep[place] += jnp.where(mine, grad_a, 0.0)
    send[place] += jnp.where(mine, 0.0, grad_a)
    fb[jnp.bitwise_and(coords[1, t], NP - 1)] += grad_b


def pick_a(t, coords, code, own, oth):
    block = jnp.bitwise_and(coords[0, t], NP - 1)
    place, other = block // 2, jnp.bitwise_xor(block % 2, code % 2)
    return jnp.where(other == 0, own[place, :R], oth[place, :R])


def pick_pair(t, coords, code, own, oth):
    core, z_here, _, _ = decode(code)
    block = jnp.bitwise_and(coords[0, t], NP - 1)
    place = pair_place(block // 2, z_here)
    return jnp.where(jnp.bitwise_xor(block % 2, core) == 0, own[place], oth[place])


def pick_b(t, coords, code, stacks):
    down, along = back(jnp.bitwise_and(coords[1, t], NP - 1), code)
    found = stacks[0][along, :R]
    for m in range(1, 4):
        found = jnp.where(down == m, stacks[m][along, :R], found)
    return found


def depth_rows(products):
    sums = dot(jnp.ones((8, T), F32), jnp.concatenate(products, axis=0), 1, 1)
    return jnp.concatenate([sums[:1, :T], sums[:1, T:], jnp.zeros((6, T), F32)], axis=0)


def send_back(coords, code, values, rows_a, rows_b, rows_c, keep, send, fb):
    raws = [dot(b, v, 1, 1) for v, b in zip(values, rows_b)]
    grads_b = [dot(a * c, v, 1, 0) for v, a, c in zip(values, rows_a, rows_c)]
    depth = depth_rows([a * raw for a, raw in zip(rows_a, raws)])
    keep[...] = jnp.zeros(keep.shape, F32)
    send[...] = jnp.zeros(send.shape, F32)
    fb[...] = jnp.zeros(fb.shape, F32)
    for t in range(TILES):
        scatter_tile(t, coords, code, raws[t] * rows_c[t], grads_b[t], keep, send, fb)
    return depth


def first_body(
    coords, counts, code_ref, gz, oz, b0, b1, b2, b3, gr, orr, data,
    keep, send, fb, ta, tb, tc,
):
    code = code_ref[0]
    core = code % 2
    picked = []
    lane_row = lanes((1, T))
    for t in range(TILES):
        k = jnp.bitwise_and(coords[2, t], 2047)
        far, near = k // T, k % T
        q, j = near // 8, near % 8
        z = q // 2
        place = (z % 4) * 8 + j
        own = gr[far, pl.ds(place, 1), :]
        oth = orr[far, pl.ds(place, 1), :]
        row = jnp.where(jnp.bitwise_xor(q % 2, core) == 0, own, oth)
        row = jnp.where(z // 4 == 0, row, pltpu.roll(row, R, 1))
        picked.append(jnp.where(lane_row < R, row, 0.0))
    chosen = jnp.concatenate([*picked, jnp.zeros((T - TILES, T), F32)], axis=0)
    column = chosen.T[:R]
    tc[...] = column
    rows_a = [pick_a(t, coords, code, gz, oz) for t in range(TILES)]
    rows_b = [pick_b(t, coords, code, (b0, b1, b2, b3)) for t in range(TILES)]
    rows_c = [column[:, t : t + 1] for t in range(TILES)]
    models = [dot(a, b * c, 0, 0) for a, b, c in zip(rows_a, rows_b, rows_c)]
    values = [
        jnp.where(t < counts[0], data[t].astype(F32) - models[t], 0.0) for t in range(TILES)
    ]
    for t in range(TILES):
        ta[t] = rows_a[t]
        tb[t] = rows_b[t]
    rows = send_back(coords, code, values, rows_a, rows_b, rows_c, keep, send, fb)
    row, lane = rows_of((8, T)), lanes((8, T))
    for t in range(TILES):
        rows = jnp.where((row == 2) & (lane == t), coords[2, t].astype(F32), rows)
    send[NZ, :8] = rows


def join_body(keep, send, received, out):
    mine, theirs = send[NZ, :8], received[NZ, :8]
    extra = jnp.where(lanes((1, T)) < 4, mine[2:3], pltpu.roll(theirs, 4, 1)[2:3])
    pad = jnp.zeros((2, T), F32)
    rows = jnp.concatenate([mine[:2], theirs[:2], extra, mine[2:3] + theirs[2:3], pad], axis=0)
    for k in range(4):
        out[k, :R] = keep[2 * k] + received[2 * k]
        out[k, R : 2 * R] = keep[2 * k + 1] + received[2 * k + 1]
        out[k, 2 * R :] = rows


def pair_body(s0, s1, s2, s3, out):
    out[: 2 * R] = s0[0, : 2 * R] + s1[: 2 * R] + s2[: 2 * R] + s3[: 2 * R]
    for k, part in enumerate((s0[0, 2 * R :], s1[2 * R :], s2[2 * R :], s3[2 * R :])):
        out[2 * R + 8 * k : 2 * R + 8 * k + 8] = part


def sum_body(mine, received, gr, ga, gb, couple, out, *, scalars):
    own = mine[:R] + received[R : 2 * R]
    ga[...] = own
    couple[0] = own
    couple[1] = mine[R : 2 * R] + received[:R]
    total = gr[0]
    for p in range(1, NP):
        total = total + gr[p]
    gb[...] = total
    blocks = [half[2 * R + 8 * k : 2 * R + 8 * k + 8] for half in (mine, received) for k in range(4)]
    rows = jnp.concatenate([b[g : g + 1] for g in range(4) for b in blocks], axis=0)
    extra = jnp.concatenate([b[4:5] for b in blocks], axis=0)
    if scalars:
        extra = blocks[0]
        for b in blocks[1:]:
            extra = extra + b
    for p in range(NP):
        out[p, :R] = total
        out[p, R : R + 32] = rows
        out[p, R + 32 : R + 40] = extra


def line_body(s0, s1, s2, s3, out):
    for k, part in enumerate((s0, s1, s2, s3)):
        out[2 * k : 2 * k + 2] = part[...]


def depth_sums(coords, code, br, index):
    lane = lanes((1, T))
    near = jnp.bitwise_and(lane, 15)
    wanted = jnp.where(near >= 8, (code * 8 + near - 8).astype(F32), -1.0)
    for t in range(TILES):
        wanted = jnp.where(near == t, coords[2, t].astype(F32), wanted)
    rows = br[:, R : R + 32, :].reshape(NP * 32, T)
    known = jnp.where(lanes((NP * 32, T)) < 16, index[:, :1], index[:, 1:2])
    chosen = (known == wanted).astype(F32).astype(jnp.bfloat16)
    high, low = halves(rows)
    part = pass_of(low, chosen, 0, 0) + pass_of(high, chosen, 0, 0)
    return part[:R] + pltpu.roll(part[R:], T - 16, 1)


def apply_tile(t, coords, code, az, ao, br, ta, tb, tc, sums):
    a, b, c = ta[t], tb[t], tc[:, t : t + 1]
    da = pick_pair(t, coords, code, az, ao)
    db = br[jnp.bitwise_and(coords[1, t], NP - 1), :R]
    dc = sums[:, t : t + 1]
    left = jnp.concatenate([da, a], axis=0)
    right = jnp.concatenate([b * c, db * c + b * dc], axis=0)
    return dot(left, right, 0, 0), a, b, c


def owned(sums):
    lane = lanes((R, T))
    return jnp.where((lane >= 8) & (lane < 16), sums, 0.0)


def middle_body(
    coords, counts, code_ref, az, ao, br, ta, tb, tc, ga, gb,
    keep, send, fb, w, gc, index,
):
    code = code_ref[0]
    lane = lanes((8, T))
    for p in range(NP):
        known = br[p, R + 32 : R + 40]
        for g in range(4):
            low, high = known[:, 2 * g : 2 * g + 1], known[:, 2 * g + 1 : 2 * g + 2]
            index[32 * p + 8 * g : 32 * p + 8 * g + 8] = jnp.where(lane == 0, low, high)
    sums = depth_sums(coords, code, br, index)
    mine = owned(sums)
    gc[...] = mine
    norm = jnp.sum(ga[...] * ga[...] + gb[...] * gb[...] + mine * mine)
    made = [apply_tile(t, coords, code, az, ao, br, ta, tb, tc, sums) for t in range(TILES)]
    values = [jnp.where(t < counts[0], made[t][0], 0.0) for t in range(TILES)]
    rows_a, rows_b, rows_c = ([m[i] for m in made] for i in (1, 2, 3))
    curve = jnp.zeros((T, T), F32)
    for t in range(TILES):
        w[t] = values[t]
        curve = curve + values[t] * values[t]
    out = send_back(coords, code, values, rows_a, rows_b, rows_c, keep, send, fb)
    row, lane = rows_of((8, T)), lanes((8, T))
    out = jnp.where((row == 2) & (lane == 0), norm, out)
    send[NZ, :8] = jnp.where((row == 2) & (lane == 1), jnp.sum(curve), out)


def both_norms(br):
    total = jnp.sum(br[:, R + 32 : R + 40, :], axis=0)
    row, lane = rows_of((8, T)), lanes((8, T))
    norm = jnp.sum(jnp.where((row == 5) & (lane == 0), total, 0.0))
    curve = jnp.sum(jnp.where((row == 5) & (lane == 1), total, 0.0))
    return norm, curve


def last_body(
    coords, counts, code_ref, az, ao, br, index, ta, tb, tc, w,
    ga0, gb0, gc0, ga1, gb1, ha, hb, hc, out, spread,
):
    code = code_ref[0]
    norm, curve = both_norms(br)
    mu = jnp.full((1, 1), curve, F32) / jnp.full((1, 1), norm, F32)
    sums = depth_sums(coords, code, br, index)
    a_rest = ga1[...] - mu * ga0[...]
    b_rest = gb1[...] - mu * gb0[...]
    c_rest = owned(sums) - mu * gc0[...]
    ha[...] = a_rest
    hb[...] = b_rest
    hc[...] = c_rest
    rest = jnp.sum(a_rest * a_rest + b_rest * b_rest + c_rest * c_rest)
    bend = jnp.zeros((T, T), F32)
    for t in range(TILES):
        product, _, _, _ = apply_tile(t, coords, code, az, ao, br, ta, tb, tc, sums)
        v = jnp.where(t < counts[0], product, 0.0) - mu * w[t]
        bend = bend + v * v
    row, lane = rows_of((8, T)), lanes((8, T))
    put = jnp.where((row == 0) & (lane == 0), rest, 0.0)
    put = jnp.where((row == 0) & (lane == 1), jnp.sum(bend), put)
    put = jnp.where((row == 0) & (lane == 2), norm, put)
    put = jnp.where((row == 0) & (lane == 3), curve, put)
    out[...] = put
    spread[...] = jnp.broadcast_to(put[:1][None], spread.shape)


def end_body(damping, sums, own, ga0, gb0, gc0, ha, hb, hc, oa, ob, oc):
    lane = lanes((1, T))

    def scalar(ref, at):
        return jnp.sum(jnp.where(lane == at, ref[:1], 0.0), axis=1, keepdims=True)

    rest, bend = scalar(sums, 0), scalar(sums, 1)
    norm, curve = scalar(own, 2), scalar(own, 3)
    lam = damping[0]
    mu = curve / norm
    nu = 1.0 / (mu + lam)
    ratio = rest / norm
    second = 1.0 / (bend / rest + lam - ratio * nu)
    on_g = nu + second * ratio * nu * nu
    on_h = -second * nu
    oa[...] = on_g * ga0[...] + on_h * ha[...]
    ob[...] = on_g * gb0[...] + on_h * hb[...]
    oc[...] = (on_g * gc0[...] + on_h * hc[...]).T[8:16]


def along_z(x):
    return lax.all_to_all(x, "z", 0, 0, tiled=True)


def along_row(x):
    return lax.all_to_all(x, ROW, 0, 0, tiled=True)


def swap(x):
    return lax.ppermute(x, "c", [(0, 1), (1, 0)])


def shift(x, axis, k):
    return lax.ppermute(x, axis, [(i, i ^ k) for i in range(4)])


def from_near(x, axis):
    return tuple(shift(x, axis, k) for k in range(1, 4))


def pair_shift(x, k):
    return lax.ppermute(x, "z", [(i, i ^ (2 * k)) for i in range(8)])


def pair_swap(x):
    return lax.ppermute(x, "z", [(i, i ^ 1) for i in range(8)])


def shares(keep, send, fb, scalars):
    joined = call(join_body, shaped(4, 2 * R + 8, T), (keep, send, swap(send)))
    gr = along_row(fb)
    strides = []
    for k in range(1, 4):
        strides.append(pair_shift(joined[k], k))
    mine = call(
        pair_body,
        shaped(2 * R + 32, T),
        (joined, *strides),
    )
    ga, gb, couple, payload = call(
        functools.partial(sum_body, scalars=scalars),
        (shaped(R, T), shaped(R, T), shaped(2, R, T), shaped(NP, R + 40, T)),
        (mine, pair_swap(mine), gr),
    )
    br = along_row(payload)
    line = [couple]
    for k in range(1, 4):
        line.append(pair_shift(couple, k))
    az = call(line_body, shaped(NZ, R, T), line)
    return ga, gb, (az, swap(az), br)


def step_of(data, coords, counts, fr, fc, fd, damping):
    code = lax.axis_index(ROW_COL).reshape(1)
    first, fc = call(
        start_body, (shaped(NZ, R + 8, T), shaped(R, T)), (fr, fd.T, fc), limit=60
    )
    gz = along_z(first)
    payload, stack = call(
        turn_body, (shaped(NP, 32, T), shaped(4, R, T)), (gz, fc, *from_near(fc, "x"))
    )
    gr = along_row(payload)
    below = []
    for k in range(1, 4):
        below.append(shift(stack, "y", k))
    gr, *stacks = lax.optimization_barrier((gr, stack, *below))
    folded = (shaped(NZ, R, T), shaped(NZ + 1, R, T), shaped(NP, R, T))
    saved = (shaped(TILES, R, T), shaped(TILES, R, T), shaped(R, T))
    keep, send, fb, ta, tb, tc = call(
        first_body,
        folded + saved,
        (coords, counts, code, gz, swap(gz), *stacks, gr, swap(gr), data),
        3,
    )
    ga0, gb0, gathered = shares(keep, send, fb, False)
    keep, send, fb, w, gc0, index = call(
        middle_body,
        folded + (shaped(TILES, T, T), shaped(R, T), shaped(NP * 32, T)),
        (coords, counts, code, *gathered, ta, tb, tc, ga0, gb0),
        3,
    )
    ga1, gb1, gathered = shares(keep, send, fb, True)
    ha, hb, hc, own, spread = call(
        last_body,
        (shaped(R, T), shaped(R, T), shaped(R, T), shaped(8, T), shaped(256, 1, T)),
        (coords, counts, code, *gathered, index, ta, tb, tc, w, ga0, gb0, gc0, ga1, gb1),
        3,
    )
    sums = jnp.sum(lax.all_to_all(spread, ALL, 0, 0, tiled=True), axis=0)
    step_a, step_b, step_c = call(
        end_body,
        (shaped(R, T), shaped(R, T), shaped(8, R)),
        (damping.reshape(1), sums, own, ga0, gb0, gc0, ha, hb, hc),
        1,
    )
    return step_a, step_b, step_c.T


def solution(mesh):
    finer = Mesh(mesh.devices.reshape(4, 4, 8, 2), ("y", "x", "z", "c"))
    in_specs = (
        P(ROW_COL, None, None),
        P(None, ROW_COL),
        P(ROW_COL),
        P(None, ROW_COL),
        P(None, COL_ROW),
        P(None, ROW_COL),
        P(),
    )
    out_specs = (P(None, ROW_COL), P(None, COL_ROW), P(None, ROW_COL))
    return jax.shard_map(
        step_of, mesh=finer, in_specs=in_specs, out_specs=out_specs, check_vma=False
    )
```

```python
import functools

import jax
import jax.numpy as jnp
from jax import lax
from jax.experimental import pallas as pl
from jax.experimental.pallas import tpu as pltpu
from jax.sharding import Mesh
from jax.sharding import PartitionSpec as P


ROW = ("y", "x")
ALL = ("y", "x", "z", "c")
ROW_COL = ("y", "x", "z", "c")
COL_ROW = ("z", "c", "y", "x")
R = 64
T = 128
TILES = 4
NZ = 8
NP = 16
F32 = jnp.float32

VMEM = pl.BlockSpec(memory_space=pltpu.VMEM)
SMEM = pl.BlockSpec(memory_space=pltpu.SMEM)


def halves(a):
    high = a.astype(jnp.bfloat16)
    return high, (a - high.astype(F32)).astype(jnp.bfloat16)


def pass_of(a, b, ca, cb):
    return lax.dot_general(a, b, (((ca,), (cb,)), ((), ())), preferred_element_type=F32)


def dot(a, b, ca, cb):
    (a_high, a_low), (b_high, b_low) = halves(a), halves(b)
    small = pass_of(a_low, b_high, ca, cb) + pass_of(a_high, b_low, ca, cb)
    return small + pass_of(a_high, b_high, ca, cb)


def shaped(*shape):
    return jax.ShapeDtypeStruct(shape, F32)


def call(body, outs, ins, scalars=0, limit=16):
    return pl.pallas_call(
        body,
        out_shape=outs,
        in_specs=[SMEM] * scalars + [VMEM] * (len(ins) - scalars),
        out_specs=jax.tree.map(lambda _: VMEM, outs),
        compiler_params=pltpu.CompilerParams(vmem_limit_bytes=limit * 2**20),
    )(*ins)


def lanes(shape):
    return lax.broadcasted_iota(jnp.int32, shape, len(shape) - 1)


def rows_of(shape):
    return lax.broadcasted_iota(jnp.int32, shape, len(shape) - 2)


def decode(code):
    return code % 2, (code // 2) % 8, (code // 16) % 4, (code // 64) % 4


def start_body(fr, fd, fc, out, near):
    near[...] = fc[...]
    columns = jnp.concatenate([fd[...], jnp.zeros((8, T - R), F32)], axis=1)
    a = fr[...]
    for z in range(NZ):
        out[z, :R] = a
        out[z, R : R + 8] = columns


def turn_body(gz, b0, b1, b2, b3, out, stack):
    for k, part in enumerate((b0, b1, b2, b3)):
        stack[k] = part[...]
    low = jnp.concatenate([gz[z, R : R + 8] for z in range(4)], axis=0)
    high = jnp.concatenate([gz[z, R : R + 8] for z in range(4, 8)], axis=0)
    packed = jnp.where(lanes((32, T)) < R, low, pltpu.roll(high, R, 1))
    for p in range(NP):
        out[p] = packed


def back(index, code):
    _, _, x, y = decode(code)
    return jnp.bitwise_xor(y, index // 4), jnp.bitwise_xor(x, index % 4)


def pair_place(there, here):
    return jnp.bitwise_xor(there, here)


def scatter_tile(t, coords, code, grad_a, grad_b, keep, send, fb):
    core, z_here, _, _ = decode(code)
    block = jnp.bitwise_and(coords[0, t], NP - 1)
    mine = jnp.bitwise_xor(block % 2, core) == 0
    place = pair_place(block // 2, z_here)
    keep[place] += jnp.where(mine, grad_a, 0.0)
    send[place] += jnp.where(mine, 0.0, grad_a)
    fb[jnp.bitwise_and(coords[1, t], NP - 1)] += grad_b


def pick_a(t, coords, code, own, oth):
    block = jnp.bitwise_and(coords[0, t], NP - 1)
    place, other = block // 2, jnp.bitwise_xor(block % 2, code % 2)
    return jnp.where(other == 0, own[place, :R], oth[place, :R])


def pick_pair(t, coords, code, own, oth):
    core, z_here, _, _ = decode(code)
    block = jnp.bitwise_and(coords[0, t], NP - 1)
    place = pair_place(block // 2, z_here)
    return jnp.where(jnp.bitwise_xor(block % 2, core) == 0, own[place], oth[place])


def pick_b(t, coords, code, stacks):
    down, along = back(jnp.bitwise_and(coords[1, t], NP - 1), code)
    found = stacks[0][along, :R]
    for m in range(1, 4):
        found = jnp.where(down == m, stacks[m][along, :R], found)
    return found


def depth_rows(products):
    sums = dot(jnp.ones((8, T), F32), jnp.concatenate(products, axis=0), 1, 1)
    return jnp.concatenate([sums[:1, :T], sums[:1, T:], jnp.zeros((6, T), F32)], axis=0)


def send_back(coords, code, values, rows_a, rows_b, rows_c, keep, send, fb):
    raws = [dot(b, v, 1, 1) for v, b in zip(values, rows_b)]
    grads_b = [dot(a * c, v, 1, 0) for v, a, c in zip(values, rows_a, rows_c)]
    depth = depth_rows([a * raw for a, raw in zip(rows_a, raws)])
    keep[...] = jnp.zeros(keep.shape, F32)
    send[...] = jnp.zeros(send.shape, F32)
    fb[...] = jnp.zeros(fb.shape, F32)
    for t in range(TILES):
        scatter_tile(t, coords, code, raws[t] * rows_c[t], grads_b[t], keep, send, fb)
    return depth


def first_body(
    coords, counts, code_ref, gz, oz, b0, b1, b2, b3, gr, orr, data,
    keep, send, fb, ta, tb, tc,
):
    code = code_ref[0]
    core = code % 2
    picked = []
    lane_row = lanes((1, T))
    for t in range(TILES):
        k = jnp.bitwise_and(coords[2, t], 2047)
        far, near = k // T, k % T
        q, j = near // 8, near % 8
        z = q // 2
        place = (z % 4) * 8 + j
        own = gr[far, pl.ds(place, 1), :]
        oth = orr[far, pl.ds(place, 1), :]
        row = jnp.where(jnp.bitwise_xor(q % 2, core) == 0, own, oth)
        row = jnp.where(z // 4 == 0, row, pltpu.roll(row, R, 1))
        picked.append(jnp.where(lane_row < R, row, 0.0))
    chosen = jnp.concatenate([*picked, jnp.zeros((T - TILES, T), F32)], axis=0)
    column = chosen.T[:R]
    tc[...] = column
    rows_a = [pick_a(t, coords, code, gz, oz) for t in range(TILES)]
    rows_b = [pick_b(t, coords, code, (b0, b1, b2, b3)) for t in range(TILES)]
    rows_c = [column[:, t : t + 1] for t in range(TILES)]
    models = [dot(a, b * c, 0, 0) for a, b, c in zip(rows_a, rows_b, rows_c)]
    values = [
        jnp.where(t < counts[0], data[t].astype(F32) - models[t], 0.0) for t in range(TILES)
    ]
    for t in range(TILES):
        ta[t] = rows_a[t]
        tb[t] = rows_b[t]
    rows = send_back(coords, code, values, rows_a, rows_b, rows_c, keep, send, fb)
    row, lane = rows_of((8, T)), lanes((8, T))
    for t in range(TILES):
        rows = jnp.where((row == 2) & (lane == t), coords[2, t].astype(F32), rows)
    send[NZ, :8] = rows


def join_body(keep, send, received, out):
    mine, theirs = send[NZ, :8], received[NZ, :8]
    extra = jnp.where(lanes((1, T)) < 4, mine[2:3], pltpu.roll(theirs, 4, 1)[2:3])
    pad = jnp.zeros((2, T), F32)
    rows = jnp.concatenate([mine[:2], theirs[:2], extra, mine[2:3] + theirs[2:3], pad], axis=0)
    for k in range(4):
        out[k, :R] = keep[2 * k] + received[2 * k]
        out[k, R : 2 * R] = keep[2 * k + 1] + received[2 * k + 1]
        out[k, 2 * R :] = rows


def pair_body(s0, s1, s2, s3, out):
    out[: 2 * R] = s0[0, : 2 * R] + s1[: 2 * R] + s2[: 2 * R] + s3[: 2 * R]
    for k, part in enumerate((s0[0, 2 * R :], s1[2 * R :], s2[2 * R :], s3[2 * R :])):
        out[2 * R + 8 * k : 2 * R + 8 * k + 8] = part


def couple_body(mine, received, ga, couple):
    own = mine[:R] + received[R : 2 * R]
    ga[...] = own
    couple[0] = own
    couple[1] = mine[R : 2 * R] + received[:R]


def sum_body(mine, received, gr, gb, out, *, scalars):
    total = gr[0]
    for p in range(1, NP):
        total = total + gr[p]
    gb[...] = total
    blocks = [half[2 * R + 8 * k : 2 * R + 8 * k + 8] for half in (mine, received) for k in range(4)]
    rows = jnp.concatenate([b[g : g + 1] for g in range(4) for b in blocks], axis=0)
    extra = jnp.concatenate([b[4:5] for b in blocks], axis=0)
    if scalars:
        extra = blocks[0]
        for b in blocks[1:]:
            extra = extra + b
    for p in range(NP):
        out[p, :R] = total
        out[p, R : R + 32] = rows
        out[p, R + 32 : R + 40] = extra


def line_body(s0, s1, s2, s3, out):
    for k, part in enumerate((s0, s1, s2, s3)):
        out[2 * k : 2 * k + 2] = part[...]


def depth_sums(coords, code, br, index):
    lane = lanes((1, T))
    near = jnp.bitwise_and(lane, 15)
    wanted = jnp.where(near >= 8, (code * 8 + near - 8).astype(F32), -1.0)
    for t in range(TILES):
        wanted = jnp.where(near == t, coords[2, t].astype(F32), wanted)
    rows = br[:, R : R + 32, :].reshape(NP * 32, T)
    known = jnp.where(lanes((NP * 32, T)) < 16, index[:, :1], index[:, 1:2])
    chosen = (known == wanted).astype(F32).astype(jnp.bfloat16)
    high, low = halves(rows)
    part = pass_of(low, chosen, 0, 0) + pass_of(high, chosen, 0, 0)
    return part[:R] + pltpu.roll(part[R:], T - 16, 1)


def apply_tile(t, coords, code, az, ao, br, ta, tb, tc, sums):
    a, b, c = ta[t], tb[t], tc[:, t : t + 1]
    da = pick_pair(t, coords, code, az, ao)
    db = br[jnp.bitwise_and(coords[1, t], NP - 1), :R]
    dc = sums[:, t : t + 1]
    left = jnp.concatenate([da, a], axis=0)
    right = jnp.concatenate([b * c, db * c + b * dc], axis=0)
    return dot(left, right, 0, 0), a, b, c


def owned(sums):
    lane = lanes((R, T))
    return jnp.where((lane >= 8) & (lane < 16), sums, 0.0)


def middle_body(
    coords, counts, code_ref, az, ao, br, ta, tb, tc, ga, gb,
    keep, send, fb, w, gc, index,
):
    code = code_ref[0]
    lane = lanes((8, T))
    for p in range(NP):
        known = br[p, R + 32 : R + 40]
        for g in range(4):
            low, high = known[:, 2 * g : 2 * g + 1], known[:, 2 * g + 1 : 2 * g + 2]
            index[32 * p + 8 * g : 32 * p + 8 * g + 8] = jnp.where(lane == 0, low, high)
    sums = depth_sums(coords, code, br, index)
    mine = owned(sums)
    gc[...] = mine
    norm = jnp.sum(ga[...] * ga[...] + gb[...] * gb[...] + mine * mine)
    made = [apply_tile(t, coords, code, az, ao, br, ta, tb, tc, sums) for t in range(TILES)]
    values = [jnp.where(t < counts[0], made[t][0], 0.0) for t in range(TILES)]
    rows_a, rows_b, rows_c = ([m[i] for m in made] for i in (1, 2, 3))
    curve = jnp.zeros((T, T), F32)
    for t in range(TILES):
        w[t] = values[t]
        curve = curve + values[t] * values[t]
    out = send_back(coords, code, values, rows_a, rows_b, rows_c, keep, send, fb)
    row, lane = rows_of((8, T)), lanes((8, T))
    out = jnp.where((row == 2) & (lane == 0), norm, out)
    send[NZ, :8] = jnp.where((row == 2) & (lane == 1), jnp.sum(curve), out)


def both_norms(br):
    total = jnp.sum(br[:, R + 32 : R + 40, :], axis=0)
    row, lane = rows_of((8, T)), lanes((8, T))
    norm = jnp.sum(jnp.where((row == 5) & (lane == 0), total, 0.0))
    curve = jnp.sum(jnp.where((row == 5) & (lane == 1), total, 0.0))
    return norm, curve


def last_body(
    coords, counts, code_ref, az, ao, br, index, ta, tb, tc, w,
    ga0, gb0, gc0, ga1, gb1, ha, hb, hc, out, spread,
):
    code = code_ref[0]
    norm, curve = both_norms(br)
    mu = jnp.full((1, 1), curve, F32) / jnp.full((1, 1), norm, F32)
    sums = depth_sums(coords, code, br, index)
    a_rest = ga1[...] - mu * ga0[...]
    b_rest = gb1[...] - mu * gb0[...]
    c_rest = owned(sums) - mu * gc0[...]
    ha[...] = a_rest
    hb[...] = b_rest
    hc[...] = c_rest
    rest = jnp.sum(a_rest * a_rest + b_rest * b_rest + c_rest * c_rest)
    bend = jnp.zeros((T, T), F32)
    for t in range(TILES):
        product, _, _, _ = apply_tile(t, coords, code, az, ao, br, ta, tb, tc, sums)
        v = jnp.where(t < counts[0], product, 0.0) - mu * w[t]
        bend = bend + v * v
    row, lane = rows_of((8, T)), lanes((8, T))
    put = jnp.where((row == 0) & (lane == 0), rest, 0.0)
    put = jnp.where((row == 0) & (lane == 1), jnp.sum(bend), put)
    put = jnp.where((row == 0) & (lane == 2), norm, put)
    put = jnp.where((row == 0) & (lane == 3), curve, put)
    out[...] = put
    spread[...] = jnp.broadcast_to(put[:1][None], spread.shape)


def end_body(damping, sums, own, ga0, gb0, gc0, ha, hb, hc, oa, ob, oc):
    lane = lanes((1, T))

    def scalar(ref, at):
        return jnp.sum(jnp.where(lane == at, ref[:1], 0.0), axis=1, keepdims=True)

    rest, bend = scalar(sums, 0), scalar(sums, 1)
    norm, curve = scalar(own, 2), scalar(own, 3)
    lam = damping[0]
    mu = curve / norm
    nu = 1.0 / (mu + lam)
    ratio = rest / norm
    second = 1.0 / (bend / rest + lam - ratio * nu)
    on_g = nu + second * ratio * nu * nu
    on_h = -second * nu
    oa[...] = on_g * ga0[...] + on_h * ha[...]
    ob[...] = on_g * gb0[...] + on_h * hb[...]
    oc[...] = (on_g * gc0[...] + on_h * hc[...]).T[8:16]


def along_z(x):
    return lax.all_to_all(x, "z", 0, 0, tiled=True)


def along_row(x):
    return lax.all_to_all(x, ROW, 0, 0, tiled=True)


def swap(x):
    return lax.ppermute(x, "c", [(0, 1), (1, 0)])


def shift(x, axis, k):
    return lax.ppermute(x, axis, [(i, i ^ k) for i in range(4)])


def from_near(x, axis):
    return tuple(shift(x, axis, k) for k in range(1, 4))


def pair_shift(x, k):
    return lax.ppermute(x, "z", [(i, i ^ (2 * k)) for i in range(8)])


def pair_swap(x):
    return lax.ppermute(x, "z", [(i, i ^ 1) for i in range(8)])


def shares(keep, send, fb, scalars):
    joined = call(join_body, shaped(4, 2 * R + 8, T), (keep, send, swap(send)))
    gr = along_row(fb)
    strides = []
    for k in range(1, 4):
        strides.append(pair_shift(joined[k], k))
    mine = call(
        pair_body,
        shaped(2 * R + 32, T),
        (joined, *strides),
    )
    received = pair_swap(mine)
    ga, couple = call(couple_body, (shaped(R, T), shaped(2, R, T)), (mine, received))
    gb, payload = call(
        functools.partial(sum_body, scalars=scalars),
        (shaped(R, T), shaped(NP, R + 40, T)),
        (mine, received, gr),
    )
    br = along_row(payload)
    line = [couple]
    for k in range(1, 4):
        line.append(pair_shift(couple, k))
    az = call(line_body, shaped(NZ, R, T), line)
    return ga, gb, (az, swap(az), br)


def step_of(data, coords, counts, fr, fc, fd, damping):
    code = lax.axis_index(ROW_COL).reshape(1)
    first, fc = call(
        start_body, (shaped(NZ, R + 8, T), shaped(R, T)), (fr, fd.T, fc), limit=60
    )
    gz = along_z(first)
    payload, stack = call(
        turn_body, (shaped(NP, 32, T), shaped(4, R, T)), (gz, fc, *from_near(fc, "x"))
    )
    gr = along_row(payload)
    below = []
    for k in range(1, 4):
        below.append(shift(stack, "y", k))
    gr, *stacks = lax.optimization_barrier((gr, stack, *below))
    folded = (shaped(NZ, R, T), shaped(NZ + 1, R, T), shaped(NP, R, T))
    saved = (shaped(TILES, R, T), shaped(TILES, R, T), shaped(R, T))
    keep, send, fb, ta, tb, tc = call(
        first_body,
        folded + saved,
        (coords, counts, code, gz, swap(gz), *stacks, gr, swap(gr), data),
        3,
    )
    ga0, gb0, gathered = shares(keep, send, fb, False)
    keep, send, fb, w, gc0, index = call(
        middle_body,
        folded + (shaped(TILES, T, T), shaped(R, T), shaped(NP * 32, T)),
        (coords, counts, code, *gathered, ta, tb, tc, ga0, gb0),
        3,
    )
    ga1, gb1, gathered = shares(keep, send, fb, True)
    ha, hb, hc, own, spread = call(
        last_body,
        (shaped(R, T), shaped(R, T), shaped(R, T), shaped(8, T), shaped(256, 1, T)),
        (coords, counts, code, *gathered, index, ta, tb, tc, w, ga0, gb0, gc0, ga1, gb1),
        3,
    )
    sums = jnp.sum(lax.all_to_all(spread, ALL, 0, 0, tiled=True), axis=0)
    step_a, step_b, step_c = call(
        end_body,
        (shaped(R, T), shaped(R, T), shaped(8, R)),
        (damping.reshape(1), sums, own, ga0, gb0, gc0, ha, hb, hc),
        1,
    )
    return step_a, step_b, step_c.T


def solution(mesh):
    finer = Mesh(mesh.devices.reshape(4, 4, 8, 2), ("y", "x", "z", "c"))
    in_specs = (
        P(ROW_COL, None, None),
        P(None, ROW_COL),
        P(ROW_COL),
        P(None, ROW_COL),
        P(None, COL_ROW),
        P(None, ROW_COL),
        P(),
    )
    out_specs = (P(None, ROW_COL), P(None, COL_ROW), P(None, ROW_COL))
    return jax.shard_map(
        step_of, mesh=finer, in_specs=in_specs, out_specs=out_specs, check_vma=False
    )
```
